8 devices in a mesh: pc: 2 (over z, y), pr: 4 (over x, core).
Axes of the slice: x: 2, y: 2, z: 1, core: 2. Of those that a mesh axis runs over, the one named last changes fastest.
Arguments:
- panel_in: float32 [6144, 16, 128], P('pr', 'pc')
- trail_in: float32 [6144, 4096], P('pr', 'pc')
Outputs:
- output 1: float32 [6144, 16, 128], P('pr', 'pc')
- output 2: float32 [6144, 4096], P('pr', 'pc')
All inputs are finite; a program needn't handle non-finite values.
Results may differ from the reference program's by a relative error of at most 0.001.
Values sent between devices are 32-bit elements.
A program may use at most 1 GiB of HBM per device.

```python
import jax
import jax.numpy as jnp
from jax import lax

N = 6144
NB = 128
K = 16
PR = 4
PC = 2
RANK = 2048

BLOCKS = N // NB
ROW_BLOCKS = BLOCKS // PR
TRAIL_COLS = N - K * NB
PREC_HIGH = lax.Precision.HIGHEST


def rows_to_owner(full_mat):
    col_width = full_mat.shape[1]
    return full_mat.reshape(ROW_BLOCKS, PR, NB, col_width).transpose(1, 0, 2, 3).reshape(N, col_width)


def rows_from_owner(stored):
    col_width = stored.shape[1]
    return stored.reshape(PR, ROW_BLOCKS, NB, col_width).transpose(1, 0, 2, 3).reshape(N, col_width)


def cols_to_owner(full_mat):
    block_count = full_mat.shape[1] // NB
    return full_mat.reshape(N, block_count // PC, PC, NB).transpose(0, 2, 1, 3).reshape(N, block_count, NB)


def cols_from_owner(stored):
    block_count = stored.shape[1]
    return stored.reshape(N, PC, block_count // PC, NB).transpose(0, 2, 1, 3).reshape(N, block_count * NB)


def build_layout(full_mat):
    row_major = rows_to_owner(full_mat)
    panel_in = cols_to_owner(row_major[:, :K * NB])
    trail_in = cols_to_owner(row_major[:, K * NB:]).reshape(N, TRAIL_COLS)
    return {"panel_in": panel_in, "trail_in": trail_in}


def setup_inputs(seed: int = 0) -> dict:
    key_low, key_diag = jax.random.split(jax.random.key(seed))
    factor = jax.random.normal(key_low, (N, RANK), jnp.float32)
    diag_shift = 0.5 + jax.random.uniform(key_diag, (N,), jnp.float32)
    low_rank = jnp.dot(factor, factor.T, precision=PREC_HIGH) / RANK
    full_mat = 0.5 * (low_rank + low_rank.T) + jnp.diag(diag_shift)
    return build_layout(full_mat)


def reference(panel_in, trail_in):
    stored = jnp.concatenate([cols_from_owner(panel_in), cols_from_owner(trail_in.reshape(N, BLOCKS - K, NB))], axis=1)
    work_mat = rows_from_owner(stored)
    factor_cols = []
    kept_rows = []
    for panel_step in range(K):
        l_diag = jnp.linalg.cholesky(work_mat[:NB, :NB])
        below_diag = lax.linalg.triangular_solve(l_diag, work_mat[NB:, :NB], left_side=False, lower=True, transpose_a=True)
        factor_cols.append(jnp.concatenate([jnp.zeros((panel_step * NB, NB), work_mat.dtype), l_diag, below_diag], axis=0))
        kept_rows.append(work_mat[:NB, (K - panel_step) * NB:])
        work_mat = work_mat[NB:, NB:] - jnp.dot(below_diag, below_diag.T, precision=PREC_HIGH)
    panel_full = jnp.concatenate(factor_cols, axis=1)
    trail_full = jnp.concatenate(kept_rows + [work_mat], axis=0)
    panel_out = cols_to_owner(rows_to_owner(panel_full))
    trail_out = cols_to_owner(rows_to_owner(trail_full)).reshape(N, TRAIL_COLS)
    return panel_out, trail_out
```

```python
import jax
import jax.numpy as jnp
from jax import lax
from jax.experimental import pallas as pl
from jax.experimental.pallas import tpu as pltpu
from jax.sharding import PartitionSpec as P

HIGH = lax.Precision.HIGHEST
MESH = pl.DeviceIdType.MESH
NB = 128
PAIRS = 8


def dot_nt(a, b):
    return lax.dot_general(a, b, (((1,), (1,)), ((), ())), precision=HIGH, preferred_element_type=jnp.float32)


def dot_nn(a, b):
    return lax.dot_general(a, b, (((1,), (0,)), ((), ())), precision=HIGH, preferred_element_type=jnp.float32)


def lane_of(x, lane):
    return jnp.broadcast_to(x[:, lane:lane + 1], (8, NB))


def row_of(x, row):
    return jnp.broadcast_to(x[row:row + 1, :], (8, NB))


def factor_block(load, store_upper, store_inv):
    lane = lax.broadcasted_iota(jnp.int32, (8, NB), 1)
    sub = lax.broadcasted_iota(jnp.int32, (8, NB), 0)
    rows = [load(i) for i in range(16)]
    for g in range(16):
        base = 8 * g
        inside = (lane >= base) & (lane < base + 8)
        cols = [lane_of(rows[g], base + t) for t in range(8)]
        cur = jnp.where(inside, jnp.where(lane - base == sub, 1.0, 0.0), rows[g])
        recips, pivots, cross = [], [], {}
        for s in range(8):
            recip = 1.0 / row_of(cols[s], s)
            pivot = row_of(cur, s)
            mult = jnp.where(sub > s, cols[s] * recip, 0.0)
            for t in range(s + 1, 8):
                cross[t, s] = row_of(cols[t], s)
                cols[t] = cols[t] - mult * cross[t, s]
            if s < 7:
                cur = cur - mult * pivot
            recips.append(recip)
            pivots.append(pivot)
        for i in range(g + 1, 16):
            part = [lane_of(rows[i], base + t) for t in range(8)]
            acc = jnp.where(inside, 0.0, rows[i])
            for s in range(8):
                mult = part[s] * recips[s]
                for t in range(s + 1, 8):
                    part[t] = part[t] - mult * cross[t, s]
                acc = acc - mult * pivots[s]
            rows[i] = acc
        diag = cols[7]
        upper = jnp.where(lane > base + 7, cur, 0.0)
        for t in range(8):
            if t < 7:
                diag = jnp.where(sub == t, cols[t], diag)
            upper = jnp.where((lane == base + t) & (sub <= t), cols[t], upper)
        scale = lax.rsqrt(diag)
        scale = scale * (1.5 - 0.5 * diag * scale * scale)
        store_upper(g, upper * scale)
        store_inv(g, jnp.where(lane < base + 8, cur, 0.0) * scale)


def body(pan, lead, trail, pan_out, trail_out, work, cols, diag, upper, inv, tile, zero,
         lead_sem, own_sem, own_send, own_recv, keep_sem, give_send, give_recv, pass_send, far_send, far_recv,
         in_sem, out_sem, pan_sem):
    my_row = lax.axis_index("pr")
    my_col = lax.axis_index("pc")
    chip = my_row // 2
    core = my_row % 2
    across = {"pr": my_row, "pc": 1 - my_col}
    beside = {"pr": 2 * chip + 1 - core, "pc": my_col}
    along = {"pr": 2 * (1 - chip) + core, "pc": my_col}
    is_giver = core == my_col

    barrier = pltpu.get_barrier_semaphore()
    for peer in (across, beside, along):
        pl.semaphore_signal(barrier, inc=1, device_id=peer, device_id_type=MESH)

    def half(c):
        return pl.ds(pl.multiple_of(c * NB, NB), NB)

    for p in range(PAIRS):
        for c in range(2):
            for r in range(4):
                for q in range(4):
                    pltpu.make_async_copy(lead.at[q, c, p, r], work.at[p, 4 * r + q, :, pl.ds(c * NB, NB)], lead_sem.at[p]).start()
    for p in range(PAIRS):
        pltpu.make_async_copy(pan.at[p, 4:12], work.at[p, 16:24, :, half(my_col)], own_sem.at[p]).start()
    zero[...] = jnp.zeros_like(zero)
    pl.semaphore_wait(barrier, 3)

    def own_copy(p):
        return pltpu.make_async_remote_copy(
            src_ref=pan.at[p, 4:12], dst_ref=work.at[p, 16:24, :, half(my_col)],
            send_sem=own_send.at[p], recv_sem=own_recv.at[p], device_id=across, device_id_type=MESH)

    def own_arrival(p):
        return pltpu.make_async_remote_copy(
            src_ref=pan.at[p, 4:12], dst_ref=work.at[p, 16:24, :, half(1 - my_col)],
            send_sem=own_send.at[p], recv_sem=own_recv.at[p], device_id=across, device_id_type=MESH)

    for p in range(PAIRS):
        own_copy(p).start()

    def keep_copy(p):
        return pltpu.make_async_copy(work.at[p, 16:24], cols.at[p, :, chip], keep_sem.at[p])

    def give_copy(p):
        return pltpu.make_async_remote_copy(
            src_ref=work.at[p, 16:24], dst_ref=cols.at[p, :, chip],
            send_sem=give_send.at[p], recv_sem=give_recv.at[p], device_id=beside, device_id_type=MESH)

    def far_copy(p):
        return pltpu.make_async_remote_copy(
            src_ref=work.at[p, 16:24], dst_ref=cols.at[p, :, chip],
            send_sem=far_send.at[p], recv_sem=far_recv.at[p], device_id=along, device_id_type=MESH)

    def far_arrival(p):
        return pltpu.make_async_remote_copy(
            src_ref=work.at[p, 16:24], dst_ref=cols.at[p, :, 1 - chip],
            send_sem=far_send.at[p], recv_sem=far_recv.at[p], device_id=along, device_id_type=MESH)

    def pass_copy(p):
        return pltpu.make_async_remote_copy(
            src_ref=cols.at[p, :, 1 - chip], dst_ref=cols.at[p, :, 1 - chip],
            send_sem=pass_send.at[p], recv_sem=far_recv.at[p], device_id=beside, device_id_type=MESH)

    def rows256(p, c):
        return work[p, pl.ds(2 * c, 2)].reshape(256, 256)

    def set_rows256(p, c, value):
        work[p, pl.ds(2 * c, 2)] = value.reshape(2, NB, 256)

    def factor(h, p):
        def store_upper(g, value):
            upper[8 * g:8 * g + 8, :] = value

        def store_inv(g, value):
            inv[h * NB + 8 * g:h * NB + 8 * g + 8, h * NB:(h + 1) * NB] = value

        factor_block(lambda i: diag[8 * i:8 * i + 8, :], store_upper, store_inv)
        work[p, 2 * p + h, :, h * NB:(h + 1) * NB] = upper[...].T

    inv[0:NB, NB:256] = jnp.zeros((NB, NB), jnp.float32)

    def chain_step(p, carry):
        pltpu.make_async_copy(work.at[p, 0:16], work.at[p, 0:16], lead_sem.at[p]).wait()
        pltpu.make_async_copy(pan.at[p, 4:12], work.at[p, 16:24, :, half(my_col)], own_sem.at[p]).wait()
        own_arrival(p).wait_recv()

        def subtract(q, carry):
            right = rows256(q, p)

            def one(c, carry):
                set_rows256(p, c, rows256(p, c) - dot_nt(rows256(q, c), right))
                return carry

            return lax.fori_loop(p, 12, one, carry)

        lax.fori_loop(0, p, subtract, 0)

        diag[...] = work[p, 2 * p, :, 0:NB]
        factor(0, p)
        work[p, 2 * p, :, NB:256] = jnp.zeros((NB, NB), jnp.float32)
        inv0 = inv[0:NB, 0:NB]
        low = dot_nt(work[p, 2 * p + 1, :, 0:NB], inv0)
        work[p, 2 * p + 1, :, 0:NB] = low
        diag[...] = work[p, 2 * p + 1, :, NB:256] - dot_nt(low, low)
        factor(1, p)
        inv[NB:256, 0:NB] = -dot_nn(inv[NB:256, NB:256], dot_nn(low, inv0))

        def solve(c, carry):
            set_rows256(p, c, dot_nt(rows256(p, c), inv[...]))
            return carry

        lax.fori_loop(p + 1, 12, solve, 0)

        @pl.when(is_giver)
        def _():
            keep_copy(p).start()
            give_copy(p).start()
            far_copy(p).start()

            @pl.when(p > 0)
            def _():
                far_arrival(p - 1).wait_recv()
                pass_copy(p - 1).start()

        return carry

    lax.fori_loop(0, PAIRS, chain_step, 0)

    @pl.when(is_giver)
    def _():
        far_arrival(PAIRS - 1).wait_recv()
        pass_copy(PAIRS - 1).start()

    def pan_result(p, r):
        block = 4 * r + my_row
        return (pltpu.make_async_copy(work.at[p, block, :, half(my_col)], pan_out.at[p, r], pan_sem.at[0]),
                pltpu.make_async_copy(zero, pan_out.at[p, r], pan_sem.at[0]))

    def start_pan(p, carry):
        pltpu.make_async_copy(work.at[p, 16:24, :, half(my_col)], pan_out.at[p, 4:12], pan_sem.at[0]).start()
        for r in range(4):
            filled, empty = pan_result(p, r)
            below = 4 * r + my_row >= 2 * p + my_col

            @pl.when(below)
            def _():
                filled.start()

            @pl.when(jnp.logical_not(below))
            def _():
                empty.start()

        return carry

    lax.fori_loop(0, PAIRS, start_pan, 0)

    def tile_in(b, slot):
        return pltpu.make_async_copy(trail.at[pl.ds(512, 1024), pl.ds(pl.multiple_of(b * 256, 256), 256)],
                                     tile.at[slot, pl.ds(512, 1024)], in_sem.at[slot])

    def tile_out(b, slot):
        return pltpu.make_async_copy(tile.at[slot], trail_out.at[:, pl.ds(pl.multiple_of(b * 256, 256), 256)], out_sem.at[slot])

    tile_in(0, 0).start()

    def drain(p, carry):
        @pl.when(is_giver)
        def _():
            keep_copy(p).wait()

        @pl.when(jnp.logical_not(is_giver))
        def _():
            pltpu.make_async_remote_copy(
                src_ref=work.at[p, 16:24], dst_ref=cols.at[p, :, chip],
                send_sem=give_send.at[p], recv_sem=give_recv.at[p], device_id=beside, device_id_type=MESH).wait_recv()
            far_arrival(p).wait_recv()

        return carry

    lax.fori_loop(0, PAIRS, drain, 0)

    def trail_step(b, carry):
        slot = b % 2

        @pl.when(b > 0)
        def _():
            tile_out(b - 1, 1 - slot).wait()

        @pl.when(b < 7)
        def _():
            tile_in(b + 1, 1 - slot).start()

        for r in range(4):
            block = 4 * r + my_row
            p = block // 2
            side = half(block % 2)
            tile[slot, r * NB:(r + 1) * NB, :] = dot_nt(work[p, block, :, side], cols[p, b, :, :, side].reshape(256, NB))
        tile_in(b, slot).wait()

        def subtract(q, carry):
            right = cols[q, b].reshape(256, 256)

            def one(c, carry):
                where = pl.ds(512 + c * 256, 256)
                tile[slot, where, :] = tile[slot, where, :] - dot_nt(rows256(q, 8 + c), right)
                return carry

            return lax.fori_loop(0, 4, one, carry)

        lax.fori_loop(0, PAIRS, subtract, 0)
        tile_out(b, slot).start()
        return carry

    lax.fori_loop(0, 8, trail_step, 0)
    tile_out(7, 1).wait()
    pltpu.make_async_copy(pan_out, pan_out, pan_sem.at[0]).wait()

    def finish(p, carry):
        own_copy(p).wait_send()

        @pl.when(is_giver)
        def _():
            give_copy(p).wait_send()
            far_copy(p).wait_send()
            pass_copy(p).wait_send()

        return carry

    lax.fori_loop(0, PAIRS, finish, 0)


def solution(mesh):
    def local_part(panel_tile, trail_tile):
        pan = panel_tile.transpose(1, 0, 2).reshape(PAIRS, 12, NB, NB)
        lead = lax.all_gather(lax.all_gather(pan[:, 0:4], "pc", axis=0), "pr", axis=0)
        any_spec = pl.BlockSpec(memory_space=pl.ANY)
        dma = pltpu.SemaphoreType.DMA
        pan_out, trail_out = pl.pallas_call(
            body,
            out_shape=(jax.ShapeDtypeStruct(pan.shape, jnp.float32), jax.ShapeDtypeStruct(trail_tile.shape, jnp.float32)),
            in_specs=[any_spec] * 3,
            out_specs=(any_spec, any_spec),
            scratch_shapes=[
                pltpu.VMEM((PAIRS, 24, NB, 256), jnp.float32),
                pltpu.VMEM((PAIRS, 8, 2, NB, 256), jnp.float32),
                pltpu.VMEM((NB, NB), jnp.float32),
                pltpu.VMEM((NB, NB), jnp.float32),
                pltpu.VMEM((256, 256), jnp.float32),
                pltpu.VMEM((2, 1536, 256), jnp.float32),
                pltpu.VMEM((NB, NB), jnp.float32),
                dma((PAIRS,)), dma((PAIRS,)), dma((PAIRS,)), dma((PAIRS,)), dma((PAIRS,)), dma((PAIRS,)), dma((PAIRS,)),
                dma((PAIRS,)), dma((PAIRS,)), dma((PAIRS,)), dma((2,)), dma((2,)), dma((1,)),
            ],
            compiler_params=pltpu.CompilerParams(collective_id=0, has_side_effects=True, vmem_limit_bytes=64 * 1024 * 1024 - 65536),
            name="factor",
        )(pan, lead, trail_tile)
        return pan_out.reshape(PAIRS, 1536, NB).transpose(1, 0, 2), trail_out

    spec_panel = P("pr", "pc", None)
    spec_trail = P("pr", "pc")
    return jax.shard_map(local_part, mesh=mesh, in_specs=(spec_panel, spec_trail), out_specs=(spec_panel, spec_trail), check_vma=False)
```

```python
import jax
import jax.numpy as jnp
from jax import lax
from jax.experimental import pallas as pl
from jax.experimental.pallas import tpu as pltpu
from jax.sharding import PartitionSpec as P

HIGH = lax.Precision.HIGHEST
MESH = pl.DeviceIdType.MESH
NB = 128
PAIRS = 8


def dot_nt(a, b):
    return lax.dot_general(a, b, (((1,), (1,)), ((), ())), precision=HIGH, preferred_element_type=jnp.float32)


def dot_nn(a, b):
    return lax.dot_general(a, b, (((1,), (0,)), ((), ())), precision=HIGH, preferred_element_type=jnp.float32)


def lane_of(x, lane):
    return jnp.broadcast_to(x[:, lane:lane + 1], (8, NB))


def row_of(x, row):
    return jnp.broadcast_to(x[row:row + 1, :], (8, NB))


def factor_block(load, store_upper, store_inv, beside=None):
    lane = lax.broadcasted_iota(jnp.int32, (8, NB), 1)
    sub = lax.broadcasted_iota(jnp.int32, (8, NB), 0)
    rows = [load(i) for i in range(16)]
    for g in range(16):
        base = 8 * g
        inside = (lane >= base) & (lane < base + 8)
        cols = [lane_of(rows[g], base + t) for t in range(8)]
        cur = jnp.where(inside, jnp.where(lane - base == sub, 1.0, 0.0), rows[g])
        recips, pivots, cross = [], [], {}
        for s in range(8):
            recip = 1.0 / row_of(cols[s], s)
            pivot = row_of(cur, s)
            mult = jnp.where(sub > s, cols[s] * recip, 0.0)
            for t in range(s + 1, 8):
                cross[t, s] = row_of(cols[t], s)
                cols[t] = cols[t] - mult * cross[t, s]
            if s < 7:
                cur = cur - mult * pivot
            recips.append(recip)
            pivots.append(pivot)
        for i in range(g + 1, 16):
            part = [lane_of(rows[i], base + t) for t in range(8)]
            acc = jnp.where(inside, 0.0, rows[i])
            for s in range(8):
                mult = part[s] * recips[s]
                for t in range(s + 1, 8):
                    part[t] = part[t] - mult * cross[t, s]
                acc = acc - mult * pivots[s]
            rows[i] = acc
        if beside is not None:
            beside(g)
        diag = cols[7]
        upper = jnp.where(lane > base + 7, cur, 0.0)
        for t in range(8):
            if t < 7:
                diag = jnp.where(sub == t, cols[t], diag)
            upper = jnp.where((lane == base + t) & (sub <= t), cols[t], upper)
        scale = lax.rsqrt(diag)
        scale = scale * (1.5 - 0.5 * diag * scale * scale)
        store_upper(g, upper * scale)
        store_inv(g, jnp.where(lane < base + 8, cur, 0.0) * scale)


def body(pan, trail, pan_out, trail_out, work, cols, schur, diag, upper, inv, gmat, top, zero,
         lead_sem, lead_send, lead_recv, own_sem, own_send, own_recv, keep_sem, give_send, give_recv, pass_send,
         far_send, far_recv, in_sem, out_sem, top_sem, pan_sem):
    my_row = lax.axis_index("pr")
    my_col = lax.axis_index("pc")
    chip = my_row // 2
    core = my_row % 2
    beside_row = 2 * chip + 1 - core
    along_row = 2 * (1 - chip) + core
    cross_row = 2 * (1 - chip) + 1 - core
    across = {"pr": my_row, "pc": 1 - my_col}
    beside = {"pr": beside_row, "pc": my_col}
    along = {"pr": along_row, "pc": my_col}
    is_giver = core == my_col

    barrier = pltpu.get_barrier_semaphore()
    for peer in (across, beside, along):
        pl.semaphore_signal(barrier, inc=1, device_id=peer, device_id_type=MESH)

    def half(c):
        return pl.ds(pl.multiple_of(c * NB, NB), NB)

    def remote(src, dst, send, recv, peer):
        return pltpu.make_async_remote_copy(src_ref=src, dst_ref=dst, send_sem=send, recv_sem=recv,
                                            device_id=peer, device_id_type=MESH)

    def strip(p, first, row, col):
        return work.at[p, first:4, row, :, half(col)]

    def mine(p, first):
        return pan.at[p, 0, first:4]

    def for_pair(p, fn):
        if isinstance(p, int):
            fn(p // 2)
        else:
            for first in range(4):
                pl.when(p // 2 == first)(lambda first=first: fn(first))

    def keep_strip(p, first):
        return pltpu.make_async_copy(mine(p, first), strip(p, first, my_row, my_col), lead_sem.at[p])

    def lead_copy(p, first, kind):
        out = strip(p, first, my_row, my_col)
        src, dst, peer = {
            0: (mine(p, first), out, beside),
            1: (mine(p, first), out, along),
            2: (mine(p, first), out, across),
            3: (strip(p, first, my_row, 1 - my_col), strip(p, first, my_row, 1 - my_col), along),
            4: (strip(p, first, along_row, my_col), strip(p, first, along_row, my_col), beside),
            5: (strip(p, first, my_row, 1 - my_col), strip(p, first, my_row, 1 - my_col), beside),
            6: (strip(p, first, along_row, 1 - my_col), strip(p, first, along_row, 1 - my_col), beside),
            7: (strip(p, first, along_row, my_col), strip(p, first, along_row, my_col), across),
        }[kind]
        slot = 3 if kind == 7 else kind
        return remote(src, dst, lead_send.at[p, slot], lead_recv.at[p, slot], peer)

    def lead_arrival(p, first, kind):
        row, col = [(beside_row, my_col), (along_row, my_col), (my_row, 1 - my_col), (along_row, 1 - my_col),
                    (cross_row, my_col), (beside_row, 1 - my_col), (cross_row, 1 - my_col)][kind]
        return remote(mine(p, first), strip(p, first, row, col), lead_send.at[p, kind], lead_recv.at[p, kind], beside)

    def stage_one(p):
        def go(first):
            for kind in (1, 2, 0):
                lead_copy(p, first, kind).start()

        for_pair(p, go)

    def stage_two(p):
        def go(first):
            lead_arrival(p, first, 1).wait_recv()
            lead_arrival(p, first, 2).wait_recv()

            @pl.when(core == 0)
            def _():
                lead_copy(p, first, 3).start()

            @pl.when(core == 1)
            def _():
                lead_copy(p, first, 7).start()

            lead_copy(p, first, 4).start()
            lead_copy(p, first, 5).start()

        for_pair(p, go)

    def stage_three(p):
        def go(first):
            lead_arrival(p, first, 3).wait_recv()
            lead_copy(p, first, 6).start()

        for_pair(p, go)

    def lead_wait(p):
        def go(first):
            keep_strip(p, first).wait()
            for kind in (0, 4, 5, 6):
                lead_arrival(p, first, kind).wait_recv()
            for kind in range(7):
                lead_copy(p, first, kind).wait_send()

        for_pair(p, go)

    def keep_own(p):
        return pltpu.make_async_copy(pan.at[p, 1:3], work.at[p, 4:6, :, :, half(my_col)], own_sem.at[p])

    def own_copy(p):
        return remote(pan.at[p, 1:3], work.at[p, 4:6, :, :, half(my_col)], own_send.at[p], own_recv.at[p], across)

    def own_arrival(p):
        return remote(pan.at[p, 1:3], work.at[p, 4:6, :, :, half(1 - my_col)], own_send.at[p], own_recv.at[p], across)

    def keep_copy(p):
        return pltpu.make_async_copy(work.at[p, 4:6], cols.at[p, :, :, chip], keep_sem.at[p])

    def give_copy(p):
        return remote(work.at[p, 4:6], cols.at[p, :, :, chip], give_send.at[p], give_recv.at[p], beside)

    def far_copy(p):
        return remote(work.at[p, 4:6], cols.at[p, :, :, chip], far_send.at[p], far_recv.at[p], along)

    def far_arrival(p):
        return remote(work.at[p, 4:6], cols.at[p, :, :, 1 - chip], far_send.at[p], far_recv.at[p], along)

    def pass_copy(p):
        return remote(cols.at[p, :, :, 1 - chip], cols.at[p, :, :, 1 - chip], pass_send.at[p], far_recv.at[p], beside)

    def cols_wait(p):
        @pl.when(is_giver)
        def _():
            keep_copy(p).wait()

        @pl.when(jnp.logical_not(is_giver))
        def _():
            give_copy(p).wait_recv()
            far_arrival(p).wait_recv()

    def rows256(p, c):
        return work[p, c // 2, pl.ds(2 * (c % 2), 2)].reshape(256, 256)

    def set_rows256(p, c, value):
        work[p, c // 2, pl.ds(2 * (c % 2), 2)] = value.reshape(2, NB, 256)

    def rows512(p, c):
        return work[p, c].reshape(512, 256)

    def set_rows512(p, c, value):
        work[p, c] = value.reshape(4, NB, 256)

    def tile_in(b):
        return pltpu.make_async_copy(trail.at[pl.ds(512, 1024), pl.ds(b * 256, 256)], schur.at[b], in_sem.at[b])

    for p in range(PAIRS):
        keep_strip(p, p // 2).start()
    zero[...] = jnp.zeros_like(zero)
    pl.semaphore_wait(barrier, 3)
    stage_one(0)
    for p in range(PAIRS):
        keep_own(p).start()
    for b in range(8):
        tile_in(b).start()
    stage_two(0)
    stage_one(1)
    own_copy(0).start()
    stage_three(0)

    def schur_update(q, b, c):
        where = pl.ds(c * 256, 256)
        right = cols[q, b // 4, b % 4].reshape(256, 256)
        schur[b, where, :] = schur[b, where, :] - dot_nt(rows256(q, 8 + c), right)

    def idle_or_update(p, h, g):
        idle = p < 2
        c = g % 4
        b = 4 * h + g // 4
        hi = jnp.where(idle, 0, 4 + c // 2)
        lo = jnp.where(idle, 0, 2 * (c % 2))
        left = work[jnp.where(idle, 0, p - 2), hi, pl.ds(lo, 2)].reshape(256, 256)
        right = cols[jnp.where(idle, PAIRS - 1, p - 2), h, g // 4].reshape(256, 256)
        b = jnp.where(idle, 8, b)
        where = pl.ds(c * 256, 256)
        schur[b, where, :] = schur[b, where, :] - dot_nt(left, right)

    def factor(h, p):
        def store_upper(g, value):
            upper[8 * g:8 * g + 8, :] = value

        def store_inv(g, value):
            inv[h, 8 * g:8 * g + 8, :] = value

        factor_block(lambda i: diag[8 * i:8 * i + 8, :], store_upper, store_inv, lambda g: idle_or_update(p, h, g))
        work[p, p // 2, 2 * (p % 2) + h, :, half(h)] = upper[...].T

    gmat[...] = jnp.zeros_like(gmat)

    def chain_step(p, carry):
        lead_wait(p)

        @pl.when(p + 2 < PAIRS)
        def _():
            stage_one(p + 2)

        @pl.when(p + 1 < PAIRS)
        def _():
            own_copy(p + 1).start()

        def subtract(q, carry):
            right = rows256(q, p)

            def one(c, carry):
                set_rows256(p, c, rows256(p, c) - dot_nt(rows256(q, c), right))
                return carry

            return lax.fori_loop(p, 8, one, carry)

        lax.fori_loop(0, p, subtract, 0)

        @pl.when(p == 2)
        def _():
            for b in range(8):
                tile_in(b).wait()

        @pl.when(p >= 2)
        def _():
            cols_wait(p - 2)

        hi, lo = p // 2, 2 * (p % 2)
        diag[...] = work[p, hi, lo, :, 0:NB]

        def factor_half(h, carry):
            factor(h, p)

            @pl.when(h == 0)
            def _():
                work[p, hi, lo, :, NB:256] = jnp.zeros((NB, NB), jnp.float32)
                low = dot_nt(work[p, hi, lo + 1, :, 0:NB], inv[0])
                work[p, hi, lo + 1, :, 0:NB] = low
                diag[...] = work[p, hi, lo + 1, :, NB:256] - dot_nt(low, low)

            @pl.when((h == 0) & (p + 1 < PAIRS))
            def _():
                stage_two(p + 1)

            return carry

        lax.fori_loop(0, 2, factor_half, 0)

        @pl.when(p + 1 < PAIRS)
        def _():
            stage_three(p + 1)

        @pl.when(is_giver & (p > 0))
        def _():
            far_arrival(p - 1).wait_recv()
            pass_copy(p - 1).start()

        gmat[0:NB, 0:NB] = inv[0]
        gmat[NB:256, NB:256] = inv[1]
        gmat[NB:256, 0:NB] = -dot_nn(inv[1], dot_nn(work[p, hi, lo + 1, :, 0:NB], inv[0]))

        keep_own(p).wait()
        own_arrival(p).wait_recv()

        def subtract_own(q, carry):
            right = rows256(q, p)

            def one(c, carry):
                set_rows512(p, c, rows512(p, c) - dot_nt(rows512(q, c), right))
                return carry

            return lax.fori_loop(4, 6, one, carry)

        lax.fori_loop(0, p, subtract_own, 0)

        def solve(c, carry):
            set_rows256(p, c, dot_nt(rows256(p, c), gmat[...]))
            return carry

        lax.fori_loop(p + 1, 12, solve, 0)

        @pl.when(is_giver)
        def _():
            far_copy(p).start()
            keep_copy(p).start()
            give_copy(p).start()

        return carry

    lax.fori_loop(0, PAIRS, chain_step, 0)

    def start_pan(p, carry):
        pltpu.make_async_copy(work.at[p, 4:6, :, :, half(my_col)], pan_out.at[p, 1:3], pan_sem.at[0]).start()
        for r in range(4):
            below = 4 * r + my_row >= 2 * p + my_col

            @pl.when(below)
            def _():
                pltpu.make_async_copy(work.at[p, r, my_row, :, half(my_col)], pan_out.at[p, 0, r], pan_sem.at[0]).start()

            @pl.when(jnp.logical_not(below))
            def _():
                pltpu.make_async_copy(zero, pan_out.at[p, 0, r], pan_sem.at[0]).start()

        return carry

    lax.fori_loop(0, PAIRS, start_pan, 0)

    def tail(q):
        cols_wait(q)

        def one(i, carry):
            schur_update(q, i // 4, i % 4)
            return carry

        lax.fori_loop(0, 32, one, 0)

    tail(PAIRS - 2)

    @pl.when(is_giver)
    def _():
        far_arrival(PAIRS - 1).wait_recv()
        pass_copy(PAIRS - 1).start()

    cols_wait(PAIRS - 1)

    def cols_of(b):
        return pl.ds(pl.multiple_of(b * 256, 256), 256)

    def schur_out(b):
        return pltpu.make_async_copy(schur.at[b], trail_out.at[pl.ds(512, 1024), cols_of(b)], out_sem.at[b])

    def top_out(b, slot):
        return pltpu.make_async_copy(top.at[slot], trail_out.at[pl.ds(0, 512), cols_of(b)], top_sem.at[slot])

    def last_step(b, carry):
        def one(c, carry):
            schur_update(PAIRS - 1, b, c)
            return carry

        lax.fori_loop(0, 4, one, 0)
        schur_out(b).start()
        slot = b % 2

        @pl.when(b >= 2)
        def _():
            top_out(b - 2, slot).wait()

        for r in range(4):
            p = 2 * r + my_row // 2
            side = half(my_row % 2)
            top[slot, r * NB:(r + 1) * NB, :] = dot_nt(work[p, r, my_row, :, side],
                                                       cols[p, b // 4, b % 4, :, :, side].reshape(256, NB))
        top_out(b, slot).start()
        return carry

    lax.fori_loop(0, 8, last_step, 0)
    top_out(6, 0).wait()
    top_out(7, 1).wait()
    for b in range(8):
        schur_out(b).wait()
    pltpu.make_async_copy(pan_out, pan_out, pan_sem.at[0]).wait()

    def finish(p, carry):
        own_copy(p).wait_send()

        @pl.when(is_giver)
        def _():
            give_copy(p).wait_send()
            far_copy(p).wait_send()
            pass_copy(p).wait_send()

        return carry

    lax.fori_loop(0, PAIRS, finish, 0)


def solution(mesh):
    def local_part(panel_tile, trail_tile):
        pan = panel_tile.transpose(1, 0, 2).reshape(PAIRS, 3, 4, NB, NB)
        any_spec = pl.BlockSpec(memory_space=pl.ANY)
        dma = pltpu.SemaphoreType.DMA
        pan_out, trail_out = pl.pallas_call(
            body,
            out_shape=(jax.ShapeDtypeStruct(pan.shape, jnp.float32), jax.ShapeDtypeStruct(trail_tile.shape, jnp.float32)),
            in_specs=[any_spec] * 2,
            out_specs=(any_spec, any_spec),
            scratch_shapes=[
                pltpu.VMEM((PAIRS, 6, 4, NB, 256), jnp.float32),
                pltpu.VMEM((PAIRS, 2, 4, 2, NB, 256), jnp.float32),
                pltpu.VMEM((9, 1024, 256), jnp.float32),
                pltpu.VMEM((NB, NB), jnp.float32),
                pltpu.VMEM((NB, NB), jnp.float32),
                pltpu.VMEM((2, NB, NB), jnp.float32),
                pltpu.VMEM((256, 256), jnp.float32),
                pltpu.VMEM((2, 512, 256), jnp.float32),
                pltpu.VMEM((NB, NB), jnp.float32),
                dma((PAIRS,)), dma((PAIRS, 7)), dma((PAIRS, 7)), dma((PAIRS,)), dma((PAIRS,)), dma((PAIRS,)), dma((PAIRS,)),
                dma((PAIRS,)), dma((PAIRS,)), dma((PAIRS,)), dma((PAIRS,)), dma((PAIRS,)), dma((8,)), dma((8,)), dma((2,)),
                dma((1,)),
            ],
            compiler_params=pltpu.CompilerParams(collective_id=0, has_side_effects=True, vmem_limit_bytes=64 * 1024 * 1024 - 65536),
            name="factor",
        )(pan, trail_tile)
        return pan_out.reshape(PAIRS, 1536, NB).transpose(1, 0, 2), trail_out

    spec_panel = P("pr", "pc", None)
    spec_trail = P("pr", "pc")
    return jax.shard_map(local_part, mesh=mesh, in_specs=(spec_panel, spec_trail), out_specs=(spec_panel, spec_trail), check_vma=False)
```

```python
import jax
import jax.numpy as jnp
from jax import lax
from jax.experimental import pallas as pl
from jax.experimental.pallas import tpu as pltpu
from jax.sharding import PartitionSpec as P

HIGH = lax.Precision.HIGHEST
MESH = pl.DeviceIdType.MESH
NB = 128
PAIRS = 8


def dot_nt(a, b):
    return lax.dot_general(a, b, (((1,), (1,)), ((), ())), precision=HIGH, preferred_element_type=jnp.float32)


def dot_nn(a, b):
    return lax.dot_general(a, b, (((1,), (0,)), ((), ())), precision=HIGH, preferred_element_type=jnp.float32)


def lane_of(x, lane):
    return jnp.broadcast_to(x[:, lane:lane + 1], (8, NB))


def row_of(x, row):
    return jnp.broadcast_to(x[row:row + 1, :], (8, NB))


def factor_block(load, store_upper, store_inv, beside=None):
    lane = lax.broadcasted_iota(jnp.int32, (8, NB), 1)
    sub = lax.broadcasted_iota(jnp.int32, (8, NB), 0)
    rows = [load(i) for i in range(16)]
    for g in range(16):
        base = 8 * g
        inside = (lane >= base) & (lane < base + 8)
        cols = [lane_of(rows[g], base + t) for t in range(8)]
        cur = jnp.where(inside, jnp.where(lane - base == sub, 1.0, 0.0), rows[g])
        recips, pivots, cross = [], [], {}
        for s in range(8):
            recip = 1.0 / row_of(cols[s], s)
            pivot = row_of(cur, s)
            mult = jnp.where(sub > s, cols[s] * recip, 0.0)
            for t in range(s + 1, 8):
                cross[t, s] = row_of(cols[t], s)
                cols[t] = cols[t] - mult * cross[t, s]
            if s < 7:
                cur = cur - mult * pivot
            recips.append(recip)
            pivots.append(pivot)
        for i in range(g + 1, 16):
            part = [lane_of(rows[i], base + t) for t in range(8)]
            acc = jnp.where(inside, 0.0, rows[i])
            for s in range(8):
                mult = part[s] * recips[s]
                for t in range(s + 1, 8):
                    part[t] = part[t] - mult * cross[t, s]
                acc = acc - mult * pivots[s]
            rows[i] = acc
        if beside is not None:
            beside(g)
        diag = cols[7]
        upper = jnp.where(lane > base + 7, cur, 0.0)
        for t in range(8):
            if t < 7:
                diag = jnp.where(sub == t, cols[t], diag)
            upper = jnp.where((lane == base + t) & (sub <= t), cols[t], upper)
        scale = lax.rsqrt(diag)
        scale = scale * (1.5 - 0.5 * diag * scale * scale)
        store_upper(g, upper * scale)
        store_inv(g, jnp.where(lane < base + 8, cur, 0.0) * scale)


def body(pan, trail, pan_out, schur_out, top_out, left_out, right_out, work, cols, schur, diag, upper, inv, gmat, top, zero,
         lead_sem, lead_send, lead_recv, own_sem, own_send, own_recv, keep_sem, give_send, give_recv, pass_send,
         far_send, far_recv, in_sem, out_sem, top_sem, left_sem, pan_sem):
    my_row = lax.axis_index("pr")
    my_col = lax.axis_index("pc")
    chip = my_row // 2
    core = my_row % 2
    beside_row = 2 * chip + 1 - core
    along_row = 2 * (1 - chip) + core
    cross_row = 2 * (1 - chip) + 1 - core
    across = {"pr": my_row, "pc": 1 - my_col}
    beside = {"pr": beside_row, "pc": my_col}
    along = {"pr": along_row, "pc": my_col}
    is_giver = core == my_col

    barrier = pltpu.get_barrier_semaphore()
    for peer in (across, beside, along):
        pl.semaphore_signal(barrier, inc=1, device_id=peer, device_id_type=MESH)

    def half(c):
        return pl.ds(pl.multiple_of(c * NB, NB), NB)

    def remote(src, dst, send, recv, peer):
        return pltpu.make_async_remote_copy(src_ref=src, dst_ref=dst, send_sem=send, recv_sem=recv,
                                            device_id=peer, device_id_type=MESH)

    def strip(p, first, row, col):
        return work.at[p, first:4, row, :, half(col)]

    def mine(p, first):
        return pan.at[p, 0, first:4]

    def for_pair(p, fn):
        if isinstance(p, int):
            fn(p // 2)
        else:
            for first in range(4):
                pl.when(p // 2 == first)(lambda first=first: fn(first))

    def keep_strip(p, first):
        return pltpu.make_async_copy(mine(p, first), strip(p, first, my_row, my_col), lead_sem.at[p])

    def lead_copy(p, first, kind):
        out = strip(p, first, my_row, my_col)
        src, dst, peer = {
            0: (mine(p, first), out, beside),
            1: (mine(p, first), out, along),
            2: (mine(p, first), out, across),
            3: (strip(p, first, my_row, 1 - my_col), strip(p, first, my_row, 1 - my_col), along),
            4: (strip(p, first, along_row, my_col), strip(p, first, along_row, my_col), beside),
            5: (strip(p, first, my_row, 1 - my_col), strip(p, first, my_row, 1 - my_col), beside),
            6: (strip(p, first, along_row, 1 - my_col), strip(p, first, along_row, 1 - my_col), beside),
            7: (strip(p, first, along_row, my_col), strip(p, first, along_row, my_col), across),
        }[kind]
        slot = 3 if kind == 7 else kind
        return remote(src, dst, lead_send.at[p, slot], lead_recv.at[p, slot], peer)

    def lead_arrival(p, first, kind):
        row, col = [(beside_row, my_col), (along_row, my_col), (my_row, 1 - my_col), (along_row, 1 - my_col),
                    (cross_row, my_col), (beside_row, 1 - my_col), (cross_row, 1 - my_col)][kind]
        return remote(mine(p, first), strip(p, first, row, col), lead_send.at[p, kind], lead_recv.at[p, kind], beside)

    def stage_one(p):
        def go(first):
            for kind in (1, 2, 0):
                lead_copy(p, first, kind).start()

        for_pair(p, go)

    def stage_two(p):
        def go(first):
            lead_arrival(p, first, 1).wait_recv()
            lead_arrival(p, first, 2).wait_recv()

            @pl.when(core == 0)
            def _():
                lead_copy(p, first, 3).start()

            @pl.when(core == 1)
            def _():
                lead_copy(p, first, 7).start()

            lead_copy(p, first, 4).start()
            lead_copy(p, first, 5).start()

        for_pair(p, go)

    def stage_three(p):
        def go(first):
            lead_arrival(p, first, 3).wait_recv()
            lead_copy(p, first, 6).start()

        for_pair(p, go)

    def lead_wait(p):
        def go(first):
            keep_strip(p, first).wait()
            for kind in (0, 4, 5, 6):
                lead_arrival(p, first, kind).wait_recv()
            for kind in range(7):
                lead_copy(p, first, kind).wait_send()

        for_pair(p, go)

    def keep_own(p):
        return pltpu.make_async_copy(pan.at[p, 1:3], work.at[p, 4:6, :, :, half(my_col)], own_sem.at[p])

    def own_copy(p):
        return remote(pan.at[p, 1:3], work.at[p, 4:6, :, :, half(my_col)], own_send.at[p], own_recv.at[p], across)

    def own_arrival(p):
        return remote(pan.at[p, 1:3], work.at[p, 4:6, :, :, half(1 - my_col)], own_send.at[p], own_recv.at[p], across)

    def keep_copy(p):
        return pltpu.make_async_copy(work.at[p, 4:6], cols.at[p, :, :, chip], keep_sem.at[p])

    def give_copy(p):
        return remote(work.at[p, 4:6], cols.at[p, :, :, chip], give_send.at[p], give_recv.at[p], beside)

    def far_copy(p):
        return remote(work.at[p, 4:6], cols.at[p, :, :, chip], far_send.at[p], far_recv.at[p], along)

    def far_arrival(p):
        return remote(work.at[p, 4:6], cols.at[p, :, :, 1 - chip], far_send.at[p], far_recv.at[p], along)

    def pass_copy(p):
        return remote(cols.at[p, :, :, 1 - chip], cols.at[p, :, :, 1 - chip], pass_send.at[p], far_recv.at[p], beside)

    def cols_wait(p):
        @pl.when(is_giver)
        def _():
            keep_copy(p).wait()

        @pl.when(jnp.logical_not(is_giver))
        def _():
            give_copy(p).wait_recv()
            far_arrival(p).wait_recv()

    def rows256(p, c):
        return work[p, c // 2, pl.ds(2 * (c % 2), 2)].reshape(256, 256)

    def set_rows256(p, c, value):
        work[p, c // 2, pl.ds(2 * (c % 2), 2)] = value.reshape(2, NB, 256)

    def own_rows(p):
        return work[p, 4:6].reshape(1024, 256)

    def set_own(p, value):
        work[p, 4:6] = value.reshape(2, 4, NB, 256)

    def tile_in(b):
        return pltpu.make_async_copy(trail.at[pl.ds(512, 1024), pl.ds(b * 256, 256)], schur.at[b], in_sem.at[b])

    for p in range(PAIRS):
        keep_strip(p, p // 2).start()
    zero[...] = jnp.zeros_like(zero)
    pl.semaphore_wait(barrier, 3)
    stage_one(0)
    for p in range(PAIRS):
        keep_own(p).start()
    for b in range(8):
        tile_in(b).start()
    stage_two(0)
    stage_one(1)
    own_copy(0).start()
    stage_three(0)

    def schur_update(q, b, c):
        where = pl.ds(c * 256, 256)
        right = cols[q, b // 4, b % 4].reshape(256, 256)
        schur[b, where, :] = schur[b, where, :] - dot_nt(rows256(q, 8 + c), right)

    def factor(h, p):
        def store_upper(g, value):
            upper[8 * g:8 * g + 8, :] = value

        def store_inv(g, value):
            inv[h, 8 * g:8 * g + 8, :] = value

        def load(i):
            return diag[8 * i:8 * i + 8, :]

        @pl.when(p < 2)
        def _():
            factor_block(load, store_upper, store_inv)

        @pl.when(p >= 2)
        def _():
            factor_block(load, store_upper, store_inv, lambda g: schur_update(p - 2, 4 * h + g // 4, g % 4))

        work[p, p // 2, 2 * (p % 2) + h, :, half(h)] = upper[...].T

    gmat[...] = jnp.zeros_like(gmat)

    def chain_step(p, carry):
        lead_wait(p)

        @pl.when(p + 2 < PAIRS)
        def _():
            stage_one(p + 2)

        @pl.when(p + 1 < PAIRS)
        def _():
            own_copy(p + 1).start()

        def subtract(q, carry):
            right = rows256(q, p)

            def one(c, carry):
                set_rows256(p, c, rows256(p, c) - dot_nt(rows256(q, c), right))
                return carry

            return lax.fori_loop(p, 8, one, carry)

        lax.fori_loop(0, p, subtract, 0)

        @pl.when(p == 2)
        def _():
            for b in range(8):
                tile_in(b).wait()

        @pl.when(p >= 2)
        def _():
            cols_wait(p - 2)

        hi, lo = p // 2, 2 * (p % 2)
        diag[...] = work[p, hi, lo, :, 0:NB]

        def factor_half(h, carry):
            factor(h, p)

            @pl.when(h == 0)
            def _():
                work[p, hi, lo, :, NB:256] = jnp.zeros((NB, NB), jnp.float32)
                low = dot_nt(work[p, hi, lo + 1, :, 0:NB], inv[0])
                work[p, hi, lo + 1, :, 0:NB] = low
                diag[...] = work[p, hi, lo + 1, :, NB:256] - dot_nt(low, low)

            @pl.when((h == 0) & (p + 1 < PAIRS))
            def _():
                stage_two(p + 1)

            return carry

        lax.fori_loop(0, 2, factor_half, 0)

        @pl.when(p + 1 < PAIRS)
        def _():
            stage_three(p + 1)

        @pl.when(is_giver & (p > 0))
        def _():
            far_arrival(p - 1).wait_recv()
            pass_copy(p - 1).start()

        gmat[0:NB, 0:NB] = inv[0]
        gmat[NB:256, NB:256] = inv[1]
        gmat[NB:256, 0:NB] = -dot_nn(inv[1], dot_nn(work[p, hi, lo + 1, :, 0:NB], inv[0]))

        keep_own(p).wait()
        own_arrival(p).wait_recv()

        def subtract_own(q, carry):
            set_own(p, own_rows(p) - dot_nt(own_rows(q), rows256(q, p)))
            return carry

        lax.fori_loop(0, p, subtract_own, 0)

        def solve(c, carry):
            set_rows256(p, c, dot_nt(rows256(p, c), gmat[...]))
            return carry

        lax.fori_loop(p + 1, 8, solve, 0)
        set_own(p, dot_nt(own_rows(p), gmat[...]))

        @pl.when(is_giver)
        def _():
            far_copy(p).start()
            keep_copy(p).start()
            give_copy(p).start()

        return carry

    lax.fori_loop(0, PAIRS, chain_step, 0)

    def start_pan(p, carry):
        pltpu.make_async_copy(work.at[p, 4:6, :, :, half(my_col)], pan_out.at[p, 1:3], pan_sem.at[0]).start()
        for r in range(4):
            below = 4 * r + my_row >= 2 * p + my_col

            @pl.when(below)
            def _():
                pltpu.make_async_copy(work.at[p, r, my_row, :, half(my_col)], pan_out.at[p, 0, r], pan_sem.at[0]).start()

            @pl.when(jnp.logical_not(below))
            def _():
                pltpu.make_async_copy(zero, pan_out.at[p, 0, r], pan_sem.at[0]).start()

        return carry

    lax.fori_loop(0, PAIRS, start_pan, 0)

    cols_wait(PAIRS - 2)

    def left_copy():
        return pltpu.make_async_copy(work.at[PAIRS - 1, 4:6], left_out, left_sem.at[0])

    def right_copy():
        return pltpu.make_async_copy(cols.at[PAIRS - 1], right_out, left_sem.at[1])

    def schur_copy(b):
        return pltpu.make_async_copy(schur.at[b], schur_out.at[b], out_sem.at[b])

    def top_copy(b, slot):
        return pltpu.make_async_copy(top.at[slot], top_out.at[b], top_sem.at[slot])

    left_copy().start()

    def tail(b, carry):
        def one(c, carry):
            schur_update(PAIRS - 2, b, c)
            return carry

        lax.fori_loop(0, 4, one, 0)
        schur_copy(b).start()
        return carry

    lax.fori_loop(0, 8, tail, 0)

    @pl.when(is_giver)
    def _():
        far_arrival(PAIRS - 1).wait_recv()
        pass_copy(PAIRS - 1).start()

    cols_wait(PAIRS - 1)
    right_copy().start()

    def top_step(b, carry):
        slot = b % 2

        @pl.when(b >= 2)
        def _():
            top_copy(b - 2, slot).wait()

        for r in range(4):
            p = 2 * r + my_row // 2
            side = half(my_row % 2)
            top[slot, r * NB:(r + 1) * NB, :] = dot_nt(work[p, r, my_row, :, side],
                                                       cols[p, b // 4, b % 4, :, :, side].reshape(256, NB))
        top_copy(b, slot).start()
        return carry

    lax.fori_loop(0, 8, top_step, 0)
    top_copy(6, 0).wait()
    top_copy(7, 1).wait()
    for b in range(8):
        schur_copy(b).wait()
    left_copy().wait()
    right_copy().wait()
    pltpu.make_async_copy(pan_out, pan_out, pan_sem.at[0]).wait()

    def finish(p, carry):
        own_copy(p).wait_send()

        @pl.when(is_giver)
        def _():
            give_copy(p).wait_send()
            far_copy(p).wait_send()
            pass_copy(p).wait_send()

        return carry

    lax.fori_loop(0, PAIRS, finish, 0)


def finish_body(schur, top, left, right, pan, trail_out, pan_out):
    trail_out[0:512, :] = top[0]
    right_tile = right[0, 0].reshape(256, 256)
    for c in range(4):
        where = slice(256 * c, 256 * c + 256)
        rows = left[c // 2, 2 * (c % 2):2 * (c % 2) + 2].reshape(256, 256)
        trail_out[512 + 256 * c:768 + 256 * c, :] = schur[0, where, :] - dot_nt(rows, right_tile)
    flat = pan_out.reshape(192 * PAIRS, NB)
    for p in range(PAIRS):
        flat[pl.ds(p, 192, stride=PAIRS), :] = pan[p]


def solution(mesh):
    def local_part(panel_tile, trail_tile):
        pan = panel_tile.transpose(1, 0, 2).reshape(PAIRS, 3, 4, NB, NB)
        any_spec = pl.BlockSpec(memory_space=pl.ANY)
        dma = pltpu.SemaphoreType.DMA
        f32 = jnp.float32
        pan_out, schur, top, left, right = pl.pallas_call(
            body,
            out_shape=(jax.ShapeDtypeStruct(pan.shape, f32), jax.ShapeDtypeStruct((8, 1024, 256), f32),
                       jax.ShapeDtypeStruct((8, 512, 256), f32), jax.ShapeDtypeStruct((2, 4, NB, 256), f32),
                       jax.ShapeDtypeStruct((2, 4, 2, NB, 256), f32)),
            in_specs=[any_spec] * 2,
            out_specs=(any_spec,) * 5,
            scratch_shapes=[
                pltpu.VMEM((PAIRS, 6, 4, NB, 256), jnp.float32),
                pltpu.VMEM((PAIRS, 2, 4, 2, NB, 256), jnp.float32),
                pltpu.VMEM((8, 1024, 256), jnp.float32),
                pltpu.VMEM((NB, NB), jnp.float32),
                pltpu.VMEM((NB, NB), jnp.float32),
                pltpu.VMEM((2, NB, NB), jnp.float32),
                pltpu.VMEM((256, 256), jnp.float32),
                pltpu.VMEM((2, 512, 256), jnp.float32),
                pltpu.VMEM((NB, NB), jnp.float32),
                dma((PAIRS,)), dma((PAIRS, 7)), dma((PAIRS, 7)), dma((PAIRS,)), dma((PAIRS,)), dma((PAIRS,)), dma((PAIRS,)),
                dma((PAIRS,)), dma((PAIRS,)), dma((PAIRS,)), dma((PAIRS,)), dma((PAIRS,)), dma((8,)), dma((8,)), dma((2,)), dma((2,)),
                dma((1,)),
            ],
            compiler_params=pltpu.CompilerParams(collective_id=0, has_side_effects=True, vmem_limit_bytes=64 * 1024 * 1024 - 65536),
            name="factor",
        )(pan, trail_tile)
        trail_out, panel_out = pl.pallas_call(
            finish_body,
            grid=(8,),
            out_shape=(jax.ShapeDtypeStruct(trail_tile.shape, f32), jax.ShapeDtypeStruct(panel_tile.shape, f32)),
            in_specs=[
                pl.BlockSpec((1, 1024, 256), lambda b: (b, 0, 0)),
                pl.BlockSpec((1, 512, 256), lambda b: (b, 0, 0)),
                pl.BlockSpec((2, 4, NB, 256), lambda b: (0, 0, 0, 0)),
                pl.BlockSpec((1, 1, 2, NB, 256), lambda b: (b // 4, b % 4, 0, 0, 0)),
                pl.BlockSpec((PAIRS, 192, NB), lambda b: (0, b, 0)),
            ],
            out_specs=(pl.BlockSpec((1536, 256), lambda b: (0, b)), pl.BlockSpec((192, PAIRS, NB), lambda b: (b, 0, 0))),
            compiler_params=pltpu.CompilerParams(vmem_limit_bytes=48 * 1024 * 1024),
            name="finish",
        )(schur, top, left, right, pan_out.reshape(PAIRS, 1536, NB))
        return panel_out, trail_out

    spec_panel = P("pr", "pc", None)
    spec_trail = P("pr", "pc")
    return jax.shard_map(local_part, mesh=mesh, in_specs=(spec_panel, spec_trail), out_specs=(spec_panel, spec_trail), check_vma=False)
```

```python
import jax
import jax.numpy as jnp
from jax import lax
from jax.experimental import pallas as pl
from jax.experimental.pallas import tpu as pltpu
from jax.sharding import PartitionSpec as P

HIGH = lax.Precision.HIGHEST
MESH = pl.DeviceIdType.MESH
NB = 128
PAIRS = 8
LAG = 3
LAST = 2


def dot_nt(a, b):
    return lax.dot_general(a, b, (((1,), (1,)), ((), ())), precision=HIGH, preferred_element_type=jnp.float32)


def dot_nn(a, b):
    return lax.dot_general(a, b, (((1,), (0,)), ((), ())), precision=HIGH, preferred_element_type=jnp.float32)


def lane_of(x, lane):
    return jnp.broadcast_to(x[:, lane:lane + 1], (8, NB))


def row_of(x, row):
    return jnp.broadcast_to(x[row:row + 1, :], (8, NB))


def factor_block(load, store_upper, store_inv, beside=None):
    lane = lax.broadcasted_iota(jnp.int32, (8, NB), 1)
    sub = lax.broadcasted_iota(jnp.int32, (8, NB), 0)
    rows = [load(i) for i in range(16)]
    for g in range(16):
        base = 8 * g
        inside = (lane >= base) & (lane < base + 8)
        cols = [lane_of(rows[g], base + t) for t in range(8)]
        cur = jnp.where(inside, jnp.where(lane - base == sub, 1.0, 0.0), rows[g])
        recips, pivots, cross = [], [], {}
        for s in range(8):
            recip = 1.0 / row_of(cols[s], s)
            pivot = row_of(cur, s)
            mult = jnp.where(sub > s, cols[s] * recip, 0.0)
            for t in range(s + 1, 8):
                cross[t, s] = row_of(cols[t], s)
                cols[t] = cols[t] - mult * cross[t, s]
            if s < 7:
                cur = cur - mult * pivot
            recips.append(recip)
            pivots.append(pivot)
        for i in range(g + 1, 16):
            part = [lane_of(rows[i], base + t) for t in range(8)]
            acc = jnp.where(inside, 0.0, rows[i])
            for s in range(8):
                mult = part[s] * recips[s]
                for t in range(s + 1, 8):
                    part[t] = part[t] - mult * cross[t, s]
                acc = acc - mult * pivots[s]
            rows[i] = acc
        if beside is not None:
            beside(g)
        diag = cols[7]
        upper = jnp.where(lane > base + 7, cur, 0.0)
        for t in range(8):
            if t < 7:
                diag = jnp.where(sub == t, cols[t], diag)
            upper = jnp.where((lane == base + t) & (sub <= t), cols[t], upper)
        scale = lax.rsqrt(diag)
        scale = scale * (1.5 - 0.5 * diag * scale * scale)
        store_upper(g, upper * scale)
        store_inv(g, jnp.where(lane < base + 8, cur, 0.0) * scale)


def body(pan, trail, pan_out, schur_out, top_out, left_out, right_out, work, cols, schur, diag, upper, inv, gmat, top, zero,
         lead_sem, lead_send, lead_recv, own_sem, own_send, own_recv, keep_sem, give_send, give_recv, pass_send,
         far_send, far_recv, in_sem, out_sem, top_sem, left_sem, pan_sem):
    my_row = lax.axis_index("pr")
    my_col = lax.axis_index("pc")
    chip = my_row // 2
    core = my_row % 2
    beside_row = 2 * chip + 1 - core
    along_row = 2 * (1 - chip) + core
    cross_row = 2 * (1 - chip) + 1 - core
    across = {"pr": my_row, "pc": 1 - my_col}
    beside = {"pr": beside_row, "pc": my_col}
    along = {"pr": along_row, "pc": my_col}
    is_giver = core == my_col

    barrier = pltpu.get_barrier_semaphore()
    for peer in (across, beside, along):
        pl.semaphore_signal(barrier, inc=1, device_id=peer, device_id_type=MESH)

    def half(c):
        return pl.ds(pl.multiple_of(c * NB, NB), NB)

    def remote(src, dst, send, recv, peer):
        return pltpu.make_async_remote_copy(src_ref=src, dst_ref=dst, send_sem=send, recv_sem=recv,
                                            device_id=peer, device_id_type=MESH)

    first_part = (0, 0, 1, 0)
    second_part = (0, 1, 4, 1)

    def for_pair(p, fn):
        if isinstance(p, int):
            fn((p, p // 2, 4, p + 1))
        else:
            for first in range(4):
                pl.when(p // 2 == first)(lambda first=first: fn((p, first, 4, p + 1)))

    def strip(part, row, col):
        p, lo, hi, _ = part
        return work.at[p, lo:hi, row, :, half(col)]

    def mine(part):
        p, lo, hi, _ = part
        return pan.at[p, 0, lo:hi]

    def keep_strip(part):
        return pltpu.make_async_copy(mine(part), strip(part, my_row, my_col), lead_sem.at[part[3]])

    def lead_copy(part, kind):
        row, col, peer, slot = {
            0: (my_row, my_col, beside, 0),
            1: (my_row, my_col, along, 1),
            2: (my_row, my_col, across, 2),
            3: (my_row, 1 - my_col, along, 3),
            4: (along_row, my_col, beside, 4),
            5: (my_row, 1 - my_col, beside, 5),
            6: (along_row, 1 - my_col, beside, 6),
            7: (along_row, my_col, across, 3),
        }[kind]
        there = strip(part, row, col)
        return remote(mine(part) if kind < 3 else there, there, lead_send.at[part[3], slot], lead_recv.at[part[3], slot], peer)

    def lead_arrival(part, kind):
        row, col = [(beside_row, my_col), (along_row, my_col), (my_row, 1 - my_col), (along_row, 1 - my_col),
                    (cross_row, my_col), (beside_row, 1 - my_col), (cross_row, 1 - my_col)][kind]
        return remote(mine(part), strip(part, row, col), lead_send.at[part[3], kind], lead_recv.at[part[3], kind], beside)

    def stage_one(part):
        for kind in (1, 2, 0):
            lead_copy(part, kind).start()

    def stage_two(part):
        lead_arrival(part, 1).wait_recv()
        lead_arrival(part, 2).wait_recv()

        @pl.when(core == 0)
        def _():
            lead_copy(part, 3).start()

        @pl.when(core == 1)
        def _():
            lead_copy(part, 7).start()

        lead_copy(part, 4).start()
        lead_copy(part, 5).start()

    def stage_three(part):
        lead_arrival(part, 3).wait_recv()
        lead_copy(part, 6).start()

    def lead_wait(part):
        keep_strip(part).wait()
        for kind in (0, 4, 5, 6):
            lead_arrival(part, kind).wait_recv()
        for kind in range(7):
            lead_copy(part, kind).wait_send()

    def keep_own(p):
        return pltpu.make_async_copy(pan.at[p, 1:3], work.at[p, 4:6, :, :, half(my_col)], own_sem.at[p])

    def own_copy(p):
        return remote(pan.at[p, 1:3], work.at[p, 4:6, :, :, half(my_col)], own_send.at[p], own_recv.at[p], across)

    def own_arrival(p):
        return remote(pan.at[p, 1:3], work.at[p, 4:6, :, :, half(1 - my_col)], own_send.at[p], own_recv.at[p], across)

    def keep_copy(p):
        return pltpu.make_async_copy(work.at[p, 4:6], cols.at[p, :, :, chip], keep_sem.at[p])

    def give_copy(p):
        return remote(work.at[p, 4:6], cols.at[p, :, :, chip], give_send.at[p], give_recv.at[p], beside)

    def far_copy(p):
        return remote(work.at[p, 4:6], cols.at[p, :, :, chip], far_send.at[p], far_recv.at[p], along)

    def far_arrival(p):
        return remote(work.at[p, 4:6], cols.at[p, :, :, 1 - chip], far_send.at[p], far_recv.at[p], along)

    def pass_copy(p):
        return remote(cols.at[p, :, :, 1 - chip], cols.at[p, :, :, 1 - chip], pass_send.at[p], far_recv.at[p], beside)

    def cols_wait(p):
        @pl.when(is_giver)
        def _():
            keep_copy(p).wait()

        @pl.when(jnp.logical_not(is_giver))
        def _():
            give_copy(p).wait_recv()
            far_arrival(p).wait_recv()

    def rows256(p, c):
        return work[p, c // 2, pl.ds(2 * (c % 2), 2)].reshape(256, 256)

    def set_rows256(p, c, value):
        work[p, c // 2, pl.ds(2 * (c % 2), 2)] = value.reshape(2, NB, 256)

    def own_rows(p):
        return work[p, 4:6].reshape(1024, 256)

    def set_own(p, value):
        work[p, 4:6] = value.reshape(2, 4, NB, 256)

    def tile_in(b):
        return pltpu.make_async_copy(trail.at[pl.ds(512, 1024), pl.ds(b * 256, 256)], schur.at[b], in_sem.at[b])

    keep_strip(first_part).start()
    keep_strip(second_part).start()
    for p in range(1, PAIRS):
        for_pair(p, lambda part: keep_strip(part).start())
    zero[...] = jnp.zeros_like(zero)
    gmat[...] = jnp.zeros_like(gmat)
    pl.semaphore_wait(barrier, 3)
    stage_one(first_part)
    stage_two(first_part)
    stage_one(second_part)
    for_pair(1, stage_one)
    stage_three(first_part)
    for p in range(PAIRS):
        keep_own(p).start()
    for b in range(8):
        tile_in(b).start()
    lead_wait(first_part)

    def schur_update(q, b, c):
        where = pl.ds(c * 256, 256)
        right = cols[q, b // 4, b % 4].reshape(256, 256)
        schur[b, where, :] = schur[b, where, :] - dot_nt(rows256(q, 8 + c), right)

    def factor(h, p):
        def store_upper(g, value):
            upper[8 * g:8 * g + 8, :] = value

        def store_inv(g, value):
            inv[h, 8 * g:8 * g + 8, :] = value

        def load(i):
            return diag[8 * i:8 * i + 8, :]

        @pl.when(p < LAG)
        def _():
            factor_block(load, store_upper, store_inv)

        @pl.when(p >= LAG)
        def _():
            factor_block(load, store_upper, store_inv, lambda g: schur_update(p - LAG, 4 * h + g // 4, g % 4))

        work[p, p // 2, 2 * (p % 2) + h, :, half(h)] = upper[...].T

    def lead_step(p):
        @pl.when(p > 0)
        def _():
            for_pair(p, lead_wait)

        def subtract(q, carry):
            right = rows256(q, p)

            def one(c, carry):
                set_rows256(p, c, rows256(p, c) - dot_nt(rows256(q, c), right))
                return carry

            return lax.fori_loop(p, 8, one, carry)

        lax.fori_loop(0, p, subtract, 0)

        @pl.when(p == LAG)
        def _():
            for b in range(8):
                tile_in(b).wait()

        @pl.when(p >= LAG)
        def _():
            cols_wait(p - LAG)

        hi, lo = p // 2, 2 * (p % 2)
        diag[...] = work[p, hi, lo, :, 0:NB]

        def factor_half(h, carry):
            factor(h, p)

            @pl.when(h == 0)
            def _():
                work[p, hi, lo, :, NB:256] = jnp.zeros((NB, NB), jnp.float32)
                low = dot_nt(work[p, hi, lo + 1, :, 0:NB], inv[0])
                work[p, hi, lo + 1, :, 0:NB] = low
                diag[...] = work[p, hi, lo + 1, :, NB:256] - dot_nt(low, low)

            @pl.when((h == 0) & (p == 0))
            def _():
                stage_two(second_part)
                for_pair(2, stage_one)
                for_pair(1, stage_two)

            @pl.when((h == 0) & (p > 0) & (p + 1 < PAIRS))
            def _():
                for_pair(p + 1, stage_two)

            @pl.when((h == 0) & (p + 3 < PAIRS))
            def _():
                for_pair(p + 3, stage_one)

            @pl.when(h == 0)
            def _():
                own_copy(p).start()

            return carry

        lax.fori_loop(0, 2, factor_half, 0)

        @pl.when(p == 0)
        def _():
            stage_three(second_part)

        @pl.when(p + 1 < PAIRS)
        def _():
            for_pair(p + 1, stage_three)

        gmat[p % 2, 0:NB, 0:NB] = inv[0]
        gmat[p % 2, NB:256, NB:256] = inv[1]
        gmat[p % 2, NB:256, 0:NB] = -dot_nn(inv[1], dot_nn(work[p, hi, lo + 1, :, 0:NB], inv[0]))

        @pl.when(p == 0)
        def _():
            lead_wait(second_part)

        def solve(c, carry):
            set_rows256(p, c, dot_nt(rows256(p, c), gmat[p % 2]))
            return carry

        lax.fori_loop(p + 1, 8, solve, 0)

    def own_step(p):
        @pl.when(is_giver & (p > 0))
        def _():
            far_arrival(p - 1).wait_recv()
            pass_copy(p - 1).start()

        keep_own(p).wait()
        own_arrival(p).wait_recv()

        def subtract(q, carry):
            set_own(p, own_rows(p) - dot_nt(own_rows(q), rows256(q, p)))
            return carry

        lax.fori_loop(0, p, subtract, 0)
        set_own(p, dot_nt(own_rows(p), gmat[p % 2]))

        @pl.when(is_giver)
        def _():
            far_copy(p).start()
            keep_copy(p).start()
            give_copy(p).start()

    def chain_step(p, carry):
        @pl.when(p < PAIRS)
        def _():
            lead_step(p)

        @pl.when(p > 0)
        def _():
            own_step(p - 1)

        return carry

    lax.fori_loop(0, PAIRS + 1, chain_step, 0)

    def start_pan(p, carry):
        pltpu.make_async_copy(work.at[p, 4:6, :, :, half(my_col)], pan_out.at[p, 1:3], pan_sem.at[0]).start()
        for r in range(4):
            below = 4 * r + my_row >= 2 * p + my_col

            @pl.when(below)
            def _():
                pltpu.make_async_copy(work.at[p, r, my_row, :, half(my_col)], pan_out.at[p, 0, r], pan_sem.at[0]).start()

            @pl.when(jnp.logical_not(below))
            def _():
                pltpu.make_async_copy(zero, pan_out.at[p, 0, r], pan_sem.at[0]).start()

        return carry

    lax.fori_loop(0, PAIRS, start_pan, 0)

    def left_copy():
        return pltpu.make_async_copy(work.at[PAIRS - LAST:PAIRS, 4:6], left_out, left_sem.at[0])

    def right_copy():
        return pltpu.make_async_copy(cols.at[PAIRS - LAST:PAIRS], right_out, left_sem.at[1])

    def schur_copy(b):
        return pltpu.make_async_copy(schur.at[b], schur_out.at[b], out_sem.at[b])

    def top_copy(b, slot):
        return pltpu.make_async_copy(top.at[slot], top_out.at[b], top_sem.at[slot])

    left_copy().start()

    for q in range(PAIRS - LAG, PAIRS - LAST):
        cols_wait(q)

    def tail(b, carry):
        for q in range(PAIRS - LAG, PAIRS - LAST):
            def one(c, carry, q=q):
                schur_update(q, b, c)
                return carry

            lax.fori_loop(0, 4, one, 0)
        schur_copy(b).start()
        return carry

    lax.fori_loop(0, 8, tail, 0)

    @pl.when(is_giver)
    def _():
        far_arrival(PAIRS - 1).wait_recv()
        pass_copy(PAIRS - 1).start()

    for q in range(PAIRS - LAST, PAIRS):
        cols_wait(q)
    right_copy().start()

    def top_step(b, carry):
        slot = b % 2

        @pl.when(b >= 2)
        def _():
            top_copy(b - 2, slot).wait()

        for r in range(4):
            p = 2 * r + my_row // 2
            side = half(my_row % 2)
            top[slot, r * NB:(r + 1) * NB, :] = dot_nt(work[p, r, my_row, :, side],
                                                       cols[p, b // 4, b % 4, :, :, side].reshape(256, NB))
        top_copy(b, slot).start()
        return carry

    lax.fori_loop(0, 8, top_step, 0)
    top_copy(6, 0).wait()
    top_copy(7, 1).wait()
    for b in range(8):
        schur_copy(b).wait()
    left_copy().wait()
    right_copy().wait()
    pltpu.make_async_copy(pan_out, pan_out, pan_sem.at[0]).wait()

    def finish(p, carry):
        own_copy(p).wait_send()

        @pl.when(is_giver)
        def _():
            give_copy(p).wait_send()
            far_copy(p).wait_send()
            pass_copy(p).wait_send()

        return carry

    lax.fori_loop(0, PAIRS, finish, 0)


def finish_body(schur, top, left, right, pan, trail_out, pan_out):
    trail_out[0:512, :] = top[0]
    for c in range(4):
        where = slice(256 * c, 256 * c + 256)
        total = schur[0, where, :]
        for q in range(LAST):
            rows = left[q, c // 2, 2 * (c % 2):2 * (c % 2) + 2].reshape(256, 256)
            total = total - dot_nt(rows, right[q, 0, 0].reshape(256, 256))
        trail_out[512 + 256 * c:768 + 256 * c, :] = total
    flat = pan_out.reshape(192 * PAIRS, NB)
    for p in range(PAIRS):
        flat[pl.ds(p, 192, stride=PAIRS), :] = pan[p]


def solution(mesh):
    def local_part(panel_tile, trail_tile):
        pan = panel_tile.transpose(1, 0, 2).reshape(PAIRS, 3, 4, NB, NB)
        any_spec = pl.BlockSpec(memory_space=pl.ANY)
        dma = pltpu.SemaphoreType.DMA
        f32 = jnp.float32
        pan_out, schur, top, left, right = pl.pallas_call(
            body,
            out_shape=(jax.ShapeDtypeStruct(pan.shape, f32), jax.ShapeDtypeStruct((8, 1024, 256), f32),
                       jax.ShapeDtypeStruct((8, 512, 256), f32), jax.ShapeDtypeStruct((LAST, 2, 4, NB, 256), f32),
                       jax.ShapeDtypeStruct((LAST, 2, 4, 2, NB, 256), f32)),
            in_specs=[any_spec] * 2,
            out_specs=(any_spec,) * 5,
            scratch_shapes=[
                pltpu.VMEM((PAIRS, 6, 4, NB, 256), jnp.float32),
                pltpu.VMEM((PAIRS, 2, 4, 2, NB, 256), jnp.float32),
                pltpu.VMEM((8, 1024, 256), jnp.float32),
                pltpu.VMEM((NB, NB), jnp.float32),
                pltpu.VMEM((NB, NB), jnp.float32),
                pltpu.VMEM((2, NB, NB), jnp.float32),
                pltpu.VMEM((2, 256, 256), jnp.float32),
                pltpu.VMEM((2, 512, 256), jnp.float32),
                pltpu.VMEM((NB, NB), jnp.float32),
                dma((PAIRS + 1,)), dma((PAIRS + 1, 7)), dma((PAIRS + 1, 7)), dma((PAIRS,)), dma((PAIRS,)), dma((PAIRS,)), dma((PAIRS,)),
                dma((PAIRS,)), dma((PAIRS,)), dma((PAIRS,)), dma((PAIRS,)), dma((PAIRS,)), dma((8,)), dma((8,)), dma((2,)), dma((2,)),
                dma((1,)),
            ],
            compiler_params=pltpu.CompilerParams(collective_id=0, has_side_effects=True, vmem_limit_bytes=64 * 1024 * 1024 - 65536),
            name="factor",
        )(pan, trail_tile)
        trail_out, panel_out = pl.pallas_call(
            finish_body,
            grid=(8,),
            out_shape=(jax.ShapeDtypeStruct(trail_tile.shape, f32), jax.ShapeDtypeStruct(panel_tile.shape, f32)),
            in_specs=[
                pl.BlockSpec((1, 1024, 256), lambda b: (b, 0, 0)),
                pl.BlockSpec((1, 512, 256), lambda b: (b, 0, 0)),
                pl.BlockSpec((LAST, 2, 4, NB, 256), lambda b: (0, 0, 0, 0, 0)),
                pl.BlockSpec((LAST, 1, 1, 2, NB, 256), lambda b: (0, b // 4, b % 4, 0, 0, 0)),
                pl.BlockSpec((PAIRS, 192, NB), lambda b: (0, b, 0)),
            ],
            out_specs=(pl.BlockSpec((1536, 256), lambda b: (0, b)), pl.BlockSpec((192, PAIRS, NB), lambda b: (b, 0, 0))),
            compiler_params=pltpu.CompilerParams(vmem_limit_bytes=64 * 1024 * 1024 - 65536),
            name="finish",
        )(schur, top, left, right, pan_out.reshape(PAIRS, 1536, NB))
        return panel_out, trail_out

    spec_panel = P("pr", "pc", None)
    spec_trail = P("pr", "pc")
    return jax.shard_map(local_part, mesh=mesh, in_specs=(spec_panel, spec_trail), out_specs=(spec_panel, spec_trail), check_vma=False)
```

```python
import jax
import jax.numpy as jnp
from jax import lax
from jax.experimental import pallas as pl
from jax.experimental.pallas import tpu as pltpu
from jax.sharding import PartitionSpec as P

HIGH = lax.Precision.HIGHEST
MESH = pl.DeviceIdType.MESH
NB = 128
PAIRS = 8
LAG = 3
LAST = 2


def dot_nt(a, b):
    return lax.dot_general(a, b, (((1,), (1,)), ((), ())), precision=HIGH, preferred_element_type=jnp.float32)


def dot_nn(a, b):
    return lax.dot_general(a, b, (((1,), (0,)), ((), ())), precision=HIGH, preferred_element_type=jnp.float32)


def lane_of(x, lane):
    return jnp.broadcast_to(x[:, lane:lane + 1], (8, NB))


def row_of(x, row):
    return jnp.broadcast_to(x[row:row + 1, :], (8, NB))


def factor_block(load, store_upper, store_inv, beside=None):
    lane = lax.broadcasted_iota(jnp.int32, (8, NB), 1)
    sub = lax.broadcasted_iota(jnp.int32, (8, NB), 0)
    rows = [load(i) for i in range(16)]
    for g in range(16):
        base = 8 * g
        inside = (lane >= base) & (lane < base + 8)
        cols = [lane_of(rows[g], base + t) for t in range(8)]
        cur = jnp.where(inside, jnp.where(lane - base == sub, 1.0, 0.0), rows[g])
        recips, pivots, cross = [], [], {}
        for s in range(8):
            recip = 1.0 / row_of(cols[s], s)
            pivot = row_of(cur, s)
            mult = jnp.where(sub > s, cols[s] * recip, 0.0)
            for t in range(s + 1, 8):
                cross[t, s] = row_of(cols[t], s)
                cols[t] = cols[t] - mult * cross[t, s]
            if s < 7:
                cur = cur - mult * pivot
            recips.append(recip)
            pivots.append(pivot)
        for i in range(g + 1, 16):
            part = [lane_of(rows[i], base + t) for t in range(8)]
            acc = jnp.where(inside, 0.0, rows[i])
            for s in range(8):
                mult = part[s] * recips[s]
                for t in range(s + 1, 8):
                    part[t] = part[t] - mult * cross[t, s]
                acc = acc - mult * pivots[s]
            rows[i] = acc
        if beside is not None:
            beside(g)
        diag = cols[7]
        upper = jnp.where(lane > base + 7, cur, 0.0)
        for t in range(8):
            if t < 7:
                diag = jnp.where(sub == t, cols[t], diag)
            upper = jnp.where((lane == base + t) & (sub <= t), cols[t], upper)
        scale = lax.rsqrt(diag)
        scale = scale * (1.5 - 0.5 * diag * scale * scale)
        store_upper(g, upper * scale)
        store_inv(g, jnp.where(lane < base + 8, cur, 0.0) * scale)


def body(pan, trail, pan_out, schur_out, top_out, left_out, right_out, work, cols, schur, diag, upper, inv, gmat, top, zero,
         lead_sem, lead_send, lead_recv, own_sem, own_send, own_recv, keep_sem, give_send, give_recv, pass_send,
         far_send, far_recv, in_sem, out_sem, top_sem, left_sem, pan_sem):
    my_row = lax.axis_index("pr")
    my_col = lax.axis_index("pc")
    chip = my_row // 2
    core = my_row % 2
    beside_row = 2 * chip + 1 - core
    along_row = 2 * (1 - chip) + core
    cross_row = 2 * (1 - chip) + 1 - core
    across = {"pr": my_row, "pc": 1 - my_col}
    beside = {"pr": beside_row, "pc": my_col}
    along = {"pr": along_row, "pc": my_col}
    is_giver = core == my_col

    barrier = pltpu.get_barrier_semaphore()
    for peer in (across, beside, along):
        pl.semaphore_signal(barrier, inc=1, device_id=peer, device_id_type=MESH)

    def half(c):
        return pl.ds(pl.multiple_of(c * NB, NB), NB)

    def remote(src, dst, send, recv, peer):
        return pltpu.make_async_remote_copy(src_ref=src, dst_ref=dst, send_sem=send, recv_sem=recv,
                                            device_id=peer, device_id_type=MESH)

    first_part = (0, 0, 1, 0)
    second_part = (0, 1, 4, 1)

    def for_pair(p, fn):
        if isinstance(p, int):
            fn((p, p // 2, 4, p + 1))
        else:
            for first in range(4):
                pl.when(p // 2 == first)(lambda first=first: fn((p, first, 4, p + 1)))

    def strip(part, row, col):
        p, lo, hi, _ = part
        return work.at[p, lo:hi, row, :, half(col)]

    def mine(part):
        p, lo, hi, _ = part
        return pan.at[p, 0, lo:hi]

    def keep_strip(part):
        return pltpu.make_async_copy(mine(part), strip(part, my_row, my_col), lead_sem.at[part[3]])

    def lead_copy(part, kind):
        row, col, peer, slot = {
            0: (my_row, my_col, beside, 0),
            1: (my_row, my_col, along, 1),
            2: (my_row, my_col, across, 2),
            3: (my_row, 1 - my_col, along, 3),
            4: (along_row, my_col, beside, 4),
            5: (my_row, 1 - my_col, beside, 5),
            6: (along_row, 1 - my_col, beside, 6),
            7: (along_row, my_col, across, 3),
        }[kind]
        there = strip(part, row, col)
        return remote(mine(part) if kind < 3 else there, there, lead_send.at[part[3], slot], lead_recv.at[part[3], slot], peer)

    def lead_arrival(part, kind):
        row, col = [(beside_row, my_col), (along_row, my_col), (my_row, 1 - my_col), (along_row, 1 - my_col),
                    (cross_row, my_col), (beside_row, 1 - my_col), (cross_row, 1 - my_col)][kind]
        return remote(mine(part), strip(part, row, col), lead_send.at[part[3], kind], lead_recv.at[part[3], kind], beside)

    def stage_one(part):
        for kind in (1, 2, 0):
            lead_copy(part, kind).start()

    def stage_two(part):
        lead_arrival(part, 1).wait_recv()
        lead_arrival(part, 2).wait_recv()

        @pl.when(core == 0)
        def _():
            lead_copy(part, 3).start()

        @pl.when(core == 1)
        def _():
            lead_copy(part, 7).start()

        lead_copy(part, 4).start()
        lead_copy(part, 5).start()

    def stage_three(part):
        lead_arrival(part, 3).wait_recv()
        lead_copy(part, 6).start()

    def lead_wait(part):
        keep_strip(part).wait()
        for kind in (0, 4, 5, 6):
            lead_arrival(part, kind).wait_recv()
        for kind in range(7):
            lead_copy(part, kind).wait_send()

    def keep_own(p):
        return pltpu.make_async_copy(pan.at[p, 1:3], work.at[p, 4:6, :, :, half(my_col)], own_sem.at[p])

    def own_copy(p):
        return remote(pan.at[p, 1:3], work.at[p, 4:6, :, :, half(my_col)], own_send.at[p], own_recv.at[p], across)

    def own_arrival(p):
        return remote(pan.at[p, 1:3], work.at[p, 4:6, :, :, half(1 - my_col)], own_send.at[p], own_recv.at[p], across)

    def keep_copy(p):
        return pltpu.make_async_copy(work.at[p, 4:6], cols.at[p, :, :, chip], keep_sem.at[p])

    def give_copy(p):
        return remote(work.at[p, 4:6], cols.at[p, :, :, chip], give_send.at[p], give_recv.at[p], beside)

    def far_copy(p):
        return remote(work.at[p, 4:6], cols.at[p, :, :, chip], far_send.at[p], far_recv.at[p], along)

    def far_arrival(p):
        return remote(work.at[p, 4:6], cols.at[p, :, :, 1 - chip], far_send.at[p], far_recv.at[p], along)

    def pass_copy(p):
        return remote(cols.at[p, :, :, 1 - chip], cols.at[p, :, :, 1 - chip], pass_send.at[p], far_recv.at[p], beside)

    def cols_wait(p):
        @pl.when(is_giver)
        def _():
            keep_copy(p).wait()

        @pl.when(jnp.logical_not(is_giver))
        def _():
            give_copy(p).wait_recv()
            far_arrival(p).wait_recv()

    def rows256(p, c):
        return work[p, c // 2, pl.ds(2 * (c % 2), 2)].reshape(256, 256)

    def set_rows256(p, c, value):
        work[p, c // 2, pl.ds(2 * (c % 2), 2)] = value.reshape(2, NB, 256)

    def rows512(p, r):
        return work[p, r].reshape(512, 256)

    def set_rows512(p, r, value):
        work[p, r] = value.reshape(4, NB, 256)

    def own_rows(p):
        return work[p, 4:6].reshape(1024, 256)

    def set_own(p, value):
        work[p, 4:6] = value.reshape(2, 4, NB, 256)

    def tile_in(b):
        return pltpu.make_async_copy(trail.at[pl.ds(512, 1024), pl.ds(b * 256, 256)], schur.at[b], in_sem.at[b])

    keep_strip(first_part).start()
    keep_strip(second_part).start()
    for p in range(1, PAIRS):
        for_pair(p, lambda part: keep_strip(part).start())
    zero[...] = jnp.zeros_like(zero)
    gmat[...] = jnp.zeros_like(gmat)
    pl.semaphore_wait(barrier, 3)
    stage_one(first_part)
    stage_two(first_part)
    stage_one(second_part)
    for_pair(1, stage_one)
    stage_three(first_part)
    for p in range(PAIRS):
        keep_own(p).start()
    for b in range(8):
        tile_in(b).start()
    lead_wait(first_part)

    def schur_update(q, b):
        schur[b] = schur[b] - dot_nt(own_rows(q), cols[q, b // 4, b % 4].reshape(256, 256))

    def factor(h, p):
        def store_upper(g, value):
            upper[8 * g:8 * g + 8, :] = value

        def store_inv(g, value):
            inv[h, 8 * g:8 * g + 8, :] = value

        def load(i):
            return diag[8 * i:8 * i + 8, :]

        @pl.when(p < LAG)
        def _():
            factor_block(load, store_upper, store_inv)

        @pl.when(p >= LAG)
        def _():
            def beside(g):
                if g % 4 == 0:
                    schur_update(p - LAG, 4 * h + g // 4)

            factor_block(load, store_upper, store_inv, beside)

        work[p, p // 2, 2 * (p % 2) + h, :, half(h)] = upper[...].T

    def lead_step(p):
        @pl.when(p > 0)
        def _():
            for_pair(p, lead_wait)

        def subtract(q, carry):
            right = rows256(q, p)

            def one(r, carry):
                set_rows512(p, r, rows512(p, r) - dot_nt(rows512(q, r), right))
                return carry

            return lax.fori_loop(p // 2, 4, one, carry)

        lax.fori_loop(0, p, subtract, 0)

        @pl.when(p == LAG)
        def _():
            for b in range(8):
                tile_in(b).wait()

        @pl.when(p >= LAG)
        def _():
            cols_wait(p - LAG)

        hi, lo = p // 2, 2 * (p % 2)
        diag[...] = work[p, hi, lo, :, 0:NB]

        def factor_half(h, carry):
            factor(h, p)

            @pl.when(h == 0)
            def _():
                work[p, hi, lo, :, NB:256] = jnp.zeros((NB, NB), jnp.float32)
                low = dot_nt(work[p, hi, lo + 1, :, 0:NB], inv[0])
                work[p, hi, lo + 1, :, 0:NB] = low
                diag[...] = work[p, hi, lo + 1, :, NB:256] - dot_nt(low, low)

            @pl.when((h == 0) & (p == 0))
            def _():
                stage_two(second_part)
                for_pair(2, stage_one)
                for_pair(1, stage_two)

            @pl.when((h == 0) & (p > 0) & (p + 1 < PAIRS))
            def _():
                for_pair(p + 1, stage_two)

            @pl.when((h == 0) & (p + 3 < PAIRS))
            def _():
                for_pair(p + 3, stage_one)

            @pl.when(h == 0)
            def _():
                own_copy(p).start()

            return carry

        lax.fori_loop(0, 2, factor_half, 0)

        @pl.when(p == 0)
        def _():
            stage_three(second_part)

        @pl.when(p + 1 < PAIRS)
        def _():
            for_pair(p + 1, stage_three)

        gmat[p % 2, 0:NB, 0:NB] = inv[0]
        gmat[p % 2, NB:256, NB:256] = inv[1]
        gmat[p % 2, NB:256, 0:NB] = -dot_nn(inv[1], dot_nn(work[p, hi, lo + 1, :, 0:NB], inv[0]))

        @pl.when(p == 0)
        def _():
            lead_wait(second_part)

        @pl.when(p % 2 == 0)
        def _():
            set_rows256(p, p + 1, dot_nt(rows256(p, p + 1), gmat[p % 2]))

        def solve(r, carry):
            set_rows512(p, r, dot_nt(rows512(p, r), gmat[p % 2]))
            return carry

        lax.fori_loop(p // 2 + 1, 4, solve, 0)

    def own_step(p):
        @pl.when(is_giver & (p > 0))
        def _():
            far_arrival(p - 1).wait_recv()
            pass_copy(p - 1).start()

        keep_own(p).wait()
        own_arrival(p).wait_recv()

        def subtract(q, carry):
            set_own(p, own_rows(p) - dot_nt(own_rows(q), rows256(q, p)))
            return carry

        lax.fori_loop(0, p, subtract, 0)
        set_own(p, dot_nt(own_rows(p), gmat[p % 2]))

        @pl.when(is_giver)
        def _():
            far_copy(p).start()
            keep_copy(p).start()
            give_copy(p).start()

    def chain_step(p, carry):
        @pl.when(p < PAIRS)
        def _():
            lead_step(p)

        @pl.when(p > 0)
        def _():
            own_step(p - 1)

        return carry

    lax.fori_loop(0, PAIRS + 1, chain_step, 0)

    def start_pan(p, carry):
        pltpu.make_async_copy(work.at[p, 4:6, :, :, half(my_col)], pan_out.at[p, 1:3], pan_sem.at[0]).start()
        for r in range(4):
            below = 4 * r + my_row >= 2 * p + my_col

            @pl.when(below)
            def _():
                pltpu.make_async_copy(work.at[p, r, my_row, :, half(my_col)], pan_out.at[p, 0, r], pan_sem.at[0]).start()

            @pl.when(jnp.logical_not(below))
            def _():
                pltpu.make_async_copy(zero, pan_out.at[p, 0, r], pan_sem.at[0]).start()

        return carry

    lax.fori_loop(0, PAIRS, start_pan, 0)

    def left_copy():
        return pltpu.make_async_copy(work.at[PAIRS - LAST:PAIRS, 4:6], left_out, left_sem.at[0])

    def right_copy():
        return pltpu.make_async_copy(cols.at[PAIRS - LAST:PAIRS], right_out, left_sem.at[1])

    def schur_copy(b):
        return pltpu.make_async_copy(schur.at[b], schur_out.at[b], out_sem.at[b])

    def top_copy(b, slot):
        return pltpu.make_async_copy(top.at[slot], top_out.at[b], top_sem.at[slot])

    left_copy().start()

    for q in range(PAIRS - LAG, PAIRS - LAST):
        cols_wait(q)

    def tail(b, carry):
        for q in range(PAIRS - LAG, PAIRS - LAST):
            schur_update(q, b)
        schur_copy(b).start()
        return carry

    lax.fori_loop(0, 8, tail, 0)

    @pl.when(is_giver)
    def _():
        far_arrival(PAIRS - 1).wait_recv()
        pass_copy(PAIRS - 1).start()

    for q in range(PAIRS - LAST, PAIRS):
        cols_wait(q)
    right_copy().start()

    def top_step(b, carry):
        slot = b % 2

        @pl.when(b >= 2)
        def _():
            top_copy(b - 2, slot).wait()

        for r in range(4):
            p = 2 * r + my_row // 2
            side = half(my_row % 2)
            top[slot, r * NB:(r + 1) * NB, :] = dot_nt(work[p, r, my_row, :, side],
                                                       cols[p, b // 4, b % 4, :, :, side].reshape(256, NB))
        top_copy(b, slot).start()
        return carry

    lax.fori_loop(0, 8, top_step, 0)
    top_copy(6, 0).wait()
    top_copy(7, 1).wait()
    for b in range(8):
        schur_copy(b).wait()
    left_copy().wait()
    right_copy().wait()
    pltpu.make_async_copy(pan_out, pan_out, pan_sem.at[0]).wait()

    def finish(p, carry):
        own_copy(p).wait_send()

        @pl.when(is_giver)
        def _():
            give_copy(p).wait_send()
            far_copy(p).wait_send()
            pass_copy(p).wait_send()

        return carry

    lax.fori_loop(0, PAIRS, finish, 0)


def finish_body(schur, top, left, right, pan, trail_out, pan_out):
    trail_out[0:512, :] = top[0]
    total = schur[0]
    for q in range(LAST):
        total = total - dot_nt(left[q].reshape(1024, 256), right[q, 0, 0].reshape(256, 256))
    trail_out[512:1536, :] = total
    flat = pan_out.reshape(192 * PAIRS, NB)
    for p in range(PAIRS):
        flat[pl.ds(p, 192, stride=PAIRS), :] = pan[p]


def solution(mesh):
    def local_part(panel_tile, trail_tile):
        pan = panel_tile.transpose(1, 0, 2).reshape(PAIRS, 3, 4, NB, NB)
        any_spec = pl.BlockSpec(memory_space=pl.ANY)
        dma = pltpu.SemaphoreType.DMA
        f32 = jnp.float32
        pan_out, schur, top, left, right = pl.pallas_call(
            body,
            out_shape=(jax.ShapeDtypeStruct(pan.shape, f32), jax.ShapeDtypeStruct((8, 1024, 256), f32),
                       jax.ShapeDtypeStruct((8, 512, 256), f32), jax.ShapeDtypeStruct((LAST, 2, 4, NB, 256), f32),
                       jax.ShapeDtypeStruct((LAST, 2, 4, 2, NB, 256), f32)),
            in_specs=[any_spec] * 2,
            out_specs=(any_spec,) * 5,
            scratch_shapes=[
                pltpu.VMEM((PAIRS, 6, 4, NB, 256), jnp.float32),
                pltpu.VMEM((PAIRS, 2, 4, 2, NB, 256), jnp.float32),
                pltpu.VMEM((8, 1024, 256), jnp.float32),
                pltpu.VMEM((NB, NB), jnp.float32),
                pltpu.VMEM((NB, NB), jnp.float32),
                pltpu.VMEM((2, NB, NB), jnp.float32),
                pltpu.VMEM((2, 256, 256), jnp.float32),
                pltpu.VMEM((2, 512, 256), jnp.float32),
                pltpu.VMEM((NB, NB), jnp.float32),
                dma((PAIRS + 1,)), dma((PAIRS + 1, 7)), dma((PAIRS + 1, 7)), dma((PAIRS,)), dma((PAIRS,)), dma((PAIRS,)), dma((PAIRS,)),
                dma((PAIRS,)), dma((PAIRS,)), dma((PAIRS,)), dma((PAIRS,)), dma((PAIRS,)), dma((8,)), dma((8,)), dma((2,)), dma((2,)),
                dma((1,)),
            ],
            compiler_params=pltpu.CompilerParams(collective_id=0, has_side_effects=True, vmem_limit_bytes=64 * 1024 * 1024 - 65536),
            name="factor",
        )(pan, trail_tile)
        trail_out, panel_out = pl.pallas_call(
            finish_body,
            grid=(8,),
            out_shape=(jax.ShapeDtypeStruct(trail_tile.shape, f32), jax.ShapeDtypeStruct(panel_tile.shape, f32)),
            in_specs=[
                pl.BlockSpec((1, 1024, 256), lambda b: (b, 0, 0)),
                pl.BlockSpec((1, 512, 256), lambda b: (b, 0, 0)),
                pl.BlockSpec((LAST, 2, 4, NB, 256), lambda b: (0, 0, 0, 0, 0)),
                pl.BlockSpec((LAST, 1, 1, 2, NB, 256), lambda b: (0, b // 4, b % 4, 0, 0, 0)),
                pl.BlockSpec((PAIRS, 192, NB), lambda b: (0, b, 0)),
            ],
            out_specs=(pl.BlockSpec((1536, 256), lambda b: (0, b)), pl.BlockSpec((192, PAIRS, NB), lambda b: (b, 0, 0))),
            compiler_params=pltpu.CompilerParams(vmem_limit_bytes=64 * 1024 * 1024 - 65536),
            name="finish",
        )(schur, top, left, right, pan_out.reshape(PAIRS, 1536, NB))
        return panel_out, trail_out

    spec_panel = P("pr", "pc", None)
    spec_trail = P("pr", "pc")
    return jax.shard_map(local_part, mesh=mesh, in_specs=(spec_panel, spec_trail), out_specs=(spec_panel, spec_trail), check_vma=False)
```

```python
import jax
import jax.numpy as jnp
from jax import lax
from jax.experimental import pallas as pl
from jax.experimental.pallas import tpu as pltpu
from jax.sharding import PartitionSpec as P

HIGH = lax.Precision.HIGHEST
MESH = pl.DeviceIdType.MESH
NB = 128
PAIRS = 8
LAG = 3
LAST = 2


def dot_nt(a, b):
    return lax.dot_general(a, b, (((1,), (1,)), ((), ())), precision=HIGH, preferred_element_type=jnp.float32)


def dot_nn(a, b):
    return lax.dot_general(a, b, (((1,), (0,)), ((), ())), precision=HIGH, preferred_element_type=jnp.float32)


def lane_of(x, lane):
    return jnp.broadcast_to(x[:, lane:lane + 1], (8, NB))


def row_of(x, row):
    return jnp.broadcast_to(x[row:row + 1, :], (8, NB))


def factor_block(load, store_upper, store_inv, beside=None):
    lane = lax.broadcasted_iota(jnp.int32, (8, NB), 1)
    sub = lax.broadcasted_iota(jnp.int32, (8, NB), 0)
    rows = [load(i) for i in range(16)]
    for g in range(16):
        base = 8 * g
        inside = (lane >= base) & (lane < base + 8)
        cols = [jnp.where(sub < 8, lane_of(rows[g], base + t), 0.0) for t in range(8)]
        cur = jnp.where(inside, jnp.where(lane - base == sub, 1.0, 0.0), rows[g])
        recips, pivots, cross = [], [], {}
        for s in range(8):
            recip = 1.0 / row_of(cols[s], s)
            pivot = row_of(cur, s)
            mult = jnp.where(sub > s, cols[s] * recip, 0.0)
            for t in range(s + 1, 8):
                cross[t, s] = row_of(cols[t], s)
                cols[t] = cols[t] - mult * cross[t, s]
            if s < 7:
                cur = cur - mult * pivot
            recips.append(recip)
            pivots.append(pivot)
        for i in range(g + 1, 16):
            part = [lane_of(rows[i], base + t) for t in range(8)]
            acc = jnp.where(inside, 0.0, rows[i])
            for s in range(8):
                mult = part[s] * recips[s]
                for t in range(s + 1, 8):
                    part[t] = part[t] - mult * cross[t, s]
                acc = acc - mult * pivots[s]
            rows[i] = acc
        if beside is not None:
            beside(g)
        diag = cols[7]
        upper = jnp.where(lane > base + 7, cur, 0.0)
        for t in range(8):
            if t < 7:
                diag = jnp.where(sub == t, cols[t], diag)
            upper = jnp.where((lane == base + t) & (sub <= t), cols[t], upper)
        scale = lax.rsqrt(diag)
        scale = scale * (1.5 - 0.5 * diag * scale * scale)
        store_upper(g, upper * scale)
        store_inv(g, jnp.where(lane < base + 8, cur, 0.0) * scale)


def body(pan, trail, pan_out, schur_out, top_out, left_out, right_out, work, cols, schur, diag, upper, inv, gmat, top, zero,
         lead_sem, lead_send, lead_recv, own_sem, own_send, own_recv, keep_sem, give_send, give_recv, pass_send,
         far_send, far_recv, in_sem, out_sem, top_sem, left_sem, pan_sem):
    my_row = lax.axis_index("pr")
    my_col = lax.axis_index("pc")
    chip = my_row // 2
    core = my_row % 2
    beside_row = 2 * chip + 1 - core
    along_row = 2 * (1 - chip) + core
    cross_row = 2 * (1 - chip) + 1 - core
    across = {"pr": my_row, "pc": 1 - my_col}
    beside = {"pr": beside_row, "pc": my_col}
    along = {"pr": along_row, "pc": my_col}
    is_giver = core == my_col

    barrier = pltpu.get_barrier_semaphore()
    for peer in (across, beside, along):
        pl.semaphore_signal(barrier, inc=1, device_id=peer, device_id_type=MESH)

    def half(c):
        return pl.ds(pl.multiple_of(c * NB, NB), NB)

    def remote(src, dst, send, recv, peer):
        return pltpu.make_async_remote_copy(src_ref=src, dst_ref=dst, send_sem=send, recv_sem=recv,
                                            device_id=peer, device_id_type=MESH)

    first_part = (0, 0, 1, 0)
    second_part = (0, 1, 4, 1)

    def for_pair(p, fn):
        if isinstance(p, int):
            fn((p, p // 2, 4, p + 1))
        else:
            for first in range(4):
                pl.when(p // 2 == first)(lambda first=first: fn((p, first, 4, p + 1)))

    def strip(part, row, col):
        p, lo, hi, _ = part
        return work.at[p, lo:hi, row, :, half(col)]

    def mine(part):
        p, lo, hi, _ = part
        return pan.at[p, 0, lo:hi]

    def keep_strip(part):
        return pltpu.make_async_copy(mine(part), strip(part, my_row, my_col), lead_sem.at[part[3]])

    def lead_copy(part, kind):
        row, col, peer, slot = {
            0: (my_row, my_col, beside, 0),
            1: (my_row, my_col, along, 1),
            2: (my_row, my_col, across, 2),
            3: (my_row, 1 - my_col, along, 3),
            4: (along_row, my_col, beside, 4),
            5: (my_row, 1 - my_col, beside, 5),
            6: (along_row, 1 - my_col, beside, 6),
            7: (along_row, my_col, across, 3),
        }[kind]
        there = strip(part, row, col)
        return remote(mine(part) if kind < 3 else there, there, lead_send.at[part[3], slot], lead_recv.at[part[3], slot], peer)

    def lead_arrival(part, kind):
        row, col = [(beside_row, my_col), (along_row, my_col), (my_row, 1 - my_col), (along_row, 1 - my_col),
                    (cross_row, my_col), (beside_row, 1 - my_col), (cross_row, 1 - my_col)][kind]
        return remote(mine(part), strip(part, row, col), lead_send.at[part[3], kind], lead_recv.at[part[3], kind], beside)

    def stage_one(part):
        for kind in (1, 2, 0):
            lead_copy(part, kind).start()

    def stage_two(part):
        lead_arrival(part, 1).wait_recv()
        lead_arrival(part, 2).wait_recv()

        @pl.when(core == 0)
        def _():
            lead_copy(part, 3).start()

        @pl.when(core == 1)
        def _():
            lead_copy(part, 7).start()

        lead_copy(part, 4).start()
        lead_copy(part, 5).start()

    def stage_three(part):
        lead_arrival(part, 3).wait_recv()
        lead_copy(part, 6).start()

    def lead_wait(part):
        keep_strip(part).wait()
        for kind in (0, 4, 5, 6):
            lead_arrival(part, kind).wait_recv()
        for kind in range(7):
            lead_copy(part, kind).wait_send()

    def keep_own(p):
        return pltpu.make_async_copy(pan.at[p, 1:3], work.at[p, 4:6, :, :, half(my_col)], own_sem.at[p])

    def own_copy(p):
        return remote(pan.at[p, 1:3], work.at[p, 4:6, :, :, half(my_col)], own_send.at[p], own_recv.at[p], across)

    def own_arrival(p):
        return remote(pan.at[p, 1:3], work.at[p, 4:6, :, :, half(1 - my_col)], own_send.at[p], own_recv.at[p], across)

    def keep_copy(p):
        return pltpu.make_async_copy(work.at[p, 4:6], cols.at[p, :, :, chip], keep_sem.at[p])

    def give_copy(p):
        return remote(work.at[p, 4:6], cols.at[p, :, :, chip], give_send.at[p], give_recv.at[p], beside)

    def far_copy(p):
        return remote(work.at[p, 4:6], cols.at[p, :, :, chip], far_send.at[p], far_recv.at[p], along)

    def far_arrival(p):
        return remote(work.at[p, 4:6], cols.at[p, :, :, 1 - chip], far_send.at[p], far_recv.at[p], along)

    def pass_copy(p):
        return remote(cols.at[p, :, :, 1 - chip], cols.at[p, :, :, 1 - chip], pass_send.at[p], far_recv.at[p], beside)

    def cols_wait(p):
        @pl.when(is_giver)
        def _():
            keep_copy(p).wait()

        @pl.when(jnp.logical_not(is_giver))
        def _():
            give_copy(p).wait_recv()
            far_arrival(p).wait_recv()

    def rows256(p, c):
        return work[p, c // 2, pl.ds(2 * (c % 2), 2)].reshape(256, 256)

    def set_rows256(p, c, value):
        work[p, c // 2, pl.ds(2 * (c % 2), 2)] = value.reshape(2, NB, 256)

    def rows512(p, r):
        return work[p, r].reshape(512, 256)

    def set_rows512(p, r, value):
        work[p, r] = value.reshape(4, NB, 256)

    def own_rows(p):
        return work[p, 4:6].reshape(1024, 256)

    def set_own(p, value):
        work[p, 4:6] = value.reshape(2, 4, NB, 256)

    def tile_in(b):
        return pltpu.make_async_copy(trail.at[pl.ds(512, 1024), pl.ds(b * 256, 256)], schur.at[b], in_sem.at[b])

    keep_strip(first_part).start()
    keep_strip(second_part).start()
    for p in range(1, PAIRS):
        for_pair(p, lambda part: keep_strip(part).start())
    zero[...] = jnp.zeros_like(zero)
    gmat[...] = jnp.zeros_like(gmat)
    pl.semaphore_wait(barrier, 3)
    stage_one(first_part)
    stage_two(first_part)
    stage_one(second_part)
    for_pair(1, stage_one)
    stage_three(first_part)
    for p in range(PAIRS):
        keep_own(p).start()
    for b in range(8):
        tile_in(b).start()
    lead_wait(first_part)

    def schur_update(q, b):
        schur[b] = schur[b] - dot_nt(own_rows(q), cols[q, b // 4, b % 4].reshape(256, 256))

    def factor(h, p):
        def store_upper(g, value):
            upper[8 * g:8 * g + 8, :] = value

        def store_inv(g, value):
            inv[h, 8 * g:8 * g + 8, :] = value

        def load(i):
            return diag[8 * i:8 * i + 8, :]

        @pl.when(p < LAG)
        def _():
            factor_block(load, store_upper, store_inv)

        @pl.when(p >= LAG)
        def _():
            def beside(g):
                if g % 4 == 0:
                    schur_update(p - LAG, 4 * h + g // 4)

            factor_block(load, store_upper, store_inv, beside)

        work[p, p // 2, 2 * (p % 2) + h, :, half(h)] = upper[...].T

    def lead_step(p):
        @pl.when(p > 0)
        def _():
            for_pair(p, lead_wait)

        def subtract(q, carry):
            right = rows256(q, p)

            def one(r, carry):
                set_rows512(p, r, rows512(p, r) - dot_nt(rows512(q, r), right))
                return carry

            return lax.fori_loop(p // 2, 4, one, carry)

        lax.fori_loop(0, p, subtract, 0)

        @pl.when(p == LAG)
        def _():
            for b in range(8):
                tile_in(b).wait()

        @pl.when(p >= LAG)
        def _():
            cols_wait(p - LAG)

        hi, lo = p // 2, 2 * (p % 2)
        diag[...] = work[p, hi, lo, :, 0:NB]

        def factor_half(h, carry):
            factor(h, p)

            @pl.when(h == 0)
            def _():
                work[p, hi, lo, :, NB:256] = jnp.zeros((NB, NB), jnp.float32)
                low = dot_nt(work[p, hi, lo + 1, :, 0:NB], inv[0])
                work[p, hi, lo + 1, :, 0:NB] = low
                diag[...] = work[p, hi, lo + 1, :, NB:256] - dot_nt(low, low)

            @pl.when((h == 0) & (p == 0))
            def _():
                stage_two(second_part)
                for_pair(2, stage_one)
                for_pair(1, stage_two)

            @pl.when((h == 0) & (p > 0) & (p + 1 < PAIRS))
            def _():
                for_pair(p + 1, stage_two)

            @pl.when((h == 0) & (p + 3 < PAIRS))
            def _():
                for_pair(p + 3, stage_one)

            @pl.when(h == 0)
            def _():
                own_copy(p).start()

            return carry

        lax.fori_loop(0, 2, factor_half, 0)

        @pl.when(p == 0)
        def _():
            stage_three(second_part)

        @pl.when(p + 1 < PAIRS)
        def _():
            for_pair(p + 1, stage_three)

        gmat[p % 2, 0:NB, 0:NB] = inv[0]
        gmat[p % 2, NB:256, NB:256] = inv[1]
        gmat[p % 2, NB:256, 0:NB] = -dot_nn(inv[1], dot_nn(work[p, hi, lo + 1, :, 0:NB], inv[0]))

        @pl.when(p == 0)
        def _():
            lead_wait(second_part)

        @pl.when(p % 2 == 0)
        def _():
            set_rows256(p, p + 1, dot_nt(rows256(p, p + 1), gmat[p % 2]))

        def solve(r, carry):
            set_rows512(p, r, dot_nt(rows512(p, r), gmat[p % 2]))
            return carry

        lax.fori_loop(p // 2 + 1, 4, solve, 0)

    def own_step(p):
        @pl.when(is_giver & (p > 0))
        def _():
            far_arrival(p - 1).wait_recv()
            pass_copy(p - 1).start()

        keep_own(p).wait()
        own_arrival(p).wait_recv()

        def subtract(q, carry):
            set_own(p, own_rows(p) - dot_nt(own_rows(q), rows256(q, p)))
            return carry

        lax.fori_loop(0, p, subtract, 0)
        set_own(p, dot_nt(own_rows(p), gmat[p % 2]))

        @pl.when(is_giver)
        def _():
            far_copy(p).start()
            keep_copy(p).start()
            give_copy(p).start()

    def chain_step(p, carry):
        @pl.when(p < PAIRS)
        def _():
            lead_step(p)

        @pl.when(p > 0)
        def _():
            own_step(p - 1)

        return carry

    lax.fori_loop(0, PAIRS + 1, chain_step, 0)

    def start_pan(p, carry):
        pltpu.make_async_copy(work.at[p, 4:6, :, :, half(my_col)], pan_out.at[p, 1:3], pan_sem.at[0]).start()
        for r in range(4):
            below = 4 * r + my_row >= 2 * p + my_col

            @pl.when(below)
            def _():
                pltpu.make_async_copy(work.at[p, r, my_row, :, half(my_col)], pan_out.at[p, 0, r], pan_sem.at[0]).start()

            @pl.when(jnp.logical_not(below))
            def _():
                pltpu.make_async_copy(zero, pan_out.at[p, 0, r], pan_sem.at[0]).start()

        return carry

    lax.fori_loop(0, PAIRS, start_pan, 0)

    def left_copy():
        return pltpu.make_async_copy(work.at[PAIRS - LAST:PAIRS, 4:6], left_out, left_sem.at[0])

    def right_copy():
        return pltpu.make_async_copy(cols.at[PAIRS - LAST:PAIRS], right_out, left_sem.at[1])

    def schur_copy(b):
        return pltpu.make_async_copy(schur.at[b], schur_out.at[b], out_sem.at[b])

    def top_copy(r):
        return pltpu.make_async_copy(top.at[r % 2], top_out.at[r], top_sem.at[r % 2])

    def top_rows(r):
        if r >= 2:
            top_copy(r - 2).wait()
        p = 2 * r + my_row // 2
        side = half(my_row % 2)

        def one(b, carry):
            top[r % 2, b] = dot_nt(work[p, r, my_row, :, side], cols[p, b // 4, b % 4, :, :, side].reshape(256, NB))
            return carry

        lax.fori_loop(0, 8, one, 0)
        top_copy(r).start()

    left_copy().start()

    for q in range(PAIRS - LAG, PAIRS - LAST):
        cols_wait(q)

    def tail(b, carry):
        for q in range(PAIRS - LAG, PAIRS - LAST):
            schur_update(q, b)
        schur_copy(b).start()
        return carry

    lax.fori_loop(0, 8, tail, 0)

    for r in range(3):
        top_rows(r)

    @pl.when(is_giver)
    def _():
        far_arrival(PAIRS - 1).wait_recv()
        pass_copy(PAIRS - 1).start()

    for q in range(PAIRS - LAST, PAIRS):
        cols_wait(q)
    right_copy().start()
    top_rows(3)
    top_copy(2).wait()
    top_copy(3).wait()
    for b in range(8):
        schur_copy(b).wait()
    left_copy().wait()
    right_copy().wait()
    pltpu.make_async_copy(pan_out, pan_out, pan_sem.at[0]).wait()

    def finish(p, carry):
        own_copy(p).wait_send()

        @pl.when(is_giver)
        def _():
            give_copy(p).wait_send()
            far_copy(p).wait_send()
            pass_copy(p).wait_send()

        return carry

    lax.fori_loop(0, PAIRS, finish, 0)


def finish_body(schur, top, left, right, pan, trail_out, pan_out):
    trail_out[0:512, :] = top[...].reshape(512, 256)
    total = schur[0]
    for q in range(LAST):
        total = total - dot_nt(left[q].reshape(1024, 256), right[q, 0, 0].reshape(256, 256))
    trail_out[512:1536, :] = total
    flat = pan_out.reshape(192 * PAIRS, NB)
    for p in range(PAIRS):
        flat[pl.ds(p, 192, stride=PAIRS), :] = pan[p]


def solution(mesh):
    def local_part(panel_tile, trail_tile):
        pan = panel_tile.transpose(1, 0, 2).reshape(PAIRS, 3, 4, NB, NB)
        any_spec = pl.BlockSpec(memory_space=pl.ANY)
        dma = pltpu.SemaphoreType.DMA
        f32 = jnp.float32
        pan_out, schur, top, left, right = pl.pallas_call(
            body,
            out_shape=(jax.ShapeDtypeStruct(pan.shape, f32), jax.ShapeDtypeStruct((8, 1024, 256), f32),
                       jax.ShapeDtypeStruct((4, 8, NB, 256), f32), jax.ShapeDtypeStruct((LAST, 2, 4, NB, 256), f32),
                       jax.ShapeDtypeStruct((LAST, 2, 4, 2, NB, 256), f32)),
            in_specs=[any_spec] * 2,
            out_specs=(any_spec,) * 5,
            scratch_shapes=[
                pltpu.VMEM((PAIRS, 6, 4, NB, 256), jnp.float32),
                pltpu.VMEM((PAIRS, 2, 4, 2, NB, 256), jnp.float32),
                pltpu.VMEM((8, 1024, 256), jnp.float32),
                pltpu.VMEM((NB, NB), jnp.float32),
                pltpu.VMEM((NB, NB), jnp.float32),
                pltpu.VMEM((2, NB, NB), jnp.float32),
                pltpu.VMEM((2, 256, 256), jnp.float32),
                pltpu.VMEM((2, 8, NB, 256), jnp.float32),
                pltpu.VMEM((NB, NB), jnp.float32),
                dma((PAIRS + 1,)), dma((PAIRS + 1, 7)), dma((PAIRS + 1, 7)), dma((PAIRS,)), dma((PAIRS,)), dma((PAIRS,)), dma((PAIRS,)),
                dma((PAIRS,)), dma((PAIRS,)), dma((PAIRS,)), dma((PAIRS,)), dma((PAIRS,)), dma((8,)), dma((8,)), dma((2,)), dma((2,)),
                dma((1,)),
            ],
            compiler_params=pltpu.CompilerParams(collective_id=0, has_side_effects=True, vmem_limit_bytes=64 * 1024 * 1024 - 65536),
            name="factor",
        )(pan, trail_tile)
        trail_out, panel_out = pl.pallas_call(
            finish_body,
            grid=(8,),
            out_shape=(jax.ShapeDtypeStruct(trail_tile.shape, f32), jax.ShapeDtypeStruct(panel_tile.shape, f32)),
            in_specs=[
                pl.BlockSpec((1, 1024, 256), lambda b: (b, 0, 0)),
                pl.BlockSpec((4, 1, NB, 256), lambda b: (0, b, 0, 0)),
                pl.BlockSpec((LAST, 2, 4, NB, 256), lambda b: (0, 0, 0, 0, 0)),
                pl.BlockSpec((LAST, 1, 1, 2, NB, 256), lambda b: (0, b // 4, b % 4, 0, 0, 0)),
                pl.BlockSpec((PAIRS, 192, NB), lambda b: (0, b, 0)),
            ],
            out_specs=(pl.BlockSpec((1536, 256), lambda b: (0, b)), pl.BlockSpec((192, PAIRS, NB), lambda b: (b, 0, 0))),
            compiler_params=pltpu.CompilerParams(vmem_limit_bytes=64 * 1024 * 1024 - 65536),
            name="finish",
        )(schur, top, left, right, pan_out.reshape(PAIRS, 1536, NB))
        return panel_out, trail_out

    spec_panel = P("pr", "pc", None)
    spec_trail = P("pr", "pc")
    return jax.shard_map(local_part, mesh=mesh, in_specs=(spec_panel, spec_trail), out_specs=(spec_panel, spec_trail), check_vma=False)
```

```python
import jax
import jax.numpy as jnp
from jax import lax
from jax.experimental import pallas as pl
from jax.experimental.pallas import tpu as pltpu
from jax.sharding import PartitionSpec as P

HIGH = lax.Precision.HIGHEST
MESH = pl.DeviceIdType.MESH
NB = 128
PAIRS = 8
LAG = 3
LAST = 2


def dot_nt(a, b):
    return lax.dot_general(a, b, (((1,), (1,)), ((), ())), precision=HIGH, preferred_element_type=jnp.float32)


def dot_nn(a, b):
    return lax.dot_general(a, b, (((1,), (0,)), ((), ())), precision=HIGH, preferred_element_type=jnp.float32)


def lane_of(x, lane):
    return jnp.broadcast_to(x[:, lane:lane + 1], (8, NB))


def row_of(x, row):
    return jnp.broadcast_to(x[row:row + 1, :], (8, NB))


def factor_block(load, store_upper, store_inv, beside=None):
    lane = lax.broadcasted_iota(jnp.int32, (8, NB), 1)
    sub = lax.broadcasted_iota(jnp.int32, (8, NB), 0)
    rows = [load(i) for i in range(16)]
    for g in range(16):
        base = 8 * g
        inside = (lane >= base) & (lane < base + 8)
        cols = [jnp.where(sub < 8, lane_of(rows[g], base + t), 0.0) for t in range(8)]
        cur = jnp.where(inside, jnp.where(lane - base == sub, 1.0, 0.0), rows[g])
        recips, pivots, cross = [], [], {}
        for s in range(8):
            recip = 1.0 / row_of(cols[s], s)
            pivot = row_of(cur, s)
            mult = jnp.where(sub > s, cols[s] * recip, 0.0)
            for t in range(s + 1, 8):
                cross[t, s] = row_of(cols[t], s)
                cols[t] = cols[t] - mult * cross[t, s]
            if s < 7:
                cur = cur - mult * pivot
            recips.append(recip)
            pivots.append(pivot)
        for i in range(g + 1, 16):
            part = [lane_of(rows[i], base + t) for t in range(8)]
            acc = jnp.where(inside, 0.0, rows[i])
            for s in range(8):
                mult = part[s] * recips[s]
                for t in range(s + 1, 8):
                    part[t] = part[t] - mult * cross[t, s]
                acc = acc - mult * pivots[s]
            rows[i] = acc
        if beside is not None:
            beside(g)
        diag = cols[7]
        upper = jnp.where(lane > base + 7, cur, 0.0)
        for t in range(8):
            if t < 7:
                diag = jnp.where(sub == t, cols[t], diag)
            upper = jnp.where((lane == base + t) & (sub <= t), cols[t], upper)
        scale = lax.rsqrt(diag)
        scale = scale * (1.5 - 0.5 * diag * scale * scale)
        store_upper(g, upper * scale)
        store_inv(g, jnp.where(lane < base + 8, cur, 0.0) * scale)


def body(pan, trail, pan_out, schur_out, top_out, left_out, right_out, work, cols, schur, diag, upper, inv, gmat, top, zero,
         lead_sem, lead_send, lead_recv, own_sem, own_send, own_recv, keep_sem, give_send, give_recv, pass_send,
         far_send, far_recv, in_sem, out_sem, top_sem, left_sem, pan_sem):
    my_row = lax.axis_index("pr")
    my_col = lax.axis_index("pc")
    chip = my_row // 2
    core = my_row % 2
    beside_row = 2 * chip + 1 - core
    along_row = 2 * (1 - chip) + core
    cross_row = 2 * (1 - chip) + 1 - core
    across = {"pr": my_row, "pc": 1 - my_col}
    beside = {"pr": beside_row, "pc": my_col}
    along = {"pr": along_row, "pc": my_col}
    is_giver = core == my_col

    barrier = pltpu.get_barrier_semaphore()
    for peer in (across, beside, along):
        pl.semaphore_signal(barrier, inc=1, device_id=peer, device_id_type=MESH)

    def half(c):
        return pl.ds(pl.multiple_of(c * NB, NB), NB)

    def remote(src, dst, send, recv, peer):
        return pltpu.make_async_remote_copy(src_ref=src, dst_ref=dst, send_sem=send, recv_sem=recv,
                                            device_id=peer, device_id_type=MESH)

    first_part = (0, 0, 1, 0)
    second_part = (0, 1, 4, 1)

    def for_pair(p, fn):
        if isinstance(p, int):
            fn((p, p // 2, 4, p + 1))
        else:
            for first in range(4):
                pl.when(p // 2 == first)(lambda first=first: fn((p, first, 4, p + 1)))

    def strip(part, row, col):
        p, lo, hi, _ = part
        return work.at[p, lo:hi, row, :, half(col)]

    def mine(part):
        p, lo, hi, _ = part
        return pan.at[p, 0, lo:hi]

    def keep_strip(part):
        return pltpu.make_async_copy(mine(part), strip(part, my_row, my_col), lead_sem.at[part[3]])

    def lead_copy(part, kind):
        row, col, peer, slot = {
            0: (my_row, my_col, beside, 0),
            1: (my_row, my_col, along, 1),
            2: (my_row, my_col, across, 2),
            3: (my_row, 1 - my_col, along, 3),
            4: (along_row, my_col, beside, 4),
            5: (my_row, 1 - my_col, beside, 5),
            6: (along_row, 1 - my_col, beside, 6),
            7: (along_row, my_col, across, 3),
        }[kind]
        there = strip(part, row, col)
        return remote(mine(part) if kind < 3 else there, there, lead_send.at[part[3], slot], lead_recv.at[part[3], slot], peer)

    def lead_arrival(part, kind):
        row, col = [(beside_row, my_col), (along_row, my_col), (my_row, 1 - my_col), (along_row, 1 - my_col),
                    (cross_row, my_col), (beside_row, 1 - my_col), (cross_row, 1 - my_col)][kind]
        return remote(mine(part), strip(part, row, col), lead_send.at[part[3], kind], lead_recv.at[part[3], kind], beside)

    def stage_one(part):
        for kind in (1, 2, 0):
            lead_copy(part, kind).start()

    def stage_two(part):
        lead_arrival(part, 1).wait_recv()
        lead_arrival(part, 2).wait_recv()

        @pl.when(core == 0)
        def _():
            lead_copy(part, 3).start()

        @pl.when(core == 1)
        def _():
            lead_copy(part, 7).start()

        lead_copy(part, 4).start()
        lead_copy(part, 5).start()

    def stage_three(part):
        lead_arrival(part, 3).wait_recv()
        lead_copy(part, 6).start()

    def lead_wait(part):
        keep_strip(part).wait()
        for kind in (0, 4, 5, 6):
            lead_arrival(part, kind).wait_recv()
        for kind in range(7):
            lead_copy(part, kind).wait_send()

    def keep_own(p):
        return pltpu.make_async_copy(pan.at[p, 1:3], work.at[p, 4:6, :, :, half(my_col)], own_sem.at[p])

    def own_copy(p):
        return remote(pan.at[p, 1:3], work.at[p, 4:6, :, :, half(my_col)], own_send.at[p], own_recv.at[p], across)

    def own_arrival(p):
        return remote(pan.at[p, 1:3], work.at[p, 4:6, :, :, half(1 - my_col)], own_send.at[p], own_recv.at[p], across)

    def keep_copy(p):
        return pltpu.make_async_copy(work.at[p, 4:6], cols.at[p, :, :, chip], keep_sem.at[p])

    def give_copy(p):
        return remote(work.at[p, 4:6], cols.at[p, :, :, chip], give_send.at[p], give_recv.at[p], beside)

    def far_copy(p):
        return remote(work.at[p, 4:6], cols.at[p, :, :, chip], far_send.at[p], far_recv.at[p], along)

    def far_arrival(p):
        return remote(work.at[p, 4:6], cols.at[p, :, :, 1 - chip], far_send.at[p], far_recv.at[p], along)

    def pass_copy(p):
        return remote(cols.at[p, :, :, 1 - chip], cols.at[p, :, :, 1 - chip], pass_send.at[p], far_recv.at[p], beside)

    def cols_wait(p):
        @pl.when(is_giver)
        def _():
            keep_copy(p).wait()

        @pl.when(jnp.logical_not(is_giver))
        def _():
            give_copy(p).wait_recv()
            far_arrival(p).wait_recv()

    def rows256(p, c):
        return work[p, c // 2, pl.ds(2 * (c % 2), 2)].reshape(256, 256)

    def set_rows256(p, c, value):
        work[p, c // 2, pl.ds(2 * (c % 2), 2)] = value.reshape(2, NB, 256)

    def rows512(p, r):
        return work[p, r].reshape(512, 256)

    def set_rows512(p, r, value):
        work[p, r] = value.reshape(4, NB, 256)

    def own_rows(p):
        return work[p, 4:6].reshape(1024, 256)

    def set_own(p, value):
        work[p, 4:6] = value.reshape(2, 4, NB, 256)

    def tile_in(b):
        return pltpu.make_async_copy(trail.at[pl.ds(512, 1024), pl.ds(b * 256, 256)], schur.at[b], in_sem.at[b])

    keep_strip(first_part).start()
    keep_strip(second_part).start()
    for p in range(1, PAIRS):
        for_pair(p, lambda part: keep_strip(part).start())
    zero[...] = jnp.zeros_like(zero)
    gmat[...] = jnp.zeros_like(gmat)
    pl.semaphore_wait(barrier, 3)
    stage_one(first_part)
    stage_two(first_part)
    stage_one(second_part)
    for_pair(1, stage_one)
    stage_three(first_part)
    lead_wait(first_part)

    def schur_update(q, b):
        schur[b] = schur[b] - dot_nt(own_rows(q), cols[q, b // 4, b % 4].reshape(256, 256))

    def factor(h, p):
        def store_upper(g, value):
            upper[8 * g:8 * g + 8, :] = value

        def store_inv(g, value):
            inv[h, 8 * g:8 * g + 8, :] = value

        def load(i):
            return diag[8 * i:8 * i + 8, :]

        @pl.when(p < LAG)
        def _():
            factor_block(load, store_upper, store_inv)

        @pl.when(p >= LAG)
        def _():
            def beside(g):
                if g % 4 == 0:
                    schur_update(p - LAG, 4 * h + g // 4)

            factor_block(load, store_upper, store_inv, beside)

        work[p, p // 2, 2 * (p % 2) + h, :, half(h)] = upper[...].T

    def lead_step(p):
        @pl.when(p > 0)
        def _():
            for_pair(p, lead_wait)

        def subtract(q, carry):
            right = rows256(q, p)

            def one(r, carry):
                set_rows512(p, r, rows512(p, r) - dot_nt(rows512(q, r), right))
                return carry

            return lax.fori_loop(p // 2, 4, one, carry)

        lax.fori_loop(0, p, subtract, 0)

        @pl.when(p == LAG)
        def _():
            for b in range(8):
                tile_in(b).wait()

        @pl.when(p >= LAG)
        def _():
            cols_wait(p - LAG)

        hi, lo = p // 2, 2 * (p % 2)
        diag[...] = work[p, hi, lo, :, 0:NB]

        def factor_half(h, carry):
            factor(h, p)

            @pl.when(h == 0)
            def _():
                work[p, hi, lo, :, NB:256] = jnp.zeros((NB, NB), jnp.float32)
                low = dot_nt(work[p, hi, lo + 1, :, 0:NB], inv[0])
                work[p, hi, lo + 1, :, 0:NB] = low
                diag[...] = work[p, hi, lo + 1, :, NB:256] - dot_nt(low, low)

            @pl.when((h == 0) & (p == 0))
            def _():
                stage_two(second_part)
                for_pair(1, stage_two)
                for_pair(2, stage_one)
                for_pair(3, stage_one)

            @pl.when((h == 0) & (p > 0) & (p + 1 < PAIRS))
            def _():
                for_pair(p + 1, stage_three)

            @pl.when(h == 0)
            def _():
                keep_own(p).start()

            @pl.when((h == 0) & (p == 1))
            def _():
                for b in range(8):
                    tile_in(b).start()

            return carry

        lax.fori_loop(0, 2, factor_half, 0)

        @pl.when(p == 0)
        def _():
            stage_three(second_part)

        gmat[p % 2, 0:NB, 0:NB] = inv[0]
        gmat[p % 2, NB:256, NB:256] = inv[1]
        gmat[p % 2, NB:256, 0:NB] = -dot_nn(inv[1], dot_nn(work[p, hi, lo + 1, :, 0:NB], inv[0]))

        @pl.when(p == 0)
        def _():
            lead_wait(second_part)

        @pl.when(p % 2 == 0)
        def _():
            set_rows256(p, p + 1, dot_nt(rows256(p, p + 1), gmat[p % 2]))

        def solve(r, carry):
            set_rows512(p, r, dot_nt(rows512(p, r), gmat[p % 2]))
            return carry

        lax.fori_loop(p // 2 + 1, 4, solve, 0)

        @pl.when(p == 0)
        def _():
            for_pair(1, stage_three)

        @pl.when(p + 2 < PAIRS)
        def _():
            for_pair(p + 2, stage_two)

        @pl.when(p + 4 < PAIRS)
        def _():
            for_pair(p + 4, stage_one)

        own_copy(p).start()

    def own_step(p):
        @pl.when(is_giver & (p > 0))
        def _():
            far_arrival(p - 1).wait_recv()
            pass_copy(p - 1).start()

        keep_own(p).wait()
        own_arrival(p).wait_recv()

        def subtract(q, carry):
            set_own(p, own_rows(p) - dot_nt(own_rows(q), rows256(q, p)))
            return carry

        lax.fori_loop(0, p, subtract, 0)
        set_own(p, dot_nt(own_rows(p), gmat[p % 2]))

        @pl.when(is_giver)
        def _():
            far_copy(p).start()
            keep_copy(p).start()
            give_copy(p).start()

    def chain_step(p, carry):
        @pl.when(p < PAIRS)
        def _():
            lead_step(p)

        @pl.when(p > 0)
        def _():
            own_step(p - 1)

        return carry

    lax.fori_loop(0, PAIRS + 1, chain_step, 0)

    def start_pan(p, carry):
        pltpu.make_async_copy(work.at[p, 4:6, :, :, half(my_col)], pan_out.at[p, 1:3], pan_sem.at[0]).start()
        for r in range(4):
            below = 4 * r + my_row >= 2 * p + my_col

            @pl.when(below)
            def _():
                pltpu.make_async_copy(work.at[p, r, my_row, :, half(my_col)], pan_out.at[p, 0, r], pan_sem.at[0]).start()

            @pl.when(jnp.logical_not(below))
            def _():
                pltpu.make_async_copy(zero, pan_out.at[p, 0, r], pan_sem.at[0]).start()

        return carry

    lax.fori_loop(0, PAIRS, start_pan, 0)

    def left_copy():
        return pltpu.make_async_copy(work.at[PAIRS - LAST:PAIRS, 4:6], left_out, left_sem.at[0])

    def right_copy():
        return pltpu.make_async_copy(cols.at[PAIRS - LAST:PAIRS], right_out, left_sem.at[1])

    def schur_copy(b):
        return pltpu.make_async_copy(schur.at[b], schur_out.at[b], out_sem.at[b])

    def top_copy(r):
        return pltpu.make_async_copy(top.at[r % 2], top_out.at[r], top_sem.at[r % 2])

    def top_rows(r):
        if r >= 2:
            top_copy(r - 2).wait()
        p = 2 * r + my_row // 2
        side = half(my_row % 2)

        def one(b, carry):
            top[r % 2, b] = dot_nt(work[p, r, my_row, :, side], cols[p, b // 4, b % 4, :, :, side].reshape(256, NB))
            return carry

        lax.fori_loop(0, 8, one, 0)
        top_copy(r).start()

    left_copy().start()

    for q in range(PAIRS - LAG, PAIRS - LAST):
        cols_wait(q)

    def tail(b, carry):
        for q in range(PAIRS - LAG, PAIRS - LAST):
            schur_update(q, b)
        schur_copy(b).start()
        return carry

    lax.fori_loop(0, 8, tail, 0)

    for r in range(3):
        top_rows(r)

    @pl.when(is_giver)
    def _():
        far_arrival(PAIRS - 1).wait_recv()
        pass_copy(PAIRS - 1).start()

    for q in range(PAIRS - LAST, PAIRS):
        cols_wait(q)
    right_copy().start()
    top_rows(3)
    top_copy(2).wait()
    top_copy(3).wait()
    for b in range(8):
        schur_copy(b).wait()
    left_copy().wait()
    right_copy().wait()
    pltpu.make_async_copy(pan_out, pan_out, pan_sem.at[0]).wait()

    def finish(p, carry):
        own_copy(p).wait_send()

        @pl.when(is_giver)
        def _():
            give_copy(p).wait_send()
            far_copy(p).wait_send()
            pass_copy(p).wait_send()

        return carry

    lax.fori_loop(0, PAIRS, finish, 0)


def finish_body(schur, top, left, right, pan, trail_out, pan_out):
    trail_out[0:512, :] = top[...].reshape(512, 256)
    total = schur[0]
    for q in range(LAST):
        total = total - dot_nt(left[q].reshape(1024, 256), right[q, 0, 0].reshape(256, 256))
    trail_out[512:1536, :] = total
    flat = pan_out.reshape(192 * PAIRS, NB)
    for p in range(PAIRS):
        flat[pl.ds(p, 192, stride=PAIRS), :] = pan[p]


def solution(mesh):
    def local_part(panel_tile, trail_tile):
        pan = panel_tile.transpose(1, 0, 2).reshape(PAIRS, 3, 4, NB, NB)
        any_spec = pl.BlockSpec(memory_space=pl.ANY)
        dma = pltpu.SemaphoreType.DMA
        f32 = jnp.float32
        pan_out, schur, top, left, right = pl.pallas_call(
            body,
            out_shape=(jax.ShapeDtypeStruct(pan.shape, f32), jax.ShapeDtypeStruct((8, 1024, 256), f32),
                       jax.ShapeDtypeStruct((4, 8, NB, 256), f32), jax.ShapeDtypeStruct((LAST, 2, 4, NB, 256), f32),
                       jax.ShapeDtypeStruct((LAST, 2, 4, 2, NB, 256), f32)),
            in_specs=[any_spec] * 2,
            out_specs=(any_spec,) * 5,
            scratch_shapes=[
                pltpu.VMEM((PAIRS, 6, 4, NB, 256), jnp.float32),
                pltpu.VMEM((PAIRS, 2, 4, 2, NB, 256), jnp.float32),
                pltpu.VMEM((8, 1024, 256), jnp.float32),
                pltpu.VMEM((NB, NB), jnp.float32),
                pltpu.VMEM((NB, NB), jnp.float32),
                pltpu.VMEM((2, NB, NB), jnp.float32),
                pltpu.VMEM((2, 256, 256), jnp.float32),
                pltpu.VMEM((2, 8, NB, 256), jnp.float32),
                pltpu.VMEM((NB, NB), jnp.float32),
                dma((PAIRS + 1,)), dma((PAIRS + 1, 7)), dma((PAIRS + 1, 7)), dma((PAIRS,)), dma((PAIRS,)), dma((PAIRS,)), dma((PAIRS,)),
                dma((PAIRS,)), dma((PAIRS,)), dma((PAIRS,)), dma((PAIRS,)), dma((PAIRS,)), dma((8,)), dma((8,)), dma((2,)), dma((2,)),
                dma((1,)),
            ],
            compiler_params=pltpu.CompilerParams(collective_id=0, has_side_effects=True, vmem_limit_bytes=64 * 1024 * 1024 - 65536),
            name="factor",
        )(pan, trail_tile)
        trail_out, panel_out = pl.pallas_call(
            finish_body,
            grid=(8,),
            out_shape=(jax.ShapeDtypeStruct(trail_tile.shape, f32), jax.ShapeDtypeStruct(panel_tile.shape, f32)),
            in_specs=[
                pl.BlockSpec((1, 1024, 256), lambda b: (b, 0, 0)),
                pl.BlockSpec((4, 1, NB, 256), lambda b: (0, b, 0, 0)),
                pl.BlockSpec((LAST, 2, 4, NB, 256), lambda b: (0, 0, 0, 0, 0)),
                pl.BlockSpec((LAST, 1, 1, 2, NB, 256), lambda b: (0, b // 4, b % 4, 0, 0, 0)),
                pl.BlockSpec((PAIRS, 192, NB), lambda b: (0, b, 0)),
            ],
            out_specs=(pl.BlockSpec((1536, 256), lambda b: (0, b)), pl.BlockSpec((192, PAIRS, NB), lambda b: (b, 0, 0))),
            compiler_params=pltpu.CompilerParams(vmem_limit_bytes=64 * 1024 * 1024 - 65536),
            name="finish",
        )(schur, top, left, right, pan_out.reshape(PAIRS, 1536, NB))
        return panel_out, trail_out

    spec_panel = P("pr", "pc", None)
    spec_trail = P("pr", "pc")
    return jax.shard_map(local_part, mesh=mesh, in_specs=(spec_panel, spec_trail), out_specs=(spec_panel, spec_trail), check_vma=False)
```

```python
import jax
import jax.numpy as jnp
from jax import lax
from jax.experimental import pallas as pl
from jax.experimental.pallas import tpu as pltpu
from jax.sharding import PartitionSpec as P

HIGH = lax.Precision.HIGHEST
MESH = pl.DeviceIdType.MESH
NB = 128
PAIRS = 8
LAG = 3
LAST = 2


def dot_nt(a, b):
    return lax.dot_general(a, b, (((1,), (1,)), ((), ())), precision=HIGH, preferred_element_type=jnp.float32)


def dot_nn(a, b):
    return lax.dot_general(a, b, (((1,), (0,)), ((), ())), precision=HIGH, preferred_element_type=jnp.float32)


def lane_of(x, lane):
    return jnp.broadcast_to(x[:, lane:lane + 1], (8, NB))


def row_of(x, row):
    return jnp.broadcast_to(x[row:row + 1, :], (8, NB))


def factor_block(load, store_upper, store_inv, beside=None):
    lane = lax.broadcasted_iota(jnp.int32, (8, NB), 1)
    sub = lax.broadcasted_iota(jnp.int32, (8, NB), 0)
    rows = [load(i) for i in range(16)]
    for g in range(16):
        base = 8 * g
        inside = (lane >= base) & (lane < base + 8)
        cols = [jnp.where(sub < 8, lane_of(rows[g], base + t), 0.0) for t in range(8)]
        cur = jnp.where(inside, jnp.where(lane - base == sub, 1.0, 0.0), rows[g])
        recips, pivots, cross = [], [], {}
        for s in range(8):
            recip = 1.0 / row_of(cols[s], s)
            pivot = row_of(cur, s)
            mult = jnp.where(sub > s, cols[s] * recip, 0.0)
            for t in range(s + 1, 8):
                cross[t, s] = row_of(cols[t], s)
                cols[t] = cols[t] - mult * cross[t, s]
            if s < 7:
                cur = cur - mult * pivot
            recips.append(recip)
            pivots.append(pivot)
        for i in range(g + 1, 16):
            part = [lane_of(rows[i], base + t) for t in range(8)]
            acc = jnp.where(inside, 0.0, rows[i])
            for s in range(8):
                mult = part[s] * recips[s]
                for t in range(s + 1, 8):
                    part[t] = part[t] - mult * cross[t, s]
                acc = acc - mult * pivots[s]
            rows[i] = acc
        if beside is not None:
            beside(g)
        diag = cols[7]
        upper = jnp.where(lane > base + 7, cur, 0.0)
        for t in range(8):
            if t < 7:
                diag = jnp.where(sub == t, cols[t], diag)
            upper = jnp.where((lane == base + t) & (sub <= t), cols[t], upper)
        scale = lax.rsqrt(diag)
        scale = scale * (1.5 - 0.5 * diag * scale * scale)
        store_upper(g, upper * scale)
        store_inv(g, jnp.where(lane < base + 8, cur, 0.0) * scale)


def body(pan, trail, pan_out, schur_out, top_out, left_out, right_out, work, cols, schur, diag, upper, inv, gmat, top, zero,
         lead_sem, lead_send, lead_recv, own_sem, own_send, own_recv, keep_sem, give_send, give_recv, pass_send,
         far_send, far_recv, in_sem, out_sem, top_sem, left_sem, pan_sem):
    my_row = lax.axis_index("pr")
    my_col = lax.axis_index("pc")
    chip = my_row // 2
    core = my_row % 2
    beside_row = 2 * chip + 1 - core
    along_row = 2 * (1 - chip) + core
    cross_row = 2 * (1 - chip) + 1 - core
    across = {"pr": my_row, "pc": 1 - my_col}
    beside = {"pr": beside_row, "pc": my_col}
    along = {"pr": along_row, "pc": my_col}
    is_giver = core == my_col

    barrier = pltpu.get_barrier_semaphore()
    for peer in (across, beside, along):
        pl.semaphore_signal(barrier, inc=1, device_id=peer, device_id_type=MESH)

    def half(c):
        return pl.ds(pl.multiple_of(c * NB, NB), NB)

    def remote(src, dst, send, recv, peer):
        return pltpu.make_async_remote_copy(src_ref=src, dst_ref=dst, send_sem=send, recv_sem=recv,
                                            device_id=peer, device_id_type=MESH)

    first_part = (0, 0, 1, 0)
    second_part = (0, 1, 4, 1)

    def for_pair(p, fn):
        if isinstance(p, int):
            fn((p, p // 2, 4, p + 1))
        else:
            for first in range(4):
                pl.when(p // 2 == first)(lambda first=first: fn((p, first, 4, p + 1)))

    def strip(part, row, col):
        p, lo, hi, _ = part
        return work.at[p, lo:hi, row, :, half(col)]

    def mine(part):
        p, lo, hi, _ = part
        return pan.at[p, 0, lo:hi]

    def keep_strip(part):
        return pltpu.make_async_copy(mine(part), strip(part, my_row, my_col), lead_sem.at[part[3]])

    def lead_copy(part, kind):
        row, col, peer, slot = {
            0: (my_row, my_col, beside, 0),
            1: (my_row, my_col, along, 1),
            2: (my_row, my_col, across, 2),
            3: (my_row, 1 - my_col, along, 3),
            4: (along_row, my_col, beside, 4),
            5: (my_row, 1 - my_col, beside, 5),
            6: (along_row, 1 - my_col, beside, 6),
            7: (along_row, my_col, across, 3),
        }[kind]
        there = strip(part, row, col)
        return remote(mine(part) if kind < 3 else there, there, lead_send.at[part[3], slot], lead_recv.at[part[3], slot], peer)

    def lead_arrival(part, kind):
        row, col = [(beside_row, my_col), (along_row, my_col), (my_row, 1 - my_col), (along_row, 1 - my_col),
                    (cross_row, my_col), (beside_row, 1 - my_col), (cross_row, 1 - my_col)][kind]
        return remote(mine(part), strip(part, row, col), lead_send.at[part[3], kind], lead_recv.at[part[3], kind], beside)

    def stage_one(part):
        for kind in (1, 2, 0):
            lead_copy(part, kind).start()

    def stage_two(part):
        lead_arrival(part, 1).wait_recv()
        lead_arrival(part, 2).wait_recv()

        @pl.when(core == 0)
        def _():
            lead_copy(part, 3).start()

        @pl.when(core == 1)
        def _():
            lead_copy(part, 7).start()

        lead_copy(part, 4).start()
        lead_copy(part, 5).start()

    def stage_three(part):
        lead_arrival(part, 3).wait_recv()
        lead_copy(part, 6).start()

    def lead_wait(part):
        keep_strip(part).wait()
        for kind in (0, 4, 5, 6):
            lead_arrival(part, kind).wait_recv()
        for kind in range(7):
            lead_copy(part, kind).wait_send()

    def keep_own(p):
        return pltpu.make_async_copy(pan.at[p, 1:3], work.at[p, 4:6, :, :, half(my_col)], own_sem.at[p])

    def own_copy(p):
        return remote(pan.at[p, 1:3], work.at[p, 4:6, :, :, half(my_col)], own_send.at[p], own_recv.at[p], across)

    def own_arrival(p):
        return remote(pan.at[p, 1:3], work.at[p, 4:6, :, :, half(1 - my_col)], own_send.at[p], own_recv.at[p], across)

    def keep_copy(p):
        return pltpu.make_async_copy(work.at[p, 4:6], cols.at[p, :, :, chip], keep_sem.at[p])

    def give_copy(p):
        return remote(work.at[p, 4:6], cols.at[p, :, :, chip], give_send.at[p], give_recv.at[p], beside)

    def far_copy(p):
        return remote(work.at[p, 4:6], cols.at[p, :, :, chip], far_send.at[p], far_recv.at[p], along)

    def far_arrival(p):
        return remote(work.at[p, 4:6], cols.at[p, :, :, 1 - chip], far_send.at[p], far_recv.at[p], along)

    def pass_copy(p):
        return remote(cols.at[p, :, :, 1 - chip], cols.at[p, :, :, 1 - chip], pass_send.at[p], far_recv.at[p], beside)

    def cols_wait(p):
        @pl.when(is_giver)
        def _():
            keep_copy(p).wait()

        @pl.when(jnp.logical_not(is_giver))
        def _():
            give_copy(p).wait_recv()
            far_arrival(p).wait_recv()

    def rows256(p, c):
        return work[p, c // 2, pl.ds(2 * (c % 2), 2)].reshape(256, 256)

    def set_rows256(p, c, value):
        work[p, c // 2, pl.ds(2 * (c % 2), 2)] = value.reshape(2, NB, 256)

    def rows512(p, r):
        return work[p, r].reshape(512, 256)

    def set_rows512(p, r, value):
        work[p, r] = value.reshape(4, NB, 256)

    def own_rows(p):
        return work[p, 4:6].reshape(1024, 256)

    def set_own(p, value):
        work[p, 4:6] = value.reshape(2, 4, NB, 256)

    def tile_in(b):
        return pltpu.make_async_copy(trail.at[pl.ds(512, 1024), pl.ds(b * 256, 256)], schur.at[b], in_sem.at[b])

    keep_strip(first_part).start()
    keep_strip(second_part).start()
    for p in range(1, PAIRS):
        for_pair(p, lambda part: keep_strip(part).start())
    zero[...] = jnp.zeros_like(zero)
    gmat[...] = jnp.zeros_like(gmat)
    pl.semaphore_wait(barrier, 3)
    stage_one(first_part)
    stage_two(first_part)
    stage_one(second_part)
    for_pair(1, stage_one)
    stage_three(first_part)
    lead_wait(first_part)

    def schur_update(q, b):
        schur[b] = schur[b] - dot_nt(own_rows(q), cols[q, b // 4, b % 4].reshape(256, 256))

    def extra_update(p, e):
        ahead = jnp.where(p < PAIRS - 1, p, 0)
        is_lead = e < ahead
        is_own = jnp.logical_not(is_lead) & (e - ahead < p - 1)
        q = jnp.where(is_lead, e, jnp.where(is_own, e - ahead, 0))
        right = jnp.where(is_lead, p + 1, jnp.where(is_own, p - 1, 0))
        pair = jnp.where(is_lead, p + 1, jnp.where(is_own, p - 1, PAIRS))
        rows = pl.ds(jnp.where(is_lead, 2, 4), 2)
        value = work[pair, rows].reshape(1024, 256) - dot_nt(work[q, rows].reshape(1024, 256), rows256(q, right))
        work[pair, rows] = value.reshape(2, 4, NB, 256)

    def factor(h, p):
        def store_upper(g, value):
            upper[8 * g:8 * g + 8, :] = value

        def store_inv(g, value):
            inv[h, 8 * g:8 * g + 8, :] = value

        def load(i):
            return diag[8 * i:8 * i + 8, :]

        @pl.when(p < LAG)
        def _():
            factor_block(load, store_upper, store_inv)

        @pl.when(p >= LAG)
        def _():
            def beside(g):
                if g % 4 == 0:
                    schur_update(p - LAG, 4 * h + g // 4)
                elif g % 4 == 2 and g < 12:
                    extra_update(p, 3 * h + g // 4)

            factor_block(load, store_upper, store_inv, beside)

        work[p, p // 2, 2 * (p % 2) + h, :, half(h)] = upper[...].T

    def lead_step(p):
        @pl.when((p > 0) & (p <= LAG))
        def _():
            for_pair(p, lead_wait)

        @pl.when((p >= LAG) & (p + 1 < PAIRS))
        def _():
            for_pair(p + 1, lead_wait)

        def subtract(q, carry):
            right = rows256(q, p)

            def one(r, carry):
                set_rows512(p, r, rows512(p, r) - dot_nt(rows512(q, r), right))
                return carry

            return lax.fori_loop(p // 2, 4, one, carry)

        lax.fori_loop((p - 1) * (p // 4), p, subtract, 0)

        @pl.when(p == LAG)
        def _():
            for b in range(8):
                tile_in(b).wait()

        @pl.when(p >= LAG)
        def _():
            cols_wait(p - LAG)

        hi, lo = p // 2, 2 * (p % 2)
        diag[...] = work[p, hi, lo, :, 0:NB]

        @pl.when(p > LAG)
        def _():
            own_wait(p - 1)

        def factor_half(h, carry):
            factor(h, p)

            @pl.when((h == 0) & (p == LAG))
            def _():
                own_wait(p - 1)

            @pl.when(h == 0)
            def _():
                work[p, hi, lo, :, NB:256] = jnp.zeros((NB, NB), jnp.float32)
                low = dot_nt(work[p, hi, lo + 1, :, 0:NB], inv[0])
                work[p, hi, lo + 1, :, 0:NB] = low
                diag[...] = work[p, hi, lo + 1, :, NB:256] - dot_nt(low, low)

            @pl.when((h == 0) & (p == 0))
            def _():
                stage_two(second_part)
                for_pair(1, stage_two)
                for_pair(2, stage_one)
                for_pair(3, stage_one)

            @pl.when((h == 0) & ((p == 1) | (p == 2)))
            def _():
                for_pair(p + 1, stage_three)

            @pl.when((h == 0) & (p >= 2) & (p + 2 < PAIRS))
            def _():
                for_pair(p + 2, stage_three)

            @pl.when(h == 0)
            def _():
                keep_own(p).start()

            @pl.when((h == 0) & (p == 1))
            def _():
                for b in range(8):
                    tile_in(b).start()

            return carry

        lax.fori_loop(0, 2, factor_half, 0)

        @pl.when(p == 0)
        def _():
            stage_three(second_part)

        gmat[p % 2, 0:NB, 0:NB] = inv[0]
        gmat[p % 2, NB:256, NB:256] = inv[1]
        gmat[p % 2, NB:256, 0:NB] = -dot_nn(inv[1], dot_nn(work[p, hi, lo + 1, :, 0:NB], inv[0]))

        @pl.when(p == 0)
        def _():
            lead_wait(second_part)

        @pl.when(p % 2 == 0)
        def _():
            set_rows256(p, p + 1, dot_nt(rows256(p, p + 1), gmat[p % 2]))

        def solve(r, carry):
            set_rows512(p, r, dot_nt(rows512(p, r), gmat[p % 2]))
            return carry

        lax.fori_loop(p // 2 + 1, 4, solve, 0)

        @pl.when(p == 0)
        def _():
            for_pair(1, stage_three)

        @pl.when(p < 2)
        def _():
            for_pair(p + 2, stage_two)

        @pl.when((p > 0) & (p + 3 < PAIRS))
        def _():
            for_pair(p + 3, stage_two)

        @pl.when(p + 4 < PAIRS)
        def _():
            for_pair(p + 4, stage_one)

        @pl.when(p <= 2)
        def _():
            own_copy(p).start()

        @pl.when((p >= 2) & (p + 1 < PAIRS))
        def _():
            own_copy(p + 1).start()

    def own_wait(p):
        keep_own(p).wait()
        own_arrival(p).wait_recv()

    def own_step(p):
        @pl.when(is_giver & (p > 0))
        def _():
            far_arrival(p - 1).wait_recv()
            pass_copy(p - 1).start()

        @pl.when((p < LAG - 1) | (p == PAIRS - 1))
        def _():
            own_wait(p)

        def subtract(q, carry):
            set_own(p, own_rows(p) - dot_nt(own_rows(q), rows256(q, p)))
            return carry

        def reached(step):
            return (p + 1 + 16 - step) // 16

        done = 2 * reached(3) - reached(5) - reached(6) + 6 * reached(7) - 6 * reached(8)
        lax.fori_loop(done, p, subtract, 0)
        set_own(p, dot_nt(own_rows(p), gmat[p % 2]))

        @pl.when(is_giver)
        def _():
            far_copy(p).start()
            keep_copy(p).start()
            give_copy(p).start()

    def chain_step(p, carry):
        @pl.when(p < PAIRS)
        def _():
            lead_step(p)

        @pl.when(p > 0)
        def _():
            own_step(p - 1)

        return carry

    lax.fori_loop(0, PAIRS + 1, chain_step, 0)

    def start_pan(p, carry):
        pltpu.make_async_copy(work.at[p, 4:6, :, :, half(my_col)], pan_out.at[p, 1:3], pan_sem.at[0]).start()
        for r in range(4):
            below = 4 * r + my_row >= 2 * p + my_col

            @pl.when(below)
            def _():
                pltpu.make_async_copy(work.at[p, r, my_row, :, half(my_col)], pan_out.at[p, 0, r], pan_sem.at[0]).start()

            @pl.when(jnp.logical_not(below))
            def _():
                pltpu.make_async_copy(zero, pan_out.at[p, 0, r], pan_sem.at[0]).start()

        return carry

    lax.fori_loop(0, PAIRS, start_pan, 0)

    def left_copy():
        return pltpu.make_async_copy(work.at[PAIRS - LAST:PAIRS, 4:6], left_out, left_sem.at[0])

    def right_copy():
        return pltpu.make_async_copy(cols.at[PAIRS - LAST:PAIRS], right_out, left_sem.at[1])

    def schur_copy(b):
        return pltpu.make_async_copy(schur.at[b], schur_out.at[b], out_sem.at[b])

    def top_copy(r):
        return pltpu.make_async_copy(top.at[r % 2], top_out.at[r], top_sem.at[r % 2])

    def top_rows(r):
        if r >= 2:
            top_copy(r - 2).wait()
        p = 2 * r + my_row // 2
        side = half(my_row % 2)

        def one(b, carry):
            top[r % 2, b] = dot_nt(work[p, r, my_row, :, side], cols[p, b // 4, b % 4, :, :, side].reshape(256, NB))
            return carry

        lax.fori_loop(0, 8, one, 0)
        top_copy(r).start()

    left_copy().start()

    for q in range(PAIRS - LAG, PAIRS - LAST):
        cols_wait(q)

    def tail(b, carry):
        for q in range(PAIRS - LAG, PAIRS - LAST):
            schur_update(q, b)
        schur_copy(b).start()
        return carry

    lax.fori_loop(0, 8, tail, 0)

    for r in range(3):
        top_rows(r)

    @pl.when(is_giver)
    def _():
        far_arrival(PAIRS - 1).wait_recv()
        pass_copy(PAIRS - 1).start()

    for q in range(PAIRS - LAST, PAIRS):
        cols_wait(q)
    right_copy().start()
    top_rows(3)
    top_copy(2).wait()
    top_copy(3).wait()
    for b in range(8):
        schur_copy(b).wait()
    left_copy().wait()
    right_copy().wait()
    pltpu.make_async_copy(pan_out, pan_out, pan_sem.at[0]).wait()

    def finish(p, carry):
        own_copy(p).wait_send()

        @pl.when(is_giver)
        def _():
            give_copy(p).wait_send()
            far_copy(p).wait_send()
            pass_copy(p).wait_send()

        return carry

    lax.fori_loop(0, PAIRS, finish, 0)


def finish_body(schur, top, left, right, pan, trail_out, pan_out):
    trail_out[0:512, :] = top[...].reshape(512, 256)
    total = schur[0]
    for q in range(LAST):
        total = total - dot_nt(left[q].reshape(1024, 256), right[q, 0, 0].reshape(256, 256))
    trail_out[512:1536, :] = total
    flat = pan_out.reshape(192 * PAIRS, NB)
    for p in range(PAIRS):
        flat[pl.ds(p, 192, stride=PAIRS), :] = pan[p]


def solution(mesh):
    def local_part(panel_tile, trail_tile):
        pan = panel_tile.transpose(1, 0, 2).reshape(PAIRS, 3, 4, NB, NB)
        any_spec = pl.BlockSpec(memory_space=pl.ANY)
        dma = pltpu.SemaphoreType.DMA
        f32 = jnp.float32
        pan_out, schur, top, left, right = pl.pallas_call(
            body,
            out_shape=(jax.ShapeDtypeStruct(pan.shape, f32), jax.ShapeDtypeStruct((8, 1024, 256), f32),
                       jax.ShapeDtypeStruct((4, 8, NB, 256), f32), jax.ShapeDtypeStruct((LAST, 2, 4, NB, 256), f32),
                       jax.ShapeDtypeStruct((LAST, 2, 4, 2, NB, 256), f32)),
            in_specs=[any_spec] * 2,
            out_specs=(any_spec,) * 5,
            scratch_shapes=[
                pltpu.VMEM((PAIRS + 1, 6, 4, NB, 256), jnp.float32),
                pltpu.VMEM((PAIRS, 2, 4, 2, NB, 256), jnp.float32),
                pltpu.VMEM((8, 1024, 256), jnp.float32),
                pltpu.VMEM((NB, NB), jnp.float32),
                pltpu.VMEM((NB, NB), jnp.float32),
                pltpu.VMEM((2, NB, NB), jnp.float32),
                pltpu.VMEM((2, 256, 256), jnp.float32),
                pltpu.VMEM((2, 8, NB, 256), jnp.float32),
                pltpu.VMEM((NB, NB), jnp.float32),
                dma((PAIRS + 1,)), dma((PAIRS + 1, 7)), dma((PAIRS + 1, 7)), dma((PAIRS,)), dma((PAIRS,)), dma((PAIRS,)), dma((PAIRS,)),
                dma((PAIRS,)), dma((PAIRS,)), dma((PAIRS,)), dma((PAIRS,)), dma((PAIRS,)), dma((8,)), dma((8,)), dma((2,)), dma((2,)),
                dma((1,)),
            ],
            compiler_params=pltpu.CompilerParams(collective_id=0, has_side_effects=True, vmem_limit_bytes=64 * 1024 * 1024 - 65536),
            name="factor",
        )(pan, trail_tile)
        trail_out, panel_out = pl.pallas_call(
            finish_body,
            grid=(8,),
            out_shape=(jax.ShapeDtypeStruct(trail_tile.shape, f32), jax.ShapeDtypeStruct(panel_tile.shape, f32)),
            in_specs=[
                pl.BlockSpec((1, 1024, 256), lambda b: (b, 0, 0)),
                pl.BlockSpec((4, 1, NB, 256), lambda b: (0, b, 0, 0)),
                pl.BlockSpec((LAST, 2, 4, NB, 256), lambda b: (0, 0, 0, 0, 0)),
                pl.BlockSpec((LAST, 1, 1, 2, NB, 256), lambda b: (0, b // 4, b % 4, 0, 0, 0)),
                pl.BlockSpec((PAIRS, 192, NB), lambda b: (0, b, 0)),
            ],
            out_specs=(pl.BlockSpec((1536, 256), lambda b: (0, b)), pl.BlockSpec((192, PAIRS, NB), lambda b: (b, 0, 0))),
            compiler_params=pltpu.CompilerParams(vmem_limit_bytes=64 * 1024 * 1024 - 65536),
            name="finish",
        )(schur, top, left, right, pan_out.reshape(PAIRS, 1536, NB))
        return panel_out, trail_out

    spec_panel = P("pr", "pc", None)
    spec_trail = P("pr", "pc")
    return jax.shard_map(local_part, mesh=mesh, in_specs=(spec_panel, spec_trail), out_specs=(spec_panel, spec_trail), check_vma=False)
```

```python
import jax
import jax.numpy as jnp
from jax import lax
from jax.experimental import pallas as pl
from jax.experimental.pallas import tpu as pltpu
from jax.sharding import PartitionSpec as P

HIGH = lax.Precision.HIGHEST
MESH = pl.DeviceIdType.MESH
NB = 128
PAIRS = 8
LAG = 3
LAST = 2


def dot_nt(a, b):
    return lax.dot_general(a, b, (((1,), (1,)), ((), ())), precision=HIGH, preferred_element_type=jnp.float32)


def dot_nn(a, b):
    return lax.dot_general(a, b, (((1,), (0,)), ((), ())), precision=HIGH, preferred_element_type=jnp.float32)


def lane_of(x, lane):
    return jnp.broadcast_to(x[:, lane:lane + 1], (8, NB))


def row_of(x, row):
    return jnp.broadcast_to(x[row:row + 1, :], (8, NB))


def factor_block(load, store_upper, store_inv, beside=None):
    lane = lax.broadcasted_iota(jnp.int32, (8, NB), 1)
    sub = lax.broadcasted_iota(jnp.int32, (8, NB), 0)
    rows = [load(i) for i in range(16)]
    for g in range(16):
        base = 8 * g
        inside = (lane >= base) & (lane < base + 8)
        cols = [jnp.where(sub < 8, lane_of(rows[g], base + t), 0.0) for t in range(8)]
        cur = jnp.where(inside, jnp.where(lane - base == sub, 1.0, 0.0), rows[g])
        recips, pivots, cross = [], [], {}
        for s in range(8):
            recip = 1.0 / row_of(cols[s], s)
            pivot = row_of(cur, s)
            mult = jnp.where(sub > s, cols[s] * recip, 0.0)
            for t in range(s + 1, 8):
                cross[t, s] = row_of(cols[t], s)
                cols[t] = cols[t] - mult * cross[t, s]
            if s < 7:
                cur = cur - mult * pivot
            recips.append(recip)
            pivots.append(pivot)
        for i in range(g + 1, 16):
            part = [lane_of(rows[i], base + t) for t in range(8)]
            acc = jnp.where(inside, 0.0, rows[i])
            for s in range(8):
                mult = part[s] * recips[s]
                for t in range(s + 1, 8):
                    part[t] = part[t] - mult * cross[t, s]
                acc = acc - mult * pivots[s]
            rows[i] = acc
        if beside is not None:
            beside(g)
        diag = cols[7]
        upper = jnp.where(lane > base + 7, cur, 0.0)
        for t in range(8):
            if t < 7:
                diag = jnp.where(sub == t, cols[t], diag)
            upper = jnp.where((lane == base + t) & (sub <= t), cols[t], upper)
        scale = lax.rsqrt(diag)
        scale = scale * (1.5 - 0.5 * diag * scale * scale)
        store_upper(g, upper * scale)
        store_inv(g, jnp.where(lane < base + 8, cur, 0.0) * scale)


def body(pan, trail, pan_out, schur_out, top_out, left_out, right_out, work, cols, schur, diag, upper, inv, gmat, top, zero,
         lead_sem, lead_send, lead_recv, own_sem, own_send, own_recv, keep_sem, give_send, give_recv, pass_send,
         far_send, far_recv, in_sem, out_sem, top_sem, left_sem, pan_sem):
    my_row = lax.axis_index("pr")
    my_col = lax.axis_index("pc")
    chip = my_row // 2
    core = my_row % 2
    beside_row = 2 * chip + 1 - core
    along_row = 2 * (1 - chip) + core
    cross_row = 2 * (1 - chip) + 1 - core
    across = {"pr": my_row, "pc": 1 - my_col}
    beside = {"pr": beside_row, "pc": my_col}
    along = {"pr": along_row, "pc": my_col}
    is_giver = core == my_col

    barrier = pltpu.get_barrier_semaphore()
    for peer in (across, beside, along):
        pl.semaphore_signal(barrier, inc=1, device_id=peer, device_id_type=MESH)

    def half(c):
        return pl.ds(pl.multiple_of(c * NB, NB), NB)

    def remote(src, dst, send, recv, peer):
        return pltpu.make_async_remote_copy(src_ref=src, dst_ref=dst, send_sem=send, recv_sem=recv,
                                            device_id=peer, device_id_type=MESH)

    first_part = (0, 0, 1, 0)
    second_part = (0, 1, 4, 1)

    def for_pair(p, fn):
        if isinstance(p, int):
            fn((p, p // 2, 4, p + 1))
        else:
            for first in range(4):
                pl.when(p // 2 == first)(lambda first=first: fn((p, first, 4, p + 1)))

    def strip(part, row, col):
        p, lo, hi, _ = part
        return work.at[p, lo:hi, row, :, half(col)]

    def mine(part):
        p, lo, hi, _ = part
        return pan.at[p, 0, lo:hi]

    def keep_strip(part):
        return pltpu.make_async_copy(mine(part), strip(part, my_row, my_col), lead_sem.at[part[3]])

    def lead_copy(part, kind):
        row, col, peer, slot = {
            0: (my_row, my_col, beside, 0),
            1: (my_row, my_col, along, 1),
            2: (my_row, my_col, across, 2),
            3: (my_row, 1 - my_col, along, 3),
            4: (along_row, my_col, beside, 4),
            5: (my_row, 1 - my_col, beside, 5),
            6: (along_row, 1 - my_col, beside, 6),
            7: (along_row, my_col, across, 3),
        }[kind]
        there = strip(part, row, col)
        return remote(mine(part) if kind < 3 else there, there, lead_send.at[part[3], slot], lead_recv.at[part[3], slot], peer)

    def lead_arrival(part, kind):
        row, col = [(beside_row, my_col), (along_row, my_col), (my_row, 1 - my_col), (along_row, 1 - my_col),
                    (cross_row, my_col), (beside_row, 1 - my_col), (cross_row, 1 - my_col)][kind]
        return remote(mine(part), strip(part, row, col), lead_send.at[part[3], kind], lead_recv.at[part[3], kind], beside)

    def stage_one(part):
        for kind in (1, 2, 0):
            lead_copy(part, kind).start()

    def stage_two(part):
        lead_arrival(part, 1).wait_recv()
        lead_arrival(part, 2).wait_recv()

        @pl.when(core == 0)
        def _():
            lead_copy(part, 3).start()

        @pl.when(core == 1)
        def _():
            lead_copy(part, 7).start()

        lead_copy(part, 4).start()
        lead_copy(part, 5).start()

    def stage_three(part):
        lead_arrival(part, 3).wait_recv()
        lead_copy(part, 6).start()

    def lead_wait(part):
        keep_strip(part).wait()
        for kind in (0, 4, 5, 6):
            lead_arrival(part, kind).wait_recv()
        for kind in range(7):
            lead_copy(part, kind).wait_send()

    def keep_own(p):
        return pltpu.make_async_copy(pan.at[p, 1:3], work.at[p, 4:6, :, :, half(my_col)], own_sem.at[p])

    def own_copy(p):
        return remote(pan.at[p, 1:3], work.at[p, 4:6, :, :, half(my_col)], own_send.at[p], own_recv.at[p], across)

    def own_arrival(p):
        return remote(pan.at[p, 1:3], work.at[p, 4:6, :, :, half(1 - my_col)], own_send.at[p], own_recv.at[p], across)

    def keep_copy(p):
        return pltpu.make_async_copy(work.at[p, 4:6], cols.at[p, :, :, chip], keep_sem.at[p])

    def give_copy(p):
        return remote(work.at[p, 4:6], cols.at[p, :, :, chip], give_send.at[p], give_recv.at[p], beside)

    def far_copy(p):
        return remote(work.at[p, 4:6], cols.at[p, :, :, chip], far_send.at[p], far_recv.at[p], along)

    def far_arrival(p):
        return remote(work.at[p, 4:6], cols.at[p, :, :, 1 - chip], far_send.at[p], far_recv.at[p], along)

    def pass_copy(p):
        return remote(cols.at[p, :, :, 1 - chip], cols.at[p, :, :, 1 - chip], pass_send.at[p], far_recv.at[p], beside)

    def cols_wait(p):
        @pl.when(is_giver)
        def _():
            keep_copy(p).wait()

        @pl.when(jnp.logical_not(is_giver))
        def _():
            give_copy(p).wait_recv()
            far_arrival(p).wait_recv()

    def rows256(p, c):
        return work[p, c // 2, pl.ds(2 * (c % 2), 2)].reshape(256, 256)

    def set_rows256(p, c, value):
        work[p, c // 2, pl.ds(2 * (c % 2), 2)] = value.reshape(2, NB, 256)

    def rows512(p, r):
        return work[p, r].reshape(512, 256)

    def set_rows512(p, r, value):
        work[p, r] = value.reshape(4, NB, 256)

    def own_rows(p):
        return work[p, 4:6].reshape(1024, 256)

    def set_own(p, value):
        work[p, 4:6] = value.reshape(2, 4, NB, 256)

    def tile_in(b):
        return pltpu.make_async_copy(trail.at[pl.ds(512, 1024), pl.ds(b * 256, 256)], schur.at[b], in_sem.at[b])

    keep_strip(first_part).start()
    keep_strip(second_part).start()
    for p in range(1, PAIRS):
        for_pair(p, lambda part: keep_strip(part).start())
    zero[...] = jnp.zeros_like(zero)
    gmat[...] = jnp.zeros_like(gmat)
    pl.semaphore_wait(barrier, 3)
    stage_one(first_part)
    stage_two(first_part)
    stage_one(second_part)
    for_pair(1, stage_one)
    stage_three(first_part)
    lead_wait(first_part)

    def schur_update(q, b):
        schur[b] = schur[b] - dot_nt(own_rows(q), cols[q, b // 4, b % 4].reshape(256, 256))

    def factor(h, p):
        def store_upper(g, value):
            upper[8 * g:8 * g + 8, :] = value

        def store_inv(g, value):
            inv[h, 8 * g:8 * g + 8, :] = value

        def load(i):
            return diag[8 * i:8 * i + 8, :]

        factor_block(load, store_upper, store_inv)
        work[p, p // 2, 2 * (p % 2) + h, :, half(h)] = upper[...].T

    def lead_step(p):
        @pl.when(p > 0)
        def _():
            for_pair(p, lead_wait)

        def subtract(q, carry):
            right = rows256(q, p)

            def one(r, carry):
                set_rows512(p, r, rows512(p, r) - dot_nt(rows512(q, r), right))
                return carry

            return lax.fori_loop(p // 2, 4, one, carry)

        lax.fori_loop(0, p, subtract, 0)

        @pl.when(p == LAG)
        def _():
            for b in range(8):
                tile_in(b).wait()

        @pl.when(p >= LAG)
        def _():
            cols_wait(p - LAG)

            def schur_step(b, carry):
                schur_update(p - LAG, b)
                return carry

            lax.fori_loop(0, 8, schur_step, 0)

        hi, lo = p // 2, 2 * (p % 2)
        diag[...] = work[p, hi, lo, :, 0:NB]

        def factor_half(h, carry):
            factor(h, p)

            @pl.when(h == 0)
            def _():
                work[p, hi, lo, :, NB:256] = jnp.zeros((NB, NB), jnp.float32)
                low = dot_nt(work[p, hi, lo + 1, :, 0:NB], inv[0])
                work[p, hi, lo + 1, :, 0:NB] = low
                diag[...] = work[p, hi, lo + 1, :, NB:256] - dot_nt(low, low)

            @pl.when((h == 0) & (p == 0))
            def _():
                stage_two(second_part)
                for_pair(1, stage_two)
                for_pair(2, stage_one)
                for_pair(3, stage_one)

            @pl.when((h == 0) & (p > 0) & (p + 1 < PAIRS))
            def _():
                for_pair(p + 1, stage_three)

            @pl.when(h == 0)
            def _():
                keep_own(p).start()

            @pl.when((h == 0) & (p == 1))
            def _():
                for b in range(8):
                    tile_in(b).start()

            return carry

        lax.fori_loop(0, 2, factor_half, 0)

        @pl.when(p == 0)
        def _():
            stage_three(second_part)

        gmat[p % 2, 0:NB, 0:NB] = inv[0]
        gmat[p % 2, NB:256, NB:256] = inv[1]
        gmat[p % 2, NB:256, 0:NB] = -dot_nn(inv[1], dot_nn(work[p, hi, lo + 1, :, 0:NB], inv[0]))

        @pl.when(p == 0)
        def _():
            lead_wait(second_part)

        @pl.when(p % 2 == 0)
        def _():
            set_rows256(p, p + 1, dot_nt(rows256(p, p + 1), gmat[p % 2]))

        def solve(r, carry):
            set_rows512(p, r, dot_nt(rows512(p, r), gmat[p % 2]))
            return carry

        lax.fori_loop(p // 2 + 1, 4, solve, 0)

        @pl.when(p == 0)
        def _():
            for_pair(1, stage_three)

        @pl.when(p + 2 < PAIRS)
        def _():
            for_pair(p + 2, stage_two)

        @pl.when(p + 4 < PAIRS)
        def _():
            for_pair(p + 4, stage_one)

        own_copy(p).start()

    def own_step(p):
        @pl.when(is_giver & (p > 0))
        def _():
            far_arrival(p - 1).wait_recv()
            pass_copy(p - 1).start()

        keep_own(p).wait()
        own_arrival(p).wait_recv()

        def subtract(q, carry):
            set_own(p, own_rows(p) - dot_nt(own_rows(q), rows256(q, p)))
            return carry

        lax.fori_loop(0, p, subtract, 0)
        set_own(p, dot_nt(own_rows(p), gmat[p % 2]))

        @pl.when(is_giver)
        def _():
            far_copy(p).start()
            keep_copy(p).start()
            give_copy(p).start()

    def chain_step(p, carry):
        @pl.when(p < PAIRS)
        def _():
            lead_step(p)

        @pl.when(p > 0)
        def _():
            own_step(p - 1)

        return carry

    lax.fori_loop(0, PAIRS + 1, chain_step, 0)

    def start_pan(p, carry):
        pltpu.make_async_copy(work.at[p, 4:6, :, :, half(my_col)], pan_out.at[p, 1:3], pan_sem.at[0]).start()
        for r in range(4):
            below = 4 * r + my_row >= 2 * p + my_col

            @pl.when(below)
            def _():
                pltpu.make_async_copy(work.at[p, r, my_row, :, half(my_col)], pan_out.at[p, 0, r], pan_sem.at[0]).start()

            @pl.when(jnp.logical_not(below))
            def _():
                pltpu.make_async_copy(zero, pan_out.at[p, 0, r], pan_sem.at[0]).start()

        return carry

    lax.fori_loop(0, PAIRS, start_pan, 0)

    def left_copy():
        return pltpu.make_async_copy(work.at[PAIRS - LAST:PAIRS, 4:6], left_out, left_sem.at[0])

    def right_copy():
        return pltpu.make_async_copy(cols.at[PAIRS - LAST:PAIRS], right_out, left_sem.at[1])

    def schur_copy(b):
        return pltpu.make_async_copy(schur.at[b], schur_out.at[b], out_sem.at[b])

    def top_copy(r):
        return pltpu.make_async_copy(top.at[r % 2], top_out.at[r], top_sem.at[r % 2])

    def top_rows(r):
        if r >= 2:
            top_copy(r - 2).wait()
        p = 2 * r + my_row // 2
        side = half(my_row % 2)

        def one(b, carry):
            top[r % 2, b] = dot_nt(work[p, r, my_row, :, side], cols[p, b // 4, b % 4, :, :, side].reshape(256, NB))
            return carry

        lax.fori_loop(0, 8, one, 0)
        top_copy(r).start()

    left_copy().start()

    for q in range(PAIRS - LAG, PAIRS - LAST):
        cols_wait(q)

    def tail(b, carry):
        for q in range(PAIRS - LAG, PAIRS - LAST):
            schur_update(q, b)
        schur_copy(b).start()
        return carry

    lax.fori_loop(0, 8, tail, 0)

    for r in range(3):
        top_rows(r)

    @pl.when(is_giver)
    def _():
        far_arrival(PAIRS - 1).wait_recv()
        pass_copy(PAIRS - 1).start()

    for q in range(PAIRS - LAST, PAIRS):
        cols_wait(q)
    right_copy().start()
    top_rows(3)
    top_copy(2).wait()
    top_copy(3).wait()
    for b in range(8):
        schur_copy(b).wait()
    left_copy().wait()
    right_copy().wait()
    pltpu.make_async_copy(pan_out, pan_out, pan_sem.at[0]).wait()

    def finish(p, carry):
        own_copy(p).wait_send()

        @pl.when(is_giver)
        def _():
            give_copy(p).wait_send()
            far_copy(p).wait_send()
            pass_copy(p).wait_send()

        return carry

    lax.fori_loop(0, PAIRS, finish, 0)


def finish_body(schur, top, left, right, pan, trail_out, pan_out):
    trail_out[0:512, :] = top[...].reshape(512, 256)
    total = schur[0]
    for q in range(LAST):
        total = total - dot_nt(left[q].reshape(1024, 256), right[q, 0, 0].reshape(256, 256))
    trail_out[512:1536, :] = total
    flat = pan_out.reshape(192 * PAIRS, NB)
    for p in range(PAIRS):
        flat[pl.ds(p, 192, stride=PAIRS), :] = pan[p]


def solution(mesh):
    def local_part(panel_tile, trail_tile):
        pan = panel_tile.transpose(1, 0, 2).reshape(PAIRS, 3, 4, NB, NB)
        any_spec = pl.BlockSpec(memory_space=pl.ANY)
        dma = pltpu.SemaphoreType.DMA
        f32 = jnp.float32
        pan_out, schur, top, left, right = pl.pallas_call(
            body,
            out_shape=(jax.ShapeDtypeStruct(pan.shape, f32), jax.ShapeDtypeStruct((8, 1024, 256), f32),
                       jax.ShapeDtypeStruct((4, 8, NB, 256), f32), jax.ShapeDtypeStruct((LAST, 2, 4, NB, 256), f32),
                       jax.ShapeDtypeStruct((LAST, 2, 4, 2, NB, 256), f32)),
            in_specs=[any_spec] * 2,
            out_specs=(any_spec,) * 5,
            scratch_shapes=[
                pltpu.VMEM((PAIRS, 6, 4, NB, 256), jnp.float32),
                pltpu.VMEM((PAIRS, 2, 4, 2, NB, 256), jnp.float32),
                pltpu.VMEM((8, 1024, 256), jnp.float32),
                pltpu.VMEM((NB, NB), jnp.float32),
                pltpu.VMEM((NB, NB), jnp.float32),
                pltpu.VMEM((2, NB, NB), jnp.float32),
                pltpu.VMEM((2, 256, 256), jnp.float32),
                pltpu.VMEM((2, 8, NB, 256), jnp.float32),
                pltpu.VMEM((NB, NB), jnp.float32),
                dma((PAIRS + 1,)), dma((PAIRS + 1, 7)), dma((PAIRS + 1, 7)), dma((PAIRS,)), dma((PAIRS,)), dma((PAIRS,)), dma((PAIRS,)),
                dma((PAIRS,)), dma((PAIRS,)), dma((PAIRS,)), dma((PAIRS,)), dma((PAIRS,)), dma((8,)), dma((8,)), dma((2,)), dma((2,)),
                dma((1,)),
            ],
            compiler_params=pltpu.CompilerParams(collective_id=0, has_side_effects=True, vmem_limit_bytes=64 * 1024 * 1024 - 65536),
            name="factor",
        )(pan, trail_tile)
        trail_out, panel_out = pl.pallas_call(
            finish_body,
            grid=(8,),
            out_shape=(jax.ShapeDtypeStruct(trail_tile.shape, f32), jax.ShapeDtypeStruct(panel_tile.shape, f32)),
            in_specs=[
                pl.BlockSpec((1, 1024, 256), lambda b: (b, 0, 0)),
                pl.BlockSpec((4, 1, NB, 256), lambda b: (0, b, 0, 0)),
                pl.BlockSpec((LAST, 2, 4, NB, 256), lambda b: (0, 0, 0, 0, 0)),
                pl.BlockSpec((LAST, 1, 1, 2, NB, 256), lambda b: (0, b // 4, b % 4, 0, 0, 0)),
                pl.BlockSpec((PAIRS, 192, NB), lambda b: (0, b, 0)),
            ],
            out_specs=(pl.BlockSpec((1536, 256), lambda b: (0, b)), pl.BlockSpec((192, PAIRS, NB), lambda b: (b, 0, 0))),
            compiler_params=pltpu.CompilerParams(vmem_limit_bytes=64 * 1024 * 1024 - 65536),
            name="finish",
        )(schur, top, left, right, pan_out.reshape(PAIRS, 1536, NB))
        return panel_out, trail_out

    spec_panel = P("pr", "pc", None)
    spec_trail = P("pr", "pc")
    return jax.shard_map(local_part, mesh=mesh, in_specs=(spec_panel, spec_trail), out_specs=(spec_panel, spec_trail), check_vma=False)
```

```python
import jax
import jax.numpy as jnp
from jax import lax
from jax.experimental import pallas as pl
from jax.experimental.pallas import tpu as pltpu
from jax.sharding import PartitionSpec as P

HIGH = lax.Precision.HIGHEST
MESH = pl.DeviceIdType.MESH
NB = 128
PAIRS = 8
LAG = 3
LAST = 2


def dot_nt(a, b):
    return lax.dot_general(a, b, (((1,), (1,)), ((), ())), precision=HIGH, preferred_element_type=jnp.float32)


def dot_nn(a, b):
    return lax.dot_general(a, b, (((1,), (0,)), ((), ())), precision=HIGH, preferred_element_type=jnp.float32)


def lane_of(x, lane):
    return jnp.broadcast_to(x[:, lane:lane + 1], (8, NB))


def row_of(x, row):
    return jnp.broadcast_to(x[row:row + 1, :], (8, NB))


def factor_block(load, store_upper, store_inv, beside=None):
    lane = lax.broadcasted_iota(jnp.int32, (8, NB), 1)
    sub = lax.broadcasted_iota(jnp.int32, (8, NB), 0)
    rows = [load(i) for i in range(16)]
    for g in range(16):
        base = 8 * g
        inside = (lane >= base) & (lane < base + 8)
        cols = [jnp.where(sub < 8, lane_of(rows[g], base + t), 0.0) for t in range(8)]
        cur = jnp.where(inside, jnp.where(lane - base == sub, 1.0, 0.0), rows[g])
        recips, pivots, cross = [], [], {}
        for s in range(8):
            recip = 1.0 / row_of(cols[s], s)
            pivot = row_of(cur, s)
            mult = jnp.where(sub > s, cols[s] * recip, 0.0)
            for t in range(s + 1, 8):
                cross[t, s] = row_of(cols[t], s)
                cols[t] = cols[t] - mult * cross[t, s]
            if s < 7:
                cur = cur - mult * pivot
            recips.append(recip)
            pivots.append(pivot)
        for i in range(g + 1, 16):
            part = [lane_of(rows[i], base + t) for t in range(8)]
            acc = jnp.where(inside, 0.0, rows[i])
            for s in range(8):
                mult = part[s] * recips[s]
                for t in range(s + 1, 8):
                    part[t] = part[t] - mult * cross[t, s]
                acc = acc - mult * pivots[s]
            rows[i] = acc
        if beside is not None:
            beside(g)
        diag = cols[7]
        upper = jnp.where(lane > base + 7, cur, 0.0)
        for t in range(8):
            if t < 7:
                diag = jnp.where(sub == t, cols[t], diag)
            upper = jnp.where((lane == base + t) & (sub <= t), cols[t], upper)
        scale = lax.rsqrt(diag)
        scale = scale * (1.5 - 0.5 * diag * scale * scale)
        store_upper(g, upper * scale)
        store_inv(g, jnp.where(lane < base + 8, cur, 0.0) * scale)


def body(pan, raw, trail, pan_out, schur_out, top_out, left_out, right_out, work, cols, schur, diag, upper, inv, gmat, top, zero, stage,
         lead_sem, lead_send, lead_recv, own_sem, own_send, own_recv, keep_sem, give_send, give_recv, pass_send,
         far_send, far_recv, in_sem, out_sem, top_sem, left_sem, pan_sem):
    my_row = lax.axis_index("pr")
    my_col = lax.axis_index("pc")
    chip = my_row // 2
    core = my_row % 2
    beside_row = 2 * chip + 1 - core
    along_row = 2 * (1 - chip) + core
    cross_row = 2 * (1 - chip) + 1 - core
    across = {"pr": my_row, "pc": 1 - my_col}
    beside = {"pr": beside_row, "pc": my_col}
    along = {"pr": along_row, "pc": my_col}
    is_giver = core == my_col

    barrier = pltpu.get_barrier_semaphore()
    for peer in (across, beside, along):
        pl.semaphore_signal(barrier, inc=1, device_id=peer, device_id_type=MESH)

    def half(c):
        return pl.ds(pl.multiple_of(c * NB, NB), NB)

    def remote(src, dst, send, recv, peer):
        return pltpu.make_async_remote_copy(src_ref=src, dst_ref=dst, send_sem=send, recv_sem=recv,
                                            device_id=peer, device_id_type=MESH)

    first_part = (0, 0, 1, 0)
    second_part = (0, 1, 4, 1)

    def for_pair(p, fn):
        if isinstance(p, int):
            fn((p, p // 2, 4, p + 1))
        else:
            for first in range(4):
                pl.when(p // 2 == first)(lambda first=first: fn((p, first, 4, p + 1)))

    def strip(part, row, col):
        p, lo, hi, _ = part
        return work.at[p, lo:hi, row, :, half(col)]

    def mine(part):
        p, lo, hi, _ = part
        return pan.at[p, lo:hi]

    def keep_strip(part):
        return pltpu.make_async_copy(mine(part), strip(part, my_row, my_col), lead_sem.at[part[3]])

    def lead_copy(part, kind):
        row, col, peer, slot = {
            0: (my_row, my_col, beside, 0),
            1: (my_row, my_col, along, 1),
            2: (my_row, my_col, across, 2),
            3: (my_row, 1 - my_col, along, 3),
            4: (along_row, my_col, beside, 4),
            5: (my_row, 1 - my_col, beside, 5),
            6: (along_row, 1 - my_col, beside, 6),
            7: (along_row, my_col, across, 3),
        }[kind]
        there = strip(part, row, col)
        return remote(mine(part) if kind < 3 else there, there, lead_send.at[part[3], slot], lead_recv.at[part[3], slot], peer)

    def lead_arrival(part, kind):
        row, col = [(beside_row, my_col), (along_row, my_col), (my_row, 1 - my_col), (along_row, 1 - my_col),
                    (cross_row, my_col), (beside_row, 1 - my_col), (cross_row, 1 - my_col)][kind]
        return remote(mine(part), strip(part, row, col), lead_send.at[part[3], kind], lead_recv.at[part[3], kind], beside)

    def stage_one(part):
        for kind in (1, 2, 0):
            lead_copy(part, kind).start()

    def stage_two(part):
        lead_arrival(part, 1).wait_recv()
        lead_arrival(part, 2).wait_recv()

        @pl.when(core == 0)
        def _():
            lead_copy(part, 3).start()

        @pl.when(core == 1)
        def _():
            lead_copy(part, 7).start()

        lead_copy(part, 4).start()
        lead_copy(part, 5).start()

    def stage_three(part):
        lead_arrival(part, 3).wait_recv()
        lead_copy(part, 6).start()

    def lead_wait(part):
        keep_strip(part).wait()
        for kind in (0, 4, 5, 6):
            lead_arrival(part, kind).wait_recv()
        for kind in range(7):
            lead_copy(part, kind).wait_send()

    def own_load():
        return pltpu.make_async_copy(raw.at[pl.ds(512, 1024)], stage, own_sem.at[0])

    def spread_own():
        flat = stage.reshape(1024 * PAIRS, NB)
        for p in range(PAIRS):
            work[p, 4:6, :, :, half(my_col)] = flat[pl.ds(p, 1024, stride=PAIRS), :].reshape(2, 4, NB, NB)

    def own_copy(p):
        there = work.at[p, 4:6, :, :, half(my_col)]
        return remote(there, there, own_send.at[p], own_recv.at[p], across)

    def own_arrival(p):
        there = work.at[p, 4:6, :, :, half(1 - my_col)]
        return remote(there, there, own_send.at[p], own_recv.at[p], across)

    def keep_copy(p):
        return pltpu.make_async_copy(work.at[p, 4:6], cols.at[p, :, :, chip], keep_sem.at[p])

    def give_copy(p):
        return remote(work.at[p, 4:6], cols.at[p, :, :, chip], give_send.at[p], give_recv.at[p], beside)

    def far_copy(p):
        return remote(work.at[p, 4:6], cols.at[p, :, :, chip], far_send.at[p], far_recv.at[p], along)

    def far_arrival(p):
        return remote(work.at[p, 4:6], cols.at[p, :, :, 1 - chip], far_send.at[p], far_recv.at[p], along)

    def pass_copy(p):
        return remote(cols.at[p, :, :, 1 - chip], cols.at[p, :, :, 1 - chip], pass_send.at[p], far_recv.at[p], beside)

    def cols_wait(p):
        @pl.when(is_giver)
        def _():
            keep_copy(p).wait()

        @pl.when(jnp.logical_not(is_giver))
        def _():
            give_copy(p).wait_recv()
            far_arrival(p).wait_recv()

    def rows256(p, c):
        return work[p, c // 2, pl.ds(2 * (c % 2), 2)].reshape(256, 256)

    def set_rows256(p, c, value):
        work[p, c // 2, pl.ds(2 * (c % 2), 2)] = value.reshape(2, NB, 256)

    def rows512(p, r):
        return work[p, r].reshape(512, 256)

    def set_rows512(p, r, value):
        work[p, r] = value.reshape(4, NB, 256)

    def own_rows(p):
        return work[p, 4:6].reshape(1024, 256)

    def set_own(p, value):
        work[p, 4:6] = value.reshape(2, 4, NB, 256)

    def tile_in(b):
        return pltpu.make_async_copy(trail.at[pl.ds(512, 1024), pl.ds(b * 256, 256)], schur.at[b], in_sem.at[b])

    keep_strip(first_part).start()
    keep_strip(second_part).start()
    for p in range(1, PAIRS):
        for_pair(p, lambda part: keep_strip(part).start())
    zero[...] = jnp.zeros_like(zero)
    gmat[...] = jnp.zeros_like(gmat)
    pl.semaphore_wait(barrier, 3)
    stage_one(first_part)
    stage_two(first_part)
    stage_one(second_part)
    for_pair(1, stage_one)
    stage_three(first_part)
    own_load().start()
    lead_wait(first_part)

    def schur_update(q, b):
        schur[b] = schur[b] - dot_nt(own_rows(q), cols[q, b // 4, b % 4].reshape(256, 256))

    def factor(h, p):
        def store_upper(g, value):
            upper[8 * g:8 * g + 8, :] = value

        def store_inv(g, value):
            inv[h, 8 * g:8 * g + 8, :] = value

        def load(i):
            return diag[8 * i:8 * i + 8, :]

        @pl.when(p < LAG)
        def _():
            factor_block(load, store_upper, store_inv)

        @pl.when(p >= LAG)
        def _():
            def beside(g):
                if g % 4 == 0:
                    schur_update(p - LAG, 4 * h + g // 4)

            factor_block(load, store_upper, store_inv, beside)

        work[p, p // 2, 2 * (p % 2) + h, :, half(h)] = upper[...].T

    def lead_step(p):
        @pl.when(p > 0)
        def _():
            for_pair(p, lead_wait)

        def subtract(q, carry):
            right = rows256(q, p)

            def one(r, carry):
                set_rows512(p, r, rows512(p, r) - dot_nt(rows512(q, r), right))
                return carry

            return lax.fori_loop(p // 2, 4, one, carry)

        lax.fori_loop(0, p, subtract, 0)

        @pl.when(p == LAG)
        def _():
            for b in range(8):
                tile_in(b).wait()

        @pl.when(p >= LAG)
        def _():
            cols_wait(p - LAG)

        hi, lo = p // 2, 2 * (p % 2)
        diag[...] = work[p, hi, lo, :, 0:NB]

        def factor_half(h, carry):
            factor(h, p)

            @pl.when(h == 0)
            def _():
                work[p, hi, lo, :, NB:256] = jnp.zeros((NB, NB), jnp.float32)
                low = dot_nt(work[p, hi, lo + 1, :, 0:NB], inv[0])
                work[p, hi, lo + 1, :, 0:NB] = low
                diag[...] = work[p, hi, lo + 1, :, NB:256] - dot_nt(low, low)

            @pl.when((h == 0) & (p == 0))
            def _():
                stage_two(second_part)
                for_pair(1, stage_two)
                for_pair(2, stage_one)
                for_pair(3, stage_one)

            @pl.when((h == 0) & (p > 0) & (p + 1 < PAIRS))
            def _():
                for_pair(p + 1, stage_three)

            @pl.when((h == 0) & (p == 0))
            def _():
                own_load().wait()
                spread_own()

            @pl.when((h == 0) & (p == 1))
            def _():
                for b in range(8):
                    tile_in(b).start()

            return carry

        lax.fori_loop(0, 2, factor_half, 0)

        @pl.when(p == 0)
        def _():
            stage_three(second_part)

        gmat[p % 2, 0:NB, 0:NB] = inv[0]
        gmat[p % 2, NB:256, NB:256] = inv[1]
        gmat[p % 2, NB:256, 0:NB] = -dot_nn(inv[1], dot_nn(work[p, hi, lo + 1, :, 0:NB], inv[0]))

        @pl.when(p == 0)
        def _():
            lead_wait(second_part)

        @pl.when(p % 2 == 0)
        def _():
            set_rows256(p, p + 1, dot_nt(rows256(p, p + 1), gmat[p % 2]))

        def solve(r, carry):
            set_rows512(p, r, dot_nt(rows512(p, r), gmat[p % 2]))
            return carry

        lax.fori_loop(p // 2 + 1, 4, solve, 0)

        @pl.when(p == 0)
        def _():
            for_pair(1, stage_three)

        @pl.when(p + 2 < PAIRS)
        def _():
            for_pair(p + 2, stage_two)

        @pl.when(p + 4 < PAIRS)
        def _():
            for_pair(p + 4, stage_one)

        own_copy(p).start()

    def own_step(p):
        @pl.when(is_giver & (p > 0) & (p < PAIRS - 1))
        def _():
            far_arrival(p - 1).wait_recv()
            pass_copy(p - 1).start()

        own_arrival(p).wait_recv()
        own_copy(p).wait_send()

        def subtract(q, carry):
            set_own(p, own_rows(p) - dot_nt(own_rows(q), rows256(q, p)))
            return carry

        lax.fori_loop(0, p, subtract, 0)
        set_own(p, dot_nt(own_rows(p), gmat[p % 2]))

        @pl.when(is_giver)
        def _():
            far_copy(p).start()
            keep_copy(p).start()
            give_copy(p).start()

    def chain_step(p, carry):
        @pl.when(p < PAIRS)
        def _():
            lead_step(p)

        @pl.when(p > 0)
        def _():
            own_step(p - 1)

        return carry

    lax.fori_loop(0, PAIRS + 1, chain_step, 0)

    def start_pan(p, carry):
        pltpu.make_async_copy(work.at[p, 4:6, :, :, half(my_col)], pan_out.at[p, 1:3], pan_sem.at[0]).start()
        for r in range(4):
            below = 4 * r + my_row >= 2 * p + my_col

            @pl.when(below)
            def _():
                pltpu.make_async_copy(work.at[p, r, my_row, :, half(my_col)], pan_out.at[p, 0, r], pan_sem.at[0]).start()

            @pl.when(jnp.logical_not(below))
            def _():
                pltpu.make_async_copy(zero, pan_out.at[p, 0, r], pan_sem.at[0]).start()

        return carry

    lax.fori_loop(0, PAIRS, start_pan, 0)

    def left_copy():
        return pltpu.make_async_copy(work.at[PAIRS - LAST:PAIRS, 4:6], left_out, left_sem.at[0])

    def right_copy():
        return pltpu.make_async_copy(cols.at[PAIRS - LAST:PAIRS], right_out, left_sem.at[1])

    def schur_copy(b):
        return pltpu.make_async_copy(schur.at[b], schur_out.at[b], out_sem.at[b])

    def top_copy(r):
        return pltpu.make_async_copy(top.at[r % 2], top_out.at[r], top_sem.at[r % 2])

    def top_rows(r):
        if r >= 2:
            top_copy(r - 2).wait()
        p = 2 * r + my_row // 2
        side = half(my_row % 2)

        def one(b, carry):
            top[r % 2, b] = dot_nt(work[p, r, my_row, :, side], cols[p, b // 4, b % 4, :, :, side].reshape(256, NB))
            return carry

        lax.fori_loop(0, 8, one, 0)
        top_copy(r).start()

    left_copy().start()

    for q in range(PAIRS - LAG, PAIRS - LAST):
        cols_wait(q)

    def tail(b, carry):
        for q in range(PAIRS - LAG, PAIRS - LAST):
            schur_update(q, b)
        schur_copy(b).start()
        return carry

    lax.fori_loop(0, 8, tail, 0)

    @pl.when(is_giver)
    def _():
        far_arrival(PAIRS - 2).wait_recv()
        pass_copy(PAIRS - 2).start()

    for r in range(3):
        top_rows(r)

    @pl.when(is_giver)
    def _():
        far_arrival(PAIRS - 1).wait_recv()
        pass_copy(PAIRS - 1).start()

    for q in range(PAIRS - LAST, PAIRS):
        cols_wait(q)
    right_copy().start()
    top_rows(3)
    top_copy(2).wait()
    top_copy(3).wait()
    for b in range(8):
        schur_copy(b).wait()
    left_copy().wait()
    right_copy().wait()
    pltpu.make_async_copy(pan_out, pan_out, pan_sem.at[0]).wait()

    def finish(p, carry):
        @pl.when(is_giver)
        def _():
            give_copy(p).wait_send()
            far_copy(p).wait_send()
            pass_copy(p).wait_send()

        return carry

    lax.fori_loop(0, PAIRS, finish, 0)


def finish_body(schur, top, left, right, pan, trail_out, pan_out):
    trail_out[0:512, :] = top[...].reshape(512, 256)
    total = schur[0]
    for q in range(LAST):
        total = total - dot_nt(left[q].reshape(1024, 256), right[q, 0, 0].reshape(256, 256))
    trail_out[512:1536, :] = total
    flat = pan_out.reshape(192 * PAIRS, NB)
    for p in range(PAIRS):
        flat[pl.ds(p, 192, stride=PAIRS), :] = pan[p]


def solution(mesh):
    def local_part(panel_tile, trail_tile):
        pan = panel_tile[:512].transpose(1, 0, 2).reshape(PAIRS, 4, NB, NB)
        any_spec = pl.BlockSpec(memory_space=pl.ANY)
        dma = pltpu.SemaphoreType.DMA
        f32 = jnp.float32
        pan_out, schur, top, left, right = pl.pallas_call(
            body,
            out_shape=(jax.ShapeDtypeStruct((PAIRS, 3, 4, NB, NB), f32), jax.ShapeDtypeStruct((8, 1024, 256), f32),
                       jax.ShapeDtypeStruct((4, 8, NB, 256), f32), jax.ShapeDtypeStruct((LAST, 2, 4, NB, 256), f32),
                       jax.ShapeDtypeStruct((LAST, 2, 4, 2, NB, 256), f32)),
            in_specs=[any_spec] * 3,
            out_specs=(any_spec,) * 5,
            scratch_shapes=[
                pltpu.VMEM((PAIRS, 6, 4, NB, 256), jnp.float32),
                pltpu.VMEM((PAIRS, 2, 4, 2, NB, 256), jnp.float32),
                pltpu.VMEM((8, 1024, 256), jnp.float32),
                pltpu.VMEM((NB, NB), jnp.float32),
                pltpu.VMEM((NB, NB), jnp.float32),
                pltpu.VMEM((2, NB, NB), jnp.float32),
                pltpu.VMEM((2, 256, 256), jnp.float32),
                pltpu.VMEM((2, 8, NB, 256), jnp.float32),
                pltpu.VMEM((NB, NB), jnp.float32),
                pltpu.VMEM((1024, PAIRS, NB), jnp.float32),
                dma((PAIRS + 1,)), dma((PAIRS + 1, 7)), dma((PAIRS + 1, 7)), dma((PAIRS,)), dma((PAIRS,)), dma((PAIRS,)), dma((PAIRS,)),
                dma((PAIRS,)), dma((PAIRS,)), dma((PAIRS,)), dma((PAIRS,)), dma((PAIRS,)), dma((8,)), dma((8,)), dma((2,)), dma((2,)),
                dma((1,)),
            ],
            compiler_params=pltpu.CompilerParams(collective_id=0, has_side_effects=True, vmem_limit_bytes=64 * 1024 * 1024 - 65536),
            name="factor",
        )(pan, panel_tile, trail_tile)
        trail_out, panel_out = pl.pallas_call(
            finish_body,
            grid=(8,),
            out_shape=(jax.ShapeDtypeStruct(trail_tile.shape, f32), jax.ShapeDtypeStruct(panel_tile.shape, f32)),
            in_specs=[
                pl.BlockSpec((1, 1024, 256), lambda b: (b, 0, 0)),
                pl.BlockSpec((4, 1, NB, 256), lambda b: (0, b, 0, 0)),
                pl.BlockSpec((LAST, 2, 4, NB, 256), lambda b: (0, 0, 0, 0, 0)),
                pl.BlockSpec((LAST, 1, 1, 2, NB, 256), lambda b: (0, b // 4, b % 4, 0, 0, 0)),
                pl.BlockSpec((PAIRS, 192, NB), lambda b: (0, b, 0)),
            ],
            out_specs=(pl.BlockSpec((1536, 256), lambda b: (0, b)), pl.BlockSpec((192, PAIRS, NB), lambda b: (b, 0, 0))),
            compiler_params=pltpu.CompilerParams(vmem_limit_bytes=64 * 1024 * 1024 - 65536),
            name="finish",
        )(schur, top, left, right, pan_out.reshape(PAIRS, 1536, NB))
        return panel_out, trail_out

    spec_panel = P("pr", "pc", None)
    spec_trail = P("pr", "pc")
    return jax.shard_map(local_part, mesh=mesh, in_specs=(spec_panel, spec_trail), out_specs=(spec_panel, spec_trail), check_vma=False)
```
